256 devices in a mesh: grp: 2 (over y_lo), mesh: 128 (over z, x, y_hi, core).
Axes of the slice: x: 4, y: 4 (y_hi: 2, y_lo: 2; y = y_hi * 2 + y_lo), z: 8, core: 2. Of those that a mesh axis runs over, the one named last changes fastest.
Arguments:
- state: float32 [2, 5, 2048, 4096], P('grp', None, 'mesh'), may hold values from -6 to 6
- burn_rate: float32 [2, 2048, 4096], P('grp', 'mesh'), may hold values from 0.1 to 1
- face_map: int32 [2, 128, 1024], P('grp', 'mesh'), may hold values from 0 to 1023, as said below
Outputs:
- new_state: float32 [2, 5, 2048, 4096], P('grp', None, 'mesh')
- head: float32 [2, 2048, 4096], P('grp', 'mesh')
The draws below stay inside these ranges and needn't reach their ends.
Inputs may be any that keep to these rules, and one draw needn't show every extreme that they name: `face_map`: entry k * 64 + j of a mesh names the cell of its partner's interface plane that feeds its ghost cell (k, j).
All inputs are finite; a program needn't handle non-finite values.
Results may differ from the reference program's by a relative error of at most 0.00025.
Values sent between devices are 32-bit elements; how exact they have to be, the bound alone decides.
A program may use at most 64 MiB of HBM per device.

```python
import math
import jax
import jax.numpy as jnp
from jax import lax

NX = 64
NY = 64
CZ = 16
FIELDS = 5
SECTIONS = 2
ITERS = 3
NZ = 2048
N_MESH = 128


def draw_face_map(key, part):
    offset_z = jax.random.randint(jax.random.fold_in(key, 101), (N_MESH, 1), 0, CZ - CZ // 4 + 1)
    offset_y = jax.random.randint(jax.random.fold_in(key, 102), (N_MESH, 1), 0, NY - NY // 4 + 1)
    cells = jnp.arange(CZ * NY, dtype=jnp.int32)[None, :]
    row_z = cells // NY
    row_y = cells % NY
    fine_rows = (offset_z + row_z // 4) * NY + (offset_y + row_y // 4)
    jitter_z = jax.random.randint(jax.random.fold_in(key, 103), (N_MESH, CZ * NY), 0, 4)
    jitter_y = jax.random.randint(jax.random.fold_in(key, 104), (N_MESH, CZ * NY), 0, 4)
    coarse_z = jnp.clip(4 * (row_z - offset_z) + jitter_z, 0, CZ - 1)
    coarse_y = jnp.clip(4 * (row_y - offset_y) + jitter_y, 0, NY - 1)
    coarse_rows = coarse_z * NY + coarse_y
    return jnp.stack([fine_rows, coarse_rows]).astype(jnp.int32)


def level_of(rng, extent, pieces, smallest, high):
    def one(axis_at, parts):
        heights = jax.random.uniform(jax.random.fold_in(jax.random.fold_in(rng, 6), axis_at), (parts,), jnp.float32, smallest / len(pieces), high / len(pieces))
        return jnp.repeat(jnp.exp(heights), extent[axis_at] // parts).reshape((-1,) + (1,) * (len(extent) - axis_at - 1))

    gain = one(*pieces[0])
    for cut in pieces[1:]:
        gain = gain * one(*cut)
    return gain


def gaussian(stream_key, shape, spread, reach, cuts=(), kind=jnp.bfloat16):
    factor_of = level_of(stream_key, shape, cuts, -0.22, 0.18) if cuts else 1.0
    values = jax.random.normal(stream_key, shape, jnp.float32) * spread * factor_of
    return jnp.minimum(jnp.maximum(values, -reach), reach).astype(kind)


def setup_inputs(seed: int = 0) -> dict:
    seeds = jax.random.split(jax.random.key(seed), 4)
    state = gaussian(seeds[0], (2, FIELDS, NZ, NX * NY), 1.0, 6.0, ((0, 2), (2, 128)), jnp.float32)
    burn_rate = jnp.clip(jnp.exp(math.log(1.0) - 2.3025851 * jax.random.uniform(seeds[1], (2, NZ, NX * NY), jnp.float32) ** level_of(seeds[1], (2, NZ, NX * NY), ((0, 2), (1, 128)), -0.2, 0.2)), 0.1, 1.0)
    face_map = draw_face_map(jax.random.fold_in(seeds[3], 71), 0)
    return dict(state=state, burn_rate=burn_rate, face_map=face_map)


COURANT = 0.1
DIFFUSION = 0.05
STOICHIOMETRY = 2.0
EXPANSION = 1.0

def sine_table(length):
    places = jnp.arange(length, dtype=jnp.float32) + 1.0
    angles = jnp.pi * places[:, None] * places[None, :] / (length + 1)
    return jnp.sin(angles) * jnp.sqrt(2.0 / (length + 1))

def mode_values(length):
    places = jnp.arange(length, dtype=jnp.float32) + 1.0
    return 2.0 - 2.0 * jnp.cos(jnp.pi * places / (length + 1))

def poisson_solve(source):
    table_z = sine_table(source.shape[1]).astype(source.dtype)
    table_x = sine_table(source.shape[2]).astype(source.dtype)
    table_y = sine_table(source.shape[3]).astype(source.dtype)
    precise = lax.Precision.HIGHEST
    spectral = jnp.einsum('ck,mkij->mcij', table_z, source, precision=precise)
    spectral = jnp.einsum('ai,mcij->mcaj', table_x, spectral, precision=precise)
    spectral = jnp.einsum('mcaj,jb->mcab', spectral, table_y, precision=precise)
    modes = (mode_values(source.shape[1])[:, None, None] + mode_values(source.shape[2])[None, :, None] + mode_values(source.shape[3])[None, None, :]).astype(source.dtype)
    spectral = spectral / modes[None]
    solved = jnp.einsum('ck,mcab->mkab', table_z, spectral, precision=precise)
    solved = jnp.einsum('ai,mkab->mkib', table_x, solved, precision=precise)
    return jnp.einsum('mkib,jb->mkij', solved, table_y, precision=precise)

def tendency(zpadded, x_low, x_high, burning):
    centre = zpadded[:, 2:-2]
    xpadded = jnp.concatenate([x_low[:, :, None, :], centre, x_high[:, :, None, :]], axis=2)
    ypadded = jnp.pad(centre, ((0, 0), (0, 0), (0, 0), (1, 1)))
    east, west = (xpadded[:, :, 2:], xpadded[:, :, :-2])
    north, south = (ypadded[..., 2:], ypadded[..., :-2])
    above, below = (zpadded[:, 3:-1], zpadded[:, 1:-3])
    above_two, below_two = (zpadded[:, 4:], zpadded[:, :-4])
    grad_x = 0.5 * (east - west)
    grad_y = 0.5 * (north - south)
    grad_z = (8.0 * (above - below) - (above_two - below_two)) / 12.0
    laplace = east + west + north + south + above + below - 6.0 * centre
    advection = centre[0] * grad_x + centre[1] * grad_y + centre[2] * grad_z
    reaction = burning * centre[3] * centre[4]
    change = -COURANT * advection + DIFFUSION * laplace
    change = change.at[3].add(-reaction).at[4].add(-STOICHIOMETRY * reaction)
    divergence = grad_x[0] + grad_y[1] + 0.5 * (above[2] - below[2])
    return (change, EXPANSION * reaction - divergence)

def with_ghosts(source, z_low, z_high, x_low, x_high):
    source = source.at[:, 0].add(z_low).at[:, -1].add(z_high)
    return source.at[:, :, 0, :].add(x_low).at[:, :, -1, :].add(x_high)

def correct(fields, pressure, z_low, z_high, x_low, x_high):
    xpadded = jnp.concatenate([x_low[:, None, :], pressure, x_high[:, None, :]], axis=1)
    ypadded = jnp.pad(pressure, ((0, 0), (0, 0), (1, 1)))
    zpadded = jnp.concatenate([z_low[None], pressure, z_high[None]], axis=0)
    grad_x = 0.5 * (xpadded[:, 2:] - xpadded[:, :-2])
    grad_y = 0.5 * (ypadded[..., 2:] - ypadded[..., :-2])
    grad_z = 0.5 * (zpadded[2:] - zpadded[:-2])
    return jnp.concatenate([fields[0:1] - grad_x[None], fields[1:2] - grad_y[None], fields[2:3] - grad_z[None], fields[3:]], axis=0)

def interface(arrays, group):
    return arrays[..., -1, :] if group == 0 else arrays[..., 0, :]

def cross_ghosts(arrays, face_map, group):
    plane = interface(arrays[1 - group], 1 - group)
    flat = plane.reshape((-1, N_MESH, CZ * NY))
    picked = jnp.take_along_axis(flat, jnp.broadcast_to(face_map[group], flat.shape).astype(jnp.int32), axis=-1)
    picked = picked.reshape(plane.shape)
    zeros = jnp.zeros_like(picked)
    return (zeros, picked) if group == 0 else (picked, zeros)

def reference(state, burn_rate, face_map):
    initial = state.reshape(2, FIELDS, NZ, NX, NY)
    burning = burn_rate.reshape(2, NZ, NX, NY)
    current = initial
    pressure = jnp.zeros((2, N_MESH, CZ, NX, NY), state.dtype)
    for section_no in range(SECTIONS):
        predicted = []
        sources = []
        for group in range(2):
            x_low, x_high = cross_ghosts(current, face_map, group)
            zpadded = jnp.pad(current[group], ((0, 0), (2, 2), (0, 0), (0, 0)))
            change, source = tendency(zpadded, x_low, x_high, burning[group])
            if section_no == 0:
                predicted.append(current[group] + change)
            else:
                predicted.append(0.5 * (initial[group] + current[group] + change))
            sources.append(source.reshape(N_MESH, CZ, NX, NY))
        pressure = jnp.zeros((2, N_MESH, CZ, NX, NY), state.dtype)
        zero_layer = jnp.zeros((1, NX, NY), state.dtype)
        for sweep in range(ITERS):
            solved = []
            for group in range(2):
                z_low = jnp.concatenate([zero_layer, pressure[group][:-1, -1]], axis=0)
                z_high = jnp.concatenate([pressure[group][1:, 0], zero_layer], axis=0)
                x_low, x_high = cross_ghosts(pressure, face_map, group)
                solved.append(poisson_solve(with_ghosts(sources[group], z_low, z_high, x_low, x_high)))
            pressure = jnp.stack(solved)
        corrected = []
        for group in range(2):
            x_low, x_high = cross_ghosts(pressure, face_map, group)
            zero_plane = jnp.zeros((NX, NY), state.dtype)
            corrected.append(correct(predicted[group], pressure[group].reshape(NZ, NX, NY), zero_plane, zero_plane, x_low.reshape(NZ, NY), x_high.reshape(NZ, NY)))
        current = jnp.stack(corrected)
    return (current.reshape(2, FIELDS, NZ, NX * NY), pressure.reshape(2, NZ, NX * NY))
```

```python
import math

import jax
import jax.numpy as jnp
import numpy as np
from jax import lax
from jax.experimental import pallas as pl
from jax.experimental.pallas import tpu as pltpu
from jax.sharding import PartitionSpec as P

NX = 64
NY = 64
CZ = 16
FIELDS = 5
SECTIONS = 2
ITERS = 3
COURANT = 0.1
DIFFUSION = 0.05
STOICHIOMETRY = 2.0
EXPANSION = 1.0

PLANE = 32
LEVEL = FIELDS * PLANE
HALO = 2
MESH = pl.DeviceIdType.MESH
F32 = jnp.float32
BF16 = jnp.bfloat16


def sine(n):
    i = np.arange(n, dtype=np.float64) + 1.0
    return np.sin(np.pi * i[:, None] * i[None, :] / (n + 1)) * math.sqrt(2.0 / (n + 1))


def eigen(n):
    i = np.arange(n, dtype=np.float64) + 1.0
    return 2.0 - 2.0 * np.cos(np.pi * i / (n + 1))


T_IM = 0
T_Z1 = 512
T_Z2 = 576
T_W = 640
T_SX = 648
T_ROWS = 776
B_Y = 0
B_XF = 128
B_XI = 192
B_ROWS = 256


def tables():
    s16, s64 = sine(CZ), sine(NX)
    tab = np.zeros((T_ROWS, 128))
    modes = eigen(CZ)[:, None, None] + eigen(NX)[None, :, None] + eigen(NY)[None, None, :]
    inv = 1.0 / modes
    tab[T_IM : T_IM + 512] = (
        inv.reshape(8, 2, 64, 64).transpose(0, 2, 1, 3).reshape(512, 128)
    )
    for p in range(8):
        for h in range(2):
            lanes = slice(64 * h, 64 * h + 64)
            for r in range(8):
                tab[T_Z1 + p * 8 + r, lanes] = s16[2 * p + h, 2 * r + h]
                tab[T_Z2 + p * 8 + r, lanes] = s16[2 * p + 1 - h, 2 * r + h]
            tab[T_W + p, lanes] = s16[2 * p + h, 0]
    tab[T_SX : T_SX + 64] = s64[:, 63][:, None]
    tab[T_SX + 64 : T_SX + 128] = s64[:, 0][:, None]
    mat = np.zeros((B_ROWS, 128))
    mat[B_Y : B_Y + 128] = np.kron(np.eye(2), s64)
    order = np.concatenate([np.arange(0, 64, 2), np.arange(1, 64, 2)])
    mat[B_XF : B_XF + 64, :64] = s64[:, order]
    mat[B_XI : B_XI + 64, :64] = s64[order, :]
    mat = mat.astype(np.float32)
    high = mat.astype(jnp.bfloat16)
    low = (mat - high.astype(np.float32)).astype(jnp.bfloat16)
    return tab.astype(np.float32), high, low


S16 = sine(CZ)


def split(v):
    high = v.astype(BF16)
    return high, (v - high.astype(F32)).astype(BF16)


def dot(a, b):
    return jnp.dot(a, b, preferred_element_type=F32)


def dot_right(v, th, tl):
    vh, vl = split(v)
    return dot(vh, th) + (dot(vl, th) + dot(vh, tl))


def dot_left(th, tl, v):
    vh, vl = split(v)
    return dot(th, vh) + (dot(th, vl) + dot(tl, vh))


def kernel(
    state, burn, fmap, tab_h, bh_h, bl_h, out_s, out_p,
    stn, bnn, fld0, fld1, fields, burning, src, ybuf, hat1, hat, prs0, prs1,
    edge, xg, zsend, zrecv, psend, qsend, qrecv, fsend, frecv, tab, bh, bl, idx, outn, outp,
    in_sem, t_sem, out_sem, send_sem, recv_sem,
):
    g = lax.axis_index("grp")
    m = lax.axis_index("mesh")
    n = lax.axis_size("mesh")
    low = lax.rem(m + n - 1, n)
    high = lax.rem(m + 1, n)
    fine = g == 0
    LOW, HIGH, PARTNER = 0, 1, 2
    where_to = ({"mesh": low}, {"mesh": high}, {"grp": 1 - g})

    loads = [
        pltpu.make_async_copy(state.at[f], stn.at[f], in_sem.at[f]) for f in range(FIELDS)
    ]
    loads.append(pltpu.make_async_copy(burn, bnn, in_sem.at[FIELDS]))
    for copy in loads:
        copy.start()
    table_loads = [
        pltpu.make_async_copy(a, b, t_sem.at[i])
        for i, (a, b) in enumerate(((fmap, idx), (tab_h, tab), (bh_h, bh), (bl_h, bl)))
    ]
    for copy in table_loads:
        copy.start()

    barrier = pltpu.get_barrier_semaphore()
    for target in where_to:
        pl.semaphore_signal(barrier, inc=1, device_id=target, device_id_type=MESH)
    pl.semaphore_wait(barrier, 3)

    def remote(exchange, to, a, b):
        slot = exchange * 3 + to
        return pltpu.make_async_remote_copy(
            src_ref=a, dst_ref=b, send_sem=send_sem.at[slot], recv_sem=recv_sem.at[slot],
            device_id=where_to[to], device_id_type=MESH,
        )

    lane = lax.broadcasted_iota(jnp.int32, (PLANE, 128), 1)
    row = lax.broadcasted_iota(jnp.int32, (PLANE, 128), 0)
    half0 = lane < 64
    y_last = (lane == 63) | (lane == 127)
    y_first = (lane == 0) | (lane == 64)
    x_last = (row == PLANE - 1) & (lane >= 64)
    x_first = (row == 0) & half0
    half8 = lax.broadcasted_iota(jnp.int32, (8, 128), 1) < 64
    half64 = lax.broadcasted_iota(jnp.int32, (64, 128), 1) < 64
    sub8 = lax.broadcasted_iota(jnp.int32, (8, 128), 0)

    def swap(v):
        return pltpu.roll(v, 64, 1)

    def rows(start, size):
        return pl.ds(pl.multiple_of(start, 8), size)

    def level(k, f):
        return ((k + HALO) * FIELDS + f) * PLANE

    def to_layers(load, store):
        for b in range(2):
            @pl.loop(0, 4)
            def _(t):
                tiles = jnp.stack(
                    [
                        load(b, pl.ds(pl.multiple_of((t * 8 + i) * 128, 128), 128))
                        for i in range(8)
                    ]
                )
                turned = jnp.swapaxes(tiles, 0, 1)
                for i in range(8):
                    store(b * 8 + i, t * 8, turned[i])

    def to_native(load, store):
        for b in range(2):
            @pl.loop(0, 4)
            def _(t):
                tiles = jnp.stack([load(b * 8 + i, t * 8) for i in range(8)])
                turned = jnp.swapaxes(tiles, 0, 1)
                for i in range(8):
                    store(b, pl.ds(pl.multiple_of((t * 8 + i) * 128, 128), 128), turned[i])

    for f in range(FIELDS):
        loads[f].wait()

        def load_state(b, lanes, f=f):
            return stn[f, b * 8 : b * 8 + 8, lanes]

        def store_state(k, r, v, f=f):
            fld0[rows(level(k, f) + r, 8), :] = v

        to_layers(load_state, store_state)

    def pack_edges():
        for f in range(FIELDS):
            even = edge[pl.ds(f * 16, 8, stride=2), :]
            odd = edge[pl.ds(f * 16 + 1, 8, stride=2), :]
            own = jnp.where(
                fine, jnp.where(half8, swap(even), odd), jnp.where(half8, even, swap(odd))
            )
            yield f, own

    def send_fields(fld, s):
        copies = [
            remote(s * 4, LOW, fld.at[pl.ds(level(0, 0), 2 * LEVEL)],
                   fld.at[pl.ds(level(CZ, 0), 2 * LEVEL)]),
            remote(s * 4, HIGH, fld.at[pl.ds(level(CZ - 2, 0), 2 * LEVEL)],
                   fld.at[pl.ds(level(-2, 0), 2 * LEVEL)]),
            remote(s * 4, PARTNER, fsend.at[s], frecv.at[s]),
        ]
        copies[0].start()
        copies[1].start()
        at = jnp.where(fine, PLANE - 1, 0)
        for k in range(CZ):
            for f in range(FIELDS):
                edge[pl.ds(f * 16 + k, 1), :] = fld[pl.ds(level(k, f) + at, 1), :]
        for f, own in pack_edges():
            fsend[s, f * 8 : f * 8 + 8, :] = own
        copies[2].start()
        return copies

    def gather(plane):
        index = idx[...]
        column = index & 127
        block = index >> 7
        out = jnp.zeros((8, 128), F32)
        for r in range(8):
            one = jnp.broadcast_to(plane[r : r + 1, :], (8, 128))
            out = jnp.where(block == r, jnp.take_along_axis(one, column, axis=1), out)
        return out

    def spread(ghost, base):
        other = swap(ghost)
        xg[pl.ds(base, 8, stride=2), :] = jnp.where(half8, ghost, other)
        xg[pl.ds(base + 1, 8, stride=2), :] = jnp.where(half8, other, ghost)

    def x_sides(v, ghost):
        ghost = jnp.broadcast_to(ghost, (PLANE, 128))
        turned = swap(v)
        up = pltpu.roll(turned, PLANE - 1, 0)
        down = pltpu.roll(turned, 1, 0)
        zero = jnp.zeros_like(ghost)
        up = jnp.where(x_last, jnp.where(fine, ghost, zero), up)
        down = jnp.where(x_first, jnp.where(fine, zero, ghost), down)
        return jnp.where(half0, turned, up), jnp.where(half0, down, turned)

    def y_sides(v):
        north = jnp.where(y_last, 0.0, pltpu.roll(v, 127, 1))
        south = jnp.where(y_first, 0.0, pltpu.roll(v, 1, 1))
        return north, south

    def tendency_plane(fld, k, finish):
        c = [fld[rows(level(k, f), PLANE), :] for f in range(FIELDS)]
        reaction = burning[rows(k * PLANE, PLANE), :] * c[3] * c[4]
        source = EXPANSION * reaction
        for f in range(FIELDS):
            above = fld[rows(level(k + 1, f), PLANE), :]
            below = fld[rows(level(k - 1, f), PLANE), :]
            above2 = fld[rows(level(k + 2, f), PLANE), :]
            below2 = fld[rows(level(k - 2, f), PLANE), :]
            east, west = x_sides(c[f], xg[pl.ds(f * 16 + k, 1), :])
            north, south = y_sides(c[f])
            gx = 0.5 * (east - west)
            gy = 0.5 * (north - south)
            dz = above - below
            gz = (2.0 / 3.0) * dz - (1.0 / 12.0) * (above2 - below2)
            lap = (east + west) + (north + south) + (above + below) - 6.0 * c[f]
            adv = c[0] * gx + c[1] * gy + c[2] * gz
            change = DIFFUSION * lap - COURANT * adv
            if f == 0:
                source = source - gx
            elif f == 1:
                source = source - gy
            elif f == 2:
                source = source - 0.5 * dz
            elif f == 3:
                change = change - reaction
            else:
                change = change - STOICHIOMETRY * reaction
            finish(k, f, c[f], change)
        src[rows(k * PLANE, PLANE), :] = source

    def z_forward(into):
        @pl.loop(0, 4)
        def _(t):
            v = [src[rows(k * PLANE + t * 8, 8), :] for k in range(CZ)]
            even = [v[k] + v[15 - k] for k in range(8)]
            odd = [v[k] - v[15 - k] for k in range(8)]
            for c in range(CZ):
                part = odd if c % 2 else even
                total = part[0] * F32(S16[c, 0])
                for k in range(1, 8):
                    total = total + part[k] * F32(S16[c, k])
                into[rows(c * PLANE + t * 8, 8), :] = total

    def z_inverse(spec, into, base):
        @pl.loop(0, 4)
        def _(t):
            v = [spec[rows(c * PLANE + t * 8, 8), :] for c in range(CZ)]
            for k in range(8):
                even = v[0] * F32(S16[0, k])
                odd = v[1] * F32(S16[1, k])
                for c in range(1, 8):
                    even = even + v[2 * c] * F32(S16[2 * c, k])
                    odd = odd + v[2 * c + 1] * F32(S16[2 * c + 1, k])
                into[rows(base + k * PLANE + t * 8, 8), :] = even + odd
                into[rows(base + (15 - k) * PLANE + t * 8, 8), :] = even - odd

    def y_matrix():
        return bh[B_Y : B_Y + 128, :], bl[B_Y : B_Y + 128, :]

    def y_transform(v):
        return dot_right(v, *y_matrix())

    def x_forward(a, b):
        even = jnp.where(half0, a, swap(b))
        odd = jnp.where(half0, swap(a), b)
        v = jnp.concatenate([even, odd], axis=0)
        return dot_left(bh[B_XF : B_XF + 64, :64], bl[B_XF : B_XF + 64, :64], v)

    def x_inverse(v):
        v = dot_left(bh[B_XI : B_XI + 64, :64], bl[B_XI : B_XI + 64, :64], v)
        even, odd = v[:PLANE], v[PLANE:]
        return jnp.where(half0, even, swap(odd)), jnp.where(half0, swap(even), odd)

    def z_plane(v):
        other = swap(v)
        out = jnp.zeros((8, 128), F32)
        for p in range(8):
            out = out + tab[T_Z1 + p * 8 : T_Z1 + p * 8 + 8, :] * v[p : p + 1, :]
            out = out + tab[T_Z2 + p * 8 : T_Z2 + p * 8 + 8, :] * other[p : p + 1, :]
        return out

    def side_x():
        return tab[rows(T_SX + g * 64, 64), :]

    def interfaces(spec):
        sx = side_x()
        acc = jnp.zeros((64, 128), F32)
        plane = []
        for p in range(8):
            v = spec[p * 64 : p * 64 + 64, :]
            acc = acc + tab[T_W + p : T_W + p + 1, :] * v
            plane.append(jnp.sum(sx * v, axis=0, keepdims=True))
        other = swap(acc)
        first = acc + other
        last = jnp.where(half64, acc - other, other - acc)
        plane = z_plane(y_transform(jnp.concatenate(plane, axis=0)))
        return first, last, plane

    def narrow(v):
        return jnp.where(half0, v[:PLANE], v[PLANE:])

    def widen(v):
        other = swap(v)
        return jnp.concatenate(
            [jnp.where(half0, v, other), jnp.where(half0, other, v)], axis=0
        )

    at_low = m > 0
    at_high = m < n - 1
    pending = []

    def solve(s, prs):
        z_forward(ybuf)
        ybuf[...] = y_transform(ybuf[...])
        for p in range(8):
            v = x_forward(
                ybuf[2 * p * PLANE : (2 * p + 1) * PLANE, :],
                ybuf[(2 * p + 1) * PLANE : (2 * p + 2) * PLANE, :],
            )
            hat1[p * 64 : p * 64 + 64, :] = v * tab[T_IM + p * 64 : T_IM + p * 64 + 64, :]
        spec = hat1
        for e in range(ITERS - 1):
            at = s * 2 + e
            first, last, plane = interfaces(spec)
            qsend[s * 3 + e] = plane
            zsend[at * 2] = narrow(first)
            zsend[at * 2 + 1] = narrow(last)
            copies = [
                remote(s * 4 + 1 + e, LOW, zsend.at[at * 2], zrecv.at[at * 2 + 1]),
                remote(s * 4 + 1 + e, HIGH, zsend.at[at * 2 + 1], zrecv.at[at * 2]),
                remote(s * 4 + 1 + e, PARTNER, qsend.at[s * 3 + e], qrecv.at[s * 3 + e]),
            ]
            for copy in copies:
                copy.start()
            copies[2].wait_recv()
            ghost = y_transform(z_plane(gather(qrecv[s * 3 + e])))
            copies[0].wait_recv()
            copies[1].wait_recv()
            pending.extend(copies)
            below = widen(jnp.where(at_low, zrecv[at * 2], 0.0))
            above = widen(jnp.where(at_high, zrecv[at * 2 + 1], 0.0))
            both = below + jnp.where(half64, above, -above)
            sx = side_x()
            for p in range(8):
                extra = tab[T_W + p : T_W + p + 1, :] * both + sx * ghost[p : p + 1, :]
                hat[p * 64 : p * 64 + 64, :] = (
                    hat1[p * 64 : p * 64 + 64, :]
                    + extra * tab[T_IM + p * 64 : T_IM + p * 64 + 64, :]
                )
            spec = hat
        e = ITERS - 1
        first, last, plane = interfaces(hat)
        qsend[s * 3 + e] = plane
        a, b = x_inverse(jnp.where(half64, first, last))
        psend[s * 2] = y_transform(a)
        psend[s * 2 + 1] = y_transform(b)
        copies = [
            remote(s * 4 + 3, LOW, psend.at[s * 2], prs.at[pl.ds((CZ + 1) * PLANE, PLANE)]),
            remote(s * 4 + 3, HIGH, psend.at[s * 2 + 1], prs.at[pl.ds(0, PLANE)]),
            remote(s * 4 + 3, PARTNER, qsend.at[s * 3 + e], qrecv.at[s * 3 + e]),
        ]
        for copy in copies:
            copy.start()
        pending.extend(copies)
        for p in range(8):
            a, b = x_inverse(hat[p * 64 : p * 64 + 64, :])
            ybuf[2 * p * PLANE : (2 * p + 1) * PLANE, :] = a
            ybuf[(2 * p + 1) * PLANE : (2 * p + 2) * PLANE, :] = b
        ybuf[...] = y_transform(ybuf[...])
        z_inverse(ybuf, prs, PLANE)
        copies[2].wait_recv()
        spread(gather(qrecv[s * 3 + e]), 0)
        copies[0].wait_recv()
        copies[1].wait_recv()

        @pl.when(jnp.logical_not(at_low))
        def _():
            prs[0:PLANE, :] = jnp.zeros((PLANE, 128), F32)

        @pl.when(jnp.logical_not(at_high))
        def _():
            prs[(CZ + 1) * PLANE : (CZ + 2) * PLANE, :] = jnp.zeros((PLANE, 128), F32)

    def correct(prs, into, base):
        @pl.loop(0, CZ)
        def _(k):
            p = prs[rows((k + 1) * PLANE, PLANE), :]
            above = prs[rows((k + 2) * PLANE, PLANE), :]
            below = prs[rows(k * PLANE, PLANE), :]
            east, west = x_sides(p, xg[pl.ds(k, 1), :])
            north, south = y_sides(p)
            for f, (a, b) in enumerate(((east, west), (north, south), (above, below))):
                at = rows(base + (k * FIELDS + f) * PLANE, PLANE)
                into[at, :] = into[at, :] - 0.5 * (a - b)

    for s in range(SECTIONS):
        fld = (fld0, fld1)[s]
        prs = (prs0, prs1)[s]
        copies = send_fields(fld, s)
        pending.extend(copies)
        if s == 0:
            loads[FIELDS].wait()

            def load_burn(b, lanes):
                return bnn[b * 8 : b * 8 + 8, lanes]

            def store_burn(k, r, v):
                burning[rows(k * PLANE + r, 8), :] = v

            to_layers(load_burn, store_burn)
            for copy in table_loads:
                copy.wait()

            def finish(k, f, c, change):
                fld1[rows(level(k, f), PLANE), :] = c + change
        else:

            def finish(k, f, c, change):
                start = fld0[rows(level(k, f), PLANE), :]
                fields[rows((k * FIELDS + f) * PLANE, PLANE), :] = 0.5 * (start + c + change)

        copies[2].wait_recv()
        for f in range(FIELDS):
            spread(gather(frecv[s, f * 8 : f * 8 + 8, :]), f * 16)

        @pl.loop(2, CZ - 2)
        def _(k, fld=fld, finish=finish):
            tendency_plane(fld, k, finish)

        copies[0].wait_recv()
        copies[1].wait_recv()

        @pl.when(jnp.logical_not(at_low))
        def _(fld=fld):
            fld[0 : 2 * LEVEL, :] = jnp.zeros((2 * LEVEL, 128), F32)

        @pl.when(jnp.logical_not(at_high))
        def _(fld=fld):
            fld[level(CZ, 0) : level(CZ + 2, 0), :] = jnp.zeros((2 * LEVEL, 128), F32)

        @pl.loop(0, 4)
        def _(i, fld=fld, finish=finish):
            tendency_plane(fld, i + (CZ - 4) * (i // 2), finish)

        solve(s, prs)
        if s == 0:
            correct(prs, fld1, level(0, 0))
        else:
            correct(prs, fields, 0)

    def load_field(k, r, f):
        return fields[rows((k * FIELDS + f) * PLANE + r, 8), :]

    stores = []
    for f in range(FIELDS):
        def store_field(b, lanes, v, f=f):
            outn[f, b * 8 : b * 8 + 8, lanes] = v

        to_native(lambda k, r, f=f: load_field(k, r, f), store_field)
        stores.append(pltpu.make_async_copy(outn.at[f], out_s.at[f], out_sem.at[f]))
        stores[-1].start()

    def store_head(b, lanes, v):
        outp[b * 8 : b * 8 + 8, lanes] = v

    to_native(lambda k, r: prs1[rows((k + 1) * PLANE + r, 8), :], store_head)
    stores.append(pltpu.make_async_copy(outp, out_p, out_sem.at[FIELDS]))
    stores[-1].start()
    for copy in pending:
        copy.wait_send()
    for copy in stores:
        copy.wait()


def step(state, burn, fmap):
    anywhere = pl.BlockSpec(memory_space=pl.ANY)
    tab, bh, bl = tables()
    vm = pltpu.VMEM
    layers = (CZ + 2 * HALO) * LEVEL
    return pl.pallas_call(
        kernel,
        out_shape=(
            jax.ShapeDtypeStruct((FIELDS, CZ, NX * NY), F32),
            jax.ShapeDtypeStruct((CZ, NX * NY), F32),
        ),
        in_specs=[anywhere] * 6,
        out_specs=(anywhere, anywhere),
        scratch_shapes=[
            vm((FIELDS, CZ, NX * NY), F32),
            vm((CZ, NX * NY), F32),
            vm((layers, 128), F32),
            vm((layers, 128), F32),
            vm((CZ * LEVEL, 128), F32),
            vm((CZ * PLANE, 128), F32),
            vm((CZ * PLANE, 128), F32),
            vm((CZ * PLANE, 128), F32),
            vm((CZ * PLANE, 128), F32),
            vm((CZ * PLANE, 128), F32),
            vm(((CZ + 2) * PLANE, 128), F32),
            vm(((CZ + 2) * PLANE, 128), F32),
            vm((FIELDS * 16, 128), F32),
            vm((FIELDS * 16, 128), F32),
            vm((8, PLANE, 128), F32),
            vm((8, PLANE, 128), F32),
            vm((4, PLANE, 128), F32),
            vm((6, 8, 128), F32),
            vm((6, 8, 128), F32),
            vm((2, FIELDS * 8, 128), F32),
            vm((2, FIELDS * 8, 128), F32),
            vm((T_ROWS, 128), F32),
            vm((B_ROWS, 128), BF16),
            vm((B_ROWS, 128), BF16),
            vm((8, 128), jnp.int32),
            vm((FIELDS, CZ, NX * NY), F32),
            vm((CZ, NX * NY), F32),
            pltpu.SemaphoreType.DMA((FIELDS + 1,)),
            pltpu.SemaphoreType.DMA((4,)),
            pltpu.SemaphoreType.DMA((FIELDS + 1,)),
            pltpu.SemaphoreType.DMA((24,)),
            pltpu.SemaphoreType.DMA((24,)),
        ],
        compiler_params=pltpu.CompilerParams(
            collective_id=0, has_side_effects=True, vmem_limit_bytes=40 << 20
        ),
        name="fire_step",
    )(state, burn, fmap, jnp.asarray(tab), jnp.asarray(bh), jnp.asarray(bl))


def shards(state, burn_rate, face_map):
    fields, head = step(state[0], burn_rate[0], face_map.reshape(8, 128))
    return fields[None], head[None]


def solution(mesh):
    placed = (P("grp", None, "mesh", None), P("grp", "mesh", None), P("grp", "mesh", None))
    return jax.shard_map(
        shards,
        mesh=mesh,
        in_specs=placed,
        out_specs=(P("grp", None, "mesh", None), P("grp", "mesh", None)),
        check_vma=False,
    )
```

```python
import math

import jax
import jax.numpy as jnp
import numpy as np
from jax import lax
from jax.experimental import pallas as pl
from jax.experimental.pallas import tpu as pltpu
from jax.sharding import PartitionSpec as P

NX = 64
NY = 64
CZ = 16
FIELDS = 5
SECTIONS = 2
ITERS = 3
COURANT = 0.1
DIFFUSION = 0.05
STOICHIOMETRY = 2.0
EXPANSION = 1.0

PLANE = 32
LEVEL = FIELDS * PLANE
HALO = 2
MESH = pl.DeviceIdType.MESH
F32 = jnp.float32
BF16 = jnp.bfloat16


def sine(n):
    i = np.arange(n, dtype=np.float64) + 1.0
    return np.sin(np.pi * i[:, None] * i[None, :] / (n + 1)) * math.sqrt(2.0 / (n + 1))


def eigen(n):
    i = np.arange(n, dtype=np.float64) + 1.0
    return 2.0 - 2.0 * np.cos(np.pi * i / (n + 1))


T_IM = 0
T_Z1 = 512
T_Z2 = 576
T_W = 640
T_GAMMA = 664
T_ALPHA = 672
T_SX = 736
T_SX2 = 864
T_ROWS = 992
B_Y = 0
B_XF = 128
B_XI = 192
B_ROWS = 256


def tables():
    s16, s64 = sine(CZ), sine(NX)
    tab = np.zeros((T_ROWS, 128))
    modes = eigen(CZ)[:, None, None] + eigen(NX)[None, :, None] + eigen(NY)[None, None, :]
    inv = 1.0 / modes
    tab[T_IM : T_IM + 512] = (
        inv.reshape(8, 2, 64, 64).transpose(0, 2, 1, 3).reshape(512, 128)
    )
    for p in range(8):
        for h in range(2):
            lanes = slice(64 * h, 64 * h + 64)
            for r in range(8):
                tab[T_Z1 + p * 8 + r, lanes] = s16[2 * p + h, 2 * r + h]
                tab[T_Z2 + p * 8 + r, lanes] = s16[2 * p + 1 - h, 2 * r + h]
            for k in range(3):
                tab[T_W + 8 * k + p, lanes] = s16[2 * p + h, k]
    for at, places in ((T_SX, (63, 0)), (T_SX2, (62, 1))):
        for side, place in enumerate(places):
            tab[at + 64 * side : at + 64 * side + 64] = s64[:, place][:, None]
    packed = tab[T_IM : T_IM + 512].reshape(8, 64, 128)
    tab[T_ALPHA : T_ALPHA + 64] = (packed * tab[T_W : T_W + 8, None, :] ** 2).sum(0)
    tab[T_GAMMA : T_GAMMA + 8] = (packed * tab[None, T_SX : T_SX + 64] ** 2).sum(1)
    mat = np.zeros((B_ROWS, 128))
    mat[B_Y : B_Y + 128] = np.kron(np.eye(2), s64)
    order = np.concatenate([np.arange(0, 64, 2), np.arange(1, 64, 2)])
    mat[B_XF : B_XF + 64, :64] = s64[:, order]
    mat[B_XI : B_XI + 64, :64] = s64[order, :]
    mat = mat.astype(np.float32)
    high = mat.astype(jnp.bfloat16)
    low = (mat - high.astype(np.float32)).astype(jnp.bfloat16)
    return tab.astype(np.float32), high, low


S16 = sine(CZ)


def split(v):
    high = v.astype(BF16)
    return high, (v - high.astype(F32)).astype(BF16)


def dot(a, b):
    return jnp.dot(a, b, preferred_element_type=F32)


def dot_right(v, th, tl):
    vh, vl = split(v)
    return dot(vh, th) + (dot(vl, th) + dot(vh, tl))


def dot_left(th, tl, v):
    vh, vl = split(v)
    return dot(th, vh) + (dot(th, vl) + dot(tl, vh))


def kernel(
    state, burn, fmap, tab_h, bh_h, bl_h, out_s, out_p,
    stn, bnn, fld0, fld1, fields, burning, src, ybuf, hat1, hat, prs, resp,
    edge, xg, zsend, zrecv, psend, qsend, qrecv, fsend, frecv, psel, tab, bh, bl, idx,
    in_sem, t_sem, send_sem, recv_sem,
):
    g = lax.axis_index("grp")
    m = lax.axis_index("mesh")
    n = lax.axis_size("mesh")
    fine = g == 0
    LOW, HIGH, PARTNER, LOW2, HIGH2, DLOW, DHIGH = range(7)
    back = (HIGH, LOW, PARTNER, HIGH2, LOW2, DHIGH, DLOW)
    has_low, has_high = m > 0, m < n - 1
    exists = (has_low, has_high, None, m > 1, m < n - 2, has_low, has_high)
    steps = (-1, 1, 0, -2, 2, -1, 1)
    where_to = [
        {"grp": 1 - g if to in (PARTNER, DLOW, DHIGH) else g, "mesh": lax.rem(m + n + steps[to], n)}
        for to in range(7)
    ]
    count = 1
    for to in range(7):
        if exists[to] is not None:
            count = count + exists[to].astype(jnp.int32)

    def guarded(condition, action):
        if condition is None:
            action()
        else:
            pl.when(condition)(action)

    loads = [
        pltpu.make_async_copy(state.at[f], stn.at[f], in_sem.at[f]) for f in range(FIELDS)
    ]
    loads.append(pltpu.make_async_copy(burn, bnn, in_sem.at[FIELDS]))
    for copy in loads:
        copy.start()
    table_loads = [
        pltpu.make_async_copy(a, b, t_sem.at[i])
        for i, (a, b) in enumerate(((fmap, idx.at[0]), (tab_h, tab), (bh_h, bh), (bl_h, bl)))
    ]
    for copy in table_loads:
        copy.start()

    def clear(ref, start, size):
        ref[start : start + size, :] = jnp.zeros((size, 128), F32)

    @pl.when(jnp.logical_not(has_low))
    def _():
        clear(fld0, 0, 2 * LEVEL)
        clear(fld1, 0, 2 * LEVEL)
        for s in range(SECTIONS):
            clear(prs.at[s], 0, 3 * PLANE)
            for part in (1, 4):
                clear(zrecv.at[s, part], 0, PLANE + 8)
            clear(qrecv.at[s, 1], 0, 8)

    @pl.when(jnp.logical_not(has_high))
    def _():
        clear(fld0, (CZ + 2) * LEVEL, 2 * LEVEL)
        clear(fld1, (CZ + 2) * LEVEL, 2 * LEVEL)
        for s in range(SECTIONS):
            clear(prs.at[s], (CZ + 3) * PLANE, 3 * PLANE)
            for part in (0, 5):
                clear(zrecv.at[s, part], 0, PLANE + 8)
            clear(qrecv.at[s, 2], 0, 8)

    @pl.when(m < 2)
    def _():
        for s in range(SECTIONS):
            clear(zrecv.at[s, 3], 0, PLANE + 8)

    @pl.when(m > n - 3)
    def _():
        for s in range(SECTIONS):
            clear(zrecv.at[s, 2], 0, PLANE + 8)

    barrier = pltpu.get_barrier_semaphore()
    for to in range(7):
        guarded(
            exists[to],
            lambda to=to: pl.semaphore_signal(
                barrier, inc=1, device_id=where_to[to], device_id_type=MESH
            ),
        )
    pl.semaphore_wait(barrier, count)

    messages = []

    class Message:
        def __init__(self, to, a, b):
            slot = len(messages)
            messages.append(self)
            self.to = to
            self.copy = pltpu.make_async_remote_copy(
                src_ref=a, dst_ref=b, send_sem=send_sem.at[slot], recv_sem=recv_sem.at[slot],
                device_id=where_to[to], device_id_type=MESH,
            )
            self.sent = False

        def start(self):
            guarded(exists[self.to], self.copy.start)

        def wait_recv(self):
            guarded(exists[back[self.to]], self.copy.wait_recv)

        def wait_send(self):
            if not self.sent:
                self.sent = True
                guarded(exists[self.to], self.copy.wait_send)

    lane = lax.broadcasted_iota(jnp.int32, (PLANE, 128), 1)
    row = lax.broadcasted_iota(jnp.int32, (PLANE, 128), 0)
    half0 = lane < 64
    y_last = (lane == 63) | (lane == 127)
    y_first = (lane == 0) | (lane == 64)
    x_last = (row == PLANE - 1) & (lane >= 64)
    x_first = (row == 0) & half0
    half8 = lax.broadcasted_iota(jnp.int32, (8, 128), 1) < 64
    half64 = lax.broadcasted_iota(jnp.int32, (64, 128), 1) < 64
    sub8 = lax.broadcasted_iota(jnp.int32, (8, 128), 0)

    def swap(v):
        return pltpu.roll(v, 64, 1)

    def rows(start, size):
        return pl.ds(pl.multiple_of(start, 8), size)

    def level(k, f):
        return ((k + HALO) * FIELDS + f) * PLANE

    def to_layers(load, store):
        for b in range(2):
            @pl.loop(0, 4)
            def _(t):
                tiles = jnp.stack(
                    [
                        load(b, pl.ds(pl.multiple_of((t * 8 + i) * 128, 128), 128))
                        for i in range(8)
                    ]
                )
                turned = jnp.swapaxes(tiles, 0, 1)
                for i in range(8):
                    store(b * 8 + i, t * 8, turned[i])

    def to_native(load, store):
        for b in range(2):
            @pl.loop(0, 4)
            def _(t):
                tiles = jnp.stack([load(b * 8 + i, t * 8) for i in range(8)])
                turned = jnp.swapaxes(tiles, 0, 1)
                for i in range(8):
                    store(b, pl.ds(pl.multiple_of((t * 8 + i) * 128, 128), 128), turned[i])

    for f in range(FIELDS):
        loads[f].wait()

        def load_state(b, lanes, f=f):
            return stn[f, b * 8 : b * 8 + 8, lanes]

        def store_state(k, r, v, f=f):
            fld0[rows(level(k, f) + r, 8), :] = v

        to_layers(load_state, store_state)

    def pack_edges():
        for f in range(FIELDS):
            even = edge[pl.ds(f * 16, 8, stride=2), :]
            odd = edge[pl.ds(f * 16 + 1, 8, stride=2), :]
            own = jnp.where(
                fine, jnp.where(half8, swap(even), odd), jnp.where(half8, even, swap(odd))
            )
            yield f, own

    def send_fields(fld, s):
        copies = [
            Message(LOW, fld.at[pl.ds(level(0, 0), 2 * LEVEL)],
                    fld.at[pl.ds(level(CZ, 0), 2 * LEVEL)]),
            Message(HIGH, fld.at[pl.ds(level(CZ - 2, 0), 2 * LEVEL)],
                    fld.at[pl.ds(level(-2, 0), 2 * LEVEL)]),
            Message(PARTNER, fsend.at[s], frecv.at[s]),
        ]
        copies[0].start()
        copies[1].start()
        at = jnp.where(fine, PLANE - 1, 0)
        for k in range(CZ):
            for f in range(FIELDS):
                edge[pl.ds(f * 16 + k, 1), :] = fld[pl.ds(level(k, f) + at, 1), :]
        for f, own in pack_edges():
            fsend[s, f * 8 : f * 8 + 8, :] = own
        copies[2].start()
        return copies

    def gather(plane, who=0):
        index = idx[who]
        column = index & 127
        block = index >> 7
        out = jnp.zeros((8, 128), F32)
        for r in range(8):
            one = jnp.broadcast_to(plane[r : r + 1, :], (8, 128))
            out = jnp.where(block == r, jnp.take_along_axis(one, column, axis=1), out)
        return out

    def spread(ghost, base):
        other = swap(ghost)
        xg[pl.ds(base, 8, stride=2), :] = jnp.where(half8, ghost, other)
        xg[pl.ds(base + 1, 8, stride=2), :] = jnp.where(half8, other, ghost)

    def x_sides(v, ghost):
        ghost = jnp.broadcast_to(ghost, (PLANE, 128))
        turned = swap(v)
        up = pltpu.roll(turned, PLANE - 1, 0)
        down = pltpu.roll(turned, 1, 0)
        zero = jnp.zeros_like(ghost)
        up = jnp.where(x_last, jnp.where(fine, ghost, zero), up)
        down = jnp.where(x_first, jnp.where(fine, zero, ghost), down)
        return jnp.where(half0, turned, up), jnp.where(half0, down, turned)

    def y_sides(v):
        north = jnp.where(y_last, 0.0, pltpu.roll(v, 127, 1))
        south = jnp.where(y_first, 0.0, pltpu.roll(v, 1, 1))
        return north, south

    XG = 48

    def tendency_plane(fld, k, finish):
        c = [fld[rows(level(k, f), PLANE), :] for f in range(FIELDS)]
        reaction = burning[rows(k * PLANE, PLANE), :] * c[3] * c[4]
        source = EXPANSION * reaction
        for f in range(FIELDS):
            above = fld[rows(level(k + 1, f), PLANE), :]
            below = fld[rows(level(k - 1, f), PLANE), :]
            above2 = fld[rows(level(k + 2, f), PLANE), :]
            below2 = fld[rows(level(k - 2, f), PLANE), :]
            east, west = x_sides(c[f], xg[pl.ds(XG + f * 16 + k, 1), :])
            north, south = y_sides(c[f])
            gx = 0.5 * (east - west)
            gy = 0.5 * (north - south)
            dz = above - below
            gz = (2.0 / 3.0) * dz - (1.0 / 12.0) * (above2 - below2)
            lap = (east + west) + (north + south) + (above + below) - 6.0 * c[f]
            adv = c[0] * gx + c[1] * gy + c[2] * gz
            change = DIFFUSION * lap - COURANT * adv
            if f == 0:
                source = source - gx
            elif f == 1:
                source = source - gy
            elif f == 2:
                source = source - 0.5 * dz
            elif f == 3:
                change = change - reaction
            else:
                change = change - STOICHIOMETRY * reaction
            finish(k, f, c[f], change)
        src[rows(k * PLANE, PLANE), :] = source

    def z_forward(into):
        @pl.loop(0, 4)
        def _(t):
            v = [src[rows(k * PLANE + t * 8, 8), :] for k in range(CZ)]
            even = [v[k] + v[15 - k] for k in range(8)]
            odd = [v[k] - v[15 - k] for k in range(8)]
            for c in range(CZ):
                part = odd if c % 2 else even
                total = part[0] * F32(S16[c, 0])
                for k in range(1, 8):
                    total = total + part[k] * F32(S16[c, k])
                into[rows(c * PLANE + t * 8, 8), :] = total

    def z_inverse(spec, into, base):
        @pl.loop(0, 4)
        def _(t):
            v = [spec[rows(c * PLANE + t * 8, 8), :] for c in range(CZ)]
            for k in range(8):
                even = v[0] * F32(S16[0, k])
                odd = v[1] * F32(S16[1, k])
                for c in range(1, 8):
                    even = even + v[2 * c] * F32(S16[2 * c, k])
                    odd = odd + v[2 * c + 1] * F32(S16[2 * c + 1, k])
                into[rows(base + k * PLANE + t * 8, 8), :] = even + odd
                into[rows(base + (15 - k) * PLANE + t * 8, 8), :] = even - odd

    def y_matrix():
        return bh[B_Y : B_Y + 128, :], bl[B_Y : B_Y + 128, :]

    def y_transform(v):
        return dot_right(v, *y_matrix())

    def x_forward(a, b):
        even = jnp.where(half0, a, swap(b))
        odd = jnp.where(half0, swap(a), b)
        v = jnp.concatenate([even, odd], axis=0)
        return dot_left(bh[B_XF : B_XF + 64, :64], bl[B_XF : B_XF + 64, :64], v)

    def x_inverse(v):
        v = dot_left(bh[B_XI : B_XI + 64, :64], bl[B_XI : B_XI + 64, :64], v)
        even, odd = v[:PLANE], v[PLANE:]
        return jnp.where(half0, even, swap(odd)), jnp.where(half0, swap(even), odd)

    def z_plane(v):
        other = swap(v)
        out = jnp.zeros((8, 128), F32)
        for p in range(8):
            out = out + tab[T_Z1 + p * 8 : T_Z1 + p * 8 + 8, :] * v[p : p + 1, :]
            out = out + tab[T_Z2 + p * 8 : T_Z2 + p * 8 + 8, :] * other[p : p + 1, :]
        return out

    def side_x(at=T_SX):
        return tab[rows(at + g * 64, 64), :]

    def weight(k, p):
        return tab[T_W + 8 * k + p : T_W + 8 * k + p + 1, :]

    def modes(p):
        return tab[T_IM + p * 64 : T_IM + p * 64 + 64, :]

    def block(ref, p):
        return ref[p * 64 : p * 64 + 64, :]

    def first_of(acc):
        return acc + swap(acc)

    def last_of(acc):
        other = swap(acc)
        return jnp.where(half64, acc - other, other - acc)

    def z_layers(spec, k):
        acc = weight(k, 0) * block(spec, 0)
        for p in range(1, 8):
            acc = acc + weight(k, p) * block(spec, p)
        return acc

    def x_planes(spec, at):
        sx = side_x(at)
        return jnp.concatenate(
            [jnp.sum(sx * block(spec, p), axis=0, keepdims=True) for p in range(8)], axis=0
        )

    def narrow(v):
        return jnp.where(half0, v[:PLANE], v[PLANE:])

    def widen(v):
        other = swap(v)
        return jnp.concatenate(
            [jnp.where(half0, v, other), jnp.where(half0, other, v)], axis=0
        )

    def z_ghosts(below, above):
        return below + jnp.where(half64, above, -above)

    def layer_response(both, ghost):
        acc = tab[T_ALPHA : T_ALPHA + 64, :] * both
        for p in range(8):
            acc = acc + resp[rows(g * 512 + p * 64, 64), :] * ghost[p : p + 1, :]
        return acc

    def plane_response(both, ghost):
        side = jnp.concatenate(
            [
                jnp.sum(resp[rows((1 - g) * 512 + p * 64, 64), :] * both, axis=0, keepdims=True)
                for p in range(8)
            ],
            axis=0,
        )
        return side + tab[T_GAMMA : T_GAMMA + 8, :] * ghost

    Z_HIGH, Z_LOW, Z_HIGH2, Z_LOW2, Z_DLOW, Z_DHIGH = range(6)

    def solve(s):
        own = prs.at[s]
        z_forward(ybuf)
        ybuf[...] = y_transform(ybuf[...])
        for p in range(8):
            v = x_forward(
                ybuf[2 * p * PLANE : (2 * p + 1) * PLANE, :],
                ybuf[(2 * p + 1) * PLANE : (2 * p + 2) * PLANE, :],
            )
            hat1[p * 64 : p * 64 + 64, :] = v * modes(p)
        acc = z_layers(hat1, 0)
        first, last = first_of(acc), last_of(acc)
        plane = z_plane(y_transform(x_planes(hat1, T_SX)))
        zsend[s, 0, 0:PLANE, :] = narrow(first)
        zsend[s, 1, 0:PLANE, :] = narrow(last)
        zsend[s, 0, PLANE : PLANE + 8, :] = plane
        zsend[s, 1, PLANE : PLANE + 8, :] = plane

        def layer(side):
            return zsend.at[s, side, pl.ds(0, PLANE)]

        def into(slot):
            return zrecv.at[s, slot, pl.ds(0, PLANE)]

        copies = [
            Message(LOW, layer(0), into(Z_HIGH)),
            Message(HIGH, layer(1), into(Z_LOW)),
            Message(DLOW, zsend.at[s, 0], zrecv.at[s, Z_DHIGH]),
            Message(DHIGH, zsend.at[s, 1], zrecv.at[s, Z_DLOW]),
            Message(LOW2, layer(0), into(Z_HIGH2)),
            Message(HIGH2, layer(1), into(Z_LOW2)),
            Message(PARTNER, zsend.at[s, 0, pl.ds(PLANE, 8)], qrecv.at[s, 3]),
        ]
        for copy in copies:
            copy.start()
        mine = z_plane(gather(plane, 1))
        for copy in copies:
            copy.wait_recv()

        def got(slot):
            return zrecv[s, slot, 0:PLANE, :]

        def got_plane(slot):
            return zrecv[s, slot, PLANE : PLANE + 8, :]

        ghosts = y_transform(
            jnp.concatenate(
                [mine, z_plane(gather(got_plane(Z_DLOW), 2)), z_plane(gather(got_plane(Z_DHIGH), 3))],
                axis=0,
            )
        )
        partner = plane_response(
            z_ghosts(widen(got(Z_DLOW)), widen(got(Z_DHIGH))), ghosts[0:8]
        )
        partner = qrecv[s, 3] + z_plane(y_transform(partner))
        ghost = y_transform(z_plane(gather(partner)))
        above = got(Z_HIGH) + narrow(
            first_of(layer_response(z_ghosts(last, widen(got(Z_HIGH2))), ghosts[16:24]))
        )
        below = got(Z_LOW) + narrow(
            last_of(layer_response(z_ghosts(widen(got(Z_LOW2)), first), ghosts[8:16]))
        )
        above = jnp.where(has_high, above, 0.0)
        below = jnp.where(has_low, below, 0.0)
        both = z_ghosts(widen(below), widen(above))
        sx = side_x()
        for p in range(8):
            extra = weight(0, p) * both + sx * ghost[p : p + 1, :]
            hat[p * 64 : p * 64 + 64, :] = block(hat1, p) + extra * modes(p)
        depth = 3 if s == 0 else 1
        planes = [x_planes(hat, T_SX)]
        if s == 0:
            planes.append(x_planes(hat, T_SX2))
        planes = y_transform(jnp.concatenate(planes, axis=0))
        for i in range(len(planes) // 8):
            qsend[s, i * 8 : i * 8 + 8, :] = z_plane(planes[i * 8 : i * 8 + 8])
        for k in range(depth):
            acc = z_layers(hat, k)
            a, b = x_inverse(jnp.where(half64, first_of(acc), last_of(acc)))
            psend[s, 0, k * PLANE : (k + 1) * PLANE, :] = y_transform(a)
            at = depth - 1 - k
            psend[s, 1, at * PLANE : (at + 1) * PLANE, :] = y_transform(b)
        size = depth * PLANE
        copies = [
            Message(LOW, psend.at[s, 0, pl.ds(0, size)], own.at[pl.ds((CZ + 3) * PLANE, size)]),
            Message(HIGH, psend.at[s, 1, pl.ds(0, size)], own.at[pl.ds((3 - depth) * PLANE, size)]),
        ]
        if s == 0:
            copies += [
                Message(DLOW, qsend.at[s, pl.ds(0, 8)], qrecv.at[s, 2]),
                Message(DHIGH, qsend.at[s, pl.ds(0, 8)], qrecv.at[s, 1]),
                Message(PARTNER, qsend.at[s], psel.at[0]),
            ]
        else:
            copies.append(Message(PARTNER, qsend.at[s, pl.ds(0, 8)], qrecv.at[s, 0]))
        for copy in copies:
            copy.start()
        for p in range(8):
            a, b = x_inverse(block(hat, p))
            ybuf[2 * p * PLANE : (2 * p + 1) * PLANE, :] = a
            ybuf[(2 * p + 1) * PLANE : (2 * p + 2) * PLANE, :] = b
        ybuf[...] = y_transform(ybuf[...])
        z_inverse(ybuf, own, 3 * PLANE)
        for copy in copies:
            copy.wait_recv()
        return copies

    def correct_plane(s, k, into, at_of):
        own = prs.at[s]
        p = own[rows((k + 3) * PLANE, PLANE), :]
        above = own[rows((k + 4) * PLANE, PLANE), :]
        below = own[rows((k + 2) * PLANE, PLANE), :]
        east, west = x_sides(p, xg[pl.ds(16 + k, 1), :])
        north, south = y_sides(p)
        for f, (a, b) in enumerate(((east, west), (north, south), (above, below))):
            at = rows(at_of(k, f), PLANE)
            into[at, :] = into[at, :] - 0.5 * (a - b)

    table_loads[0].wait()
    early = send_fields(fld0, 0)
    maps = [
        Message(PARTNER, idx.at[0], idx.at[1]),
        Message(HIGH, idx.at[0], idx.at[2]),
        Message(LOW, idx.at[0], idx.at[3]),
    ]
    for copy in maps:
        copy.start()
    loads[FIELDS].wait()

    def load_burn(b, lanes):
        return bnn[b * 8 : b * 8 + 8, lanes]

    def store_burn(k, r, v):
        burning[rows(k * PLANE + r, 8), :] = v

    to_layers(load_burn, store_burn)
    for copy in table_loads[1:]:
        copy.wait()
    for side in range(2):
        sx = tab[T_SX + side * 64 : T_SX + side * 64 + 64, :]
        for p in range(8):
            start = side * 512 + p * 64
            resp[start : start + 64, :] = modes(p) * weight(0, p) * sx

    def finish0(k, f, c, change):
        fld1[rows(level(k, f), PLANE), :] = c + change

    early[2].wait_recv()
    for f in range(FIELDS):
        spread(gather(frecv[0, f * 8 : f * 8 + 8, :]), XG + f * 16)

    @pl.loop(2, CZ - 2)
    def _(k):
        tendency_plane(fld0, k, finish0)

    early[0].wait_recv()
    early[1].wait_recv()

    @pl.loop(0, 4)
    def _(i):
        tendency_plane(fld0, i + (CZ - 4) * (i // 2), finish0)

    early = send_fields(fld1, 1)
    for copy in maps:
        copy.wait_recv()
    solve(0)

    near = psel[0, 0:8, :]
    beside = psel[0, 8:16, :]
    spread(gather(near), 16)
    spread(gather(qrecv[0, 1], 2), 0)
    spread(gather(qrecv[0, 2], 3), 32)
    for copy in early:
        copy.wait_recv()
    for copy in early:
        copy.wait_send()
    sides = gather(qsend[0, 0:8, :], 1)
    sign = jnp.where(fine, -0.5, 0.5)
    new0 = frecv[1, 0:8, :] - sign * (sides - beside)
    lane8 = lax.broadcasted_iota(jnp.int32, (8, 128), 1)
    north = jnp.where((lane8 == 63) | (lane8 == 127), 0.0, pltpu.roll(near, 127, 1))
    south = jnp.where((lane8 == 0) | (lane8 == 64), 0.0, pltpu.roll(near, 1, 1))
    new1 = frecv[1, 8:16, :] - 0.5 * (north - south)
    other = swap(near)
    up = pltpu.roll(other, 7, 0)
    down = pltpu.roll(other, 1, 0)
    over = jnp.broadcast_to(swap(qrecv[0, 2])[0:1, :], (8, 128))
    under = jnp.broadcast_to(swap(qrecv[0, 1])[7:8, :], (8, 128))
    above = jnp.where(half8, other, jnp.where(sub8 == 7, over, up))
    below = jnp.where(half8, jnp.where(sub8 == 0, under, down), other)
    new2 = frecv[1, 16:24, :] - 0.5 * (above - below)
    for f, v in enumerate((new0, new1, new2, frecv[1, 24:32, :], frecv[1, 32:40, :])):
        spread(gather(v), XG + f * 16)

    @pl.loop(0, CZ)
    def _(k):
        correct_plane(0, k, fld1, level)

    @pl.when(has_low)
    def _():
        @pl.loop(-2, 0)
        def _(k):
            correct_plane(0, k, fld1, level)

    @pl.when(has_high)
    def _():
        @pl.loop(CZ, CZ + 2)
        def _(k):
            correct_plane(0, k, fld1, level)

    def finish1(k, f, c, change):
        start = fld0[rows(level(k, f), PLANE), :]
        fields[rows((k * FIELDS + f) * PLANE, PLANE), :] = 0.5 * (start + c + change)

    @pl.loop(0, CZ)
    def _(k):
        tendency_plane(fld1, k, finish1)

    solve(1)
    spread(gather(qrecv[1, 0]), 16)

    @pl.loop(0, CZ)
    def _(k):
        correct_plane(1, k, fields, lambda k, f: (k * FIELDS + f) * PLANE)

    for f in range(FIELDS):
        def load_field(k, r, f=f):
            return fields[rows((k * FIELDS + f) * PLANE + r, 8), :]

        def store_field(b, lanes, v, f=f):
            out_s[f, b * 8 : b * 8 + 8, lanes] = v

        to_native(load_field, store_field)

    def store_head(b, lanes, v):
        out_p[b * 8 : b * 8 + 8, lanes] = v

    to_native(lambda k, r: prs[1, rows((k + 3) * PLANE + r, 8), :], store_head)
    for copy in messages:
        copy.wait_send()


def step(state, burn, fmap):
    hbm = pl.BlockSpec(memory_space=pltpu.HBM)
    vmem = pl.BlockSpec(memory_space=pltpu.VMEM)
    tab, bh, bl = tables()
    vm = pltpu.VMEM
    layers = (CZ + 2 * HALO) * LEVEL
    return pl.pallas_call(
        kernel,
        out_shape=(
            jax.ShapeDtypeStruct((FIELDS, CZ, NX * NY), F32),
            jax.ShapeDtypeStruct((CZ, NX * NY), F32),
        ),
        in_specs=[hbm] * 6,
        out_specs=(vmem, vmem),
        scratch_shapes=[
            vm((FIELDS, CZ, NX * NY), F32),
            vm((CZ, NX * NY), F32),
            vm((layers, 128), F32),
            vm((layers, 128), F32),
            vm((CZ * LEVEL, 128), F32),
            vm((CZ * PLANE, 128), F32),
            vm((CZ * PLANE, 128), F32),
            vm((CZ * PLANE, 128), F32),
            vm((CZ * PLANE, 128), F32),
            vm((CZ * PLANE, 128), F32),
            vm((SECTIONS, (CZ + 6) * PLANE, 128), F32),
            vm((1024, 128), F32),
            vm((FIELDS * 16, 128), F32),
            vm((48 + FIELDS * 16, 128), F32),
            vm((SECTIONS, 2, PLANE + 8, 128), F32),
            vm((SECTIONS, 6, PLANE + 8, 128), F32),
            vm((SECTIONS, 2, 3 * PLANE, 128), F32),
            vm((SECTIONS, 16, 128), F32),
            vm((SECTIONS, 4, 8, 128), F32),
            vm((SECTIONS, FIELDS * 8, 128), F32),
            vm((SECTIONS, FIELDS * 8, 128), F32),
            vm((1, 16, 128), F32),
            vm((T_ROWS, 128), F32),
            vm((B_ROWS, 128), BF16),
            vm((B_ROWS, 128), BF16),
            vm((4, 8, 128), jnp.int32),
            pltpu.SemaphoreType.DMA((FIELDS + 1,)),
            pltpu.SemaphoreType.DMA((4,)),
            pltpu.SemaphoreType.DMA((40,)),
            pltpu.SemaphoreType.DMA((40,)),
        ],
        compiler_params=pltpu.CompilerParams(
            collective_id=0, has_side_effects=True, vmem_limit_bytes=40 << 20
        ),
        name="fire_step",
    )(*[pltpu.with_memory_space_constraint(v, pltpu.HBM) for v in (state, burn, fmap, jnp.asarray(tab), jnp.asarray(bh), jnp.asarray(bl))])


def shards(state, burn_rate, face_map):
    fields, head = step(state[0], burn_rate[0], face_map.reshape(8, 128))
    return fields[None], head[None]


def solution(mesh):
    placed = (P("grp", None, "mesh", None), P("grp", "mesh", None), P("grp", "mesh", None))
    return jax.shard_map(
        shards,
        mesh=mesh,
        in_specs=placed,
        out_specs=(P("grp", None, "mesh", None), P("grp", "mesh", None)),
        check_vma=False,
    )
```

```python
import math

import jax
import jax.numpy as jnp
import numpy as np
from jax import lax
from jax.experimental import pallas as pl
from jax.experimental.pallas import tpu as pltpu
from jax.sharding import PartitionSpec as P

NX = 64
NY = 64
CZ = 16
FIELDS = 5
SECTIONS = 2
ITERS = 3
COURANT = 0.1
DIFFUSION = 0.05
STOICHIOMETRY = 2.0
EXPANSION = 1.0

PLANE = 32
LEVEL = FIELDS * PLANE
HALO = 2
MESH = pl.DeviceIdType.MESH
F32 = jnp.float32
BF16 = jnp.bfloat16


def sine(n):
    i = np.arange(n, dtype=np.float64) + 1.0
    return np.sin(np.pi * i[:, None] * i[None, :] / (n + 1)) * math.sqrt(2.0 / (n + 1))


def eigen(n):
    i = np.arange(n, dtype=np.float64) + 1.0
    return 2.0 - 2.0 * np.cos(np.pi * i / (n + 1))


T_IM = 0
T_Z1 = 512
T_Z2 = 576
T_W = 640
T_GAMMA = 664
T_ALPHA = 672
T_SX = 736
T_SX2 = 864
T_ROWS = 992
B_Y = 0
B_XF = 128
B_XI = 192
B_ROWS = 256


def tables():
    s16, s64 = sine(CZ), sine(NX)
    tab = np.zeros((T_ROWS, 128))
    modes = eigen(CZ)[:, None, None] + eigen(NX)[None, :, None] + eigen(NY)[None, None, :]
    inv = 1.0 / modes
    tab[T_IM : T_IM + 512] = (
        inv.reshape(8, 2, 64, 64).transpose(0, 2, 1, 3).reshape(512, 128)
    )
    for p in range(8):
        for h in range(2):
            lanes = slice(64 * h, 64 * h + 64)
            for r in range(8):
                tab[T_Z1 + p * 8 + r, lanes] = s16[2 * p + h, 2 * r + h]
                tab[T_Z2 + p * 8 + r, lanes] = s16[2 * p + 1 - h, 2 * r + h]
            for k in range(3):
                tab[T_W + 8 * k + p, lanes] = s16[2 * p + h, k]
    for at, places in ((T_SX, (63, 0)), (T_SX2, (62, 1))):
        for side, place in enumerate(places):
            tab[at + 64 * side : at + 64 * side + 64] = s64[:, place][:, None]
    packed = tab[T_IM : T_IM + 512].reshape(8, 64, 128)
    tab[T_ALPHA : T_ALPHA + 64] = (packed * tab[T_W : T_W + 8, None, :] ** 2).sum(0)
    tab[T_GAMMA : T_GAMMA + 8] = (packed * tab[None, T_SX : T_SX + 64] ** 2).sum(1)
    mat = np.zeros((B_ROWS, 128))
    mat[B_Y : B_Y + 128] = np.kron(np.eye(2), s64)
    order = np.concatenate([np.arange(0, 64, 2), np.arange(1, 64, 2)])
    mat[B_XF : B_XF + 64, :64] = s64[:, order]
    mat[B_XI : B_XI + 64, :64] = s64[order, :]
    mat = mat.astype(np.float32)
    high = mat.astype(jnp.bfloat16)
    low = (mat - high.astype(np.float32)).astype(jnp.bfloat16)
    return tab.astype(np.float32), high, low


S16 = sine(CZ)


def split(v):
    high = v.astype(BF16)
    return high, (v - high.astype(F32)).astype(BF16)


def dot(a, b):
    return jnp.dot(a, b, preferred_element_type=F32)


def dot_right(v, th, tl):
    vh, vl = split(v)
    return dot(vh, th) + (dot(vl, th) + dot(vh, tl))


def dot_left(th, tl, v):
    vh, vl = split(v)
    return dot(th, vh) + (dot(th, vl) + dot(tl, vh))


def kernel(
    state, burn, fmap, tab_h, bh_h, bl_h, out_s, out_p,
    stn, bnn, fld0, fld1, fields, burning, src, ybuf, hat1, hat, prs, resp,
    turns, xg, zsend, zrecv, psend, qsend, qrecv, fsend, frecv, psel, tab, bh, bl, idx,
    in_sem, t_sem, send_sem, recv_sem,
):
    g = lax.axis_index("grp")
    m = lax.axis_index("mesh")
    n = lax.axis_size("mesh")
    fine = g == 0
    LOW, HIGH, PARTNER, LOW2, HIGH2, DLOW, DHIGH = range(7)
    back = (HIGH, LOW, PARTNER, HIGH2, LOW2, DHIGH, DLOW)
    has_low, has_high = m > 0, m < n - 1
    exists = (has_low, has_high, None, m > 1, m < n - 2, has_low, has_high)
    steps = (-1, 1, 0, -2, 2, -1, 1)
    where_to = [
        {"grp": 1 - g if to in (PARTNER, DLOW, DHIGH) else g, "mesh": lax.rem(m + n + steps[to], n)}
        for to in range(7)
    ]
    count = 1
    for to in range(7):
        if exists[to] is not None:
            count = count + exists[to].astype(jnp.int32)

    def guarded(condition, action):
        if condition is None:
            action()
        else:
            pl.when(condition)(action)

    loads = [
        pltpu.make_async_copy(state.at[f], stn.at[f], in_sem.at[f]) for f in range(FIELDS)
    ]
    loads.append(pltpu.make_async_copy(burn, bnn, in_sem.at[FIELDS]))
    for copy in loads:
        copy.start()
    table_loads = [
        pltpu.make_async_copy(a, b, t_sem.at[i])
        for i, (a, b) in enumerate(((fmap, idx.at[0]), (tab_h, tab), (bh_h, bh), (bl_h, bl)))
    ]
    for copy in table_loads:
        copy.start()

    def clear(ref, start, size):
        ref[start : start + size, :] = jnp.zeros((size, 128), F32)

    @pl.when(jnp.logical_not(has_low))
    def _():
        clear(fld0, 0, 2 * LEVEL)
        clear(fld1, 0, 2 * LEVEL)
        for s in range(SECTIONS):
            clear(prs.at[s], 0, 3 * PLANE)
            for part in (1, 4):
                clear(zrecv.at[s, part], 0, PLANE + 8)
            clear(qrecv.at[s, 1], 0, 8)

    @pl.when(jnp.logical_not(has_high))
    def _():
        clear(fld0, (CZ + 2) * LEVEL, 2 * LEVEL)
        clear(fld1, (CZ + 2) * LEVEL, 2 * LEVEL)
        for s in range(SECTIONS):
            clear(prs.at[s], (CZ + 3) * PLANE, 3 * PLANE)
            for part in (0, 5):
                clear(zrecv.at[s, part], 0, PLANE + 8)
            clear(qrecv.at[s, 2], 0, 8)

    @pl.when(m < 2)
    def _():
        for s in range(SECTIONS):
            clear(zrecv.at[s, 3], 0, PLANE + 8)

    @pl.when(m > n - 3)
    def _():
        for s in range(SECTIONS):
            clear(zrecv.at[s, 2], 0, PLANE + 8)

    barrier = pltpu.get_barrier_semaphore()
    for to in range(7):
        guarded(
            exists[to],
            lambda to=to: pl.semaphore_signal(
                barrier, inc=1, device_id=where_to[to], device_id_type=MESH
            ),
        )

    messages = []

    class Message:
        def __init__(self, to, a, b):
            slot = len(messages)
            messages.append(self)
            self.to = to
            self.copy = pltpu.make_async_remote_copy(
                src_ref=a, dst_ref=b, send_sem=send_sem.at[slot], recv_sem=recv_sem.at[slot],
                device_id=where_to[to], device_id_type=MESH,
            )
            self.sent = False

        def start(self):
            guarded(exists[self.to], self.copy.start)

        def wait_recv(self):
            guarded(exists[back[self.to]], self.copy.wait_recv)

        def wait_send(self):
            if not self.sent:
                self.sent = True
                guarded(exists[self.to], self.copy.wait_send)

    lane = lax.broadcasted_iota(jnp.int32, (PLANE, 128), 1)
    half0 = lane < 64
    y_last = (lane == 63) | (lane == 127)
    y_first = (lane == 0) | (lane == 64)
    half8 = lax.broadcasted_iota(jnp.int32, (8, 128), 1) < 64
    half64 = lax.broadcasted_iota(jnp.int32, (64, 128), 1) < 64
    sub8 = lax.broadcasted_iota(jnp.int32, (8, 128), 0)

    def swap(v):
        return pltpu.roll(v, 64, 1)

    def rows(start, size):
        return pl.ds(pl.multiple_of(start, 8), size)

    def level(k, f):
        return ((k + HALO) * FIELDS + f) * PLANE

    def to_layers(load, store):
        for b in range(2):
            @pl.loop(0, 4)
            def _(t):
                tiles = jnp.stack(
                    [
                        load(b, pl.ds(pl.multiple_of((t * 8 + i) * 128, 128), 128))
                        for i in range(8)
                    ]
                )
                turned = jnp.swapaxes(tiles, 0, 1)
                for i in range(8):
                    store(b * 8 + i, t * 8, turned[i])

    def to_native(load, store):
        for b in range(2):
            @pl.loop(0, 4)
            def _(t):
                tiles = jnp.stack([load(b * 8 + i, t * 8) for i in range(8)])
                turned = jnp.swapaxes(tiles, 0, 1)
                for i in range(8):
                    store(b, pl.ds(pl.multiple_of((t * 8 + i) * 128, 128), 128), turned[i])

    for f in range(FIELDS):
        loads[f].wait()

        def load_state(b, lanes, f=f):
            return stn[f, b * 8 : b * 8 + 8, lanes]

        def store_state(k, r, v, f=f):
            fld0[rows(level(k, f) + r, 8), :] = v

        to_layers(load_state, store_state)

    def own_plane(fld, f):
        at = jnp.where(fine, PLANE - 1, 0)
        tiles = []
        for odd in range(2):
            tile = jnp.zeros((8, 128), F32)
            for r in range(8):
                one = fld[pl.ds(level(2 * r + odd, f) + at, 1), :]
                tile = jnp.where(sub8 == r, jnp.broadcast_to(one, (8, 128)), tile)
            tiles.append(tile)
        even, odd = tiles
        return jnp.where(
            fine, jnp.where(half8, swap(even), odd), jnp.where(half8, even, swap(odd))
        )

    def field_messages(fld, s):
        return [
            Message(LOW, fld.at[pl.ds(level(0, 0), 2 * LEVEL)],
                    fld.at[pl.ds(level(CZ, 0), 2 * LEVEL)]),
            Message(HIGH, fld.at[pl.ds(level(CZ - 2, 0), 2 * LEVEL)],
                    fld.at[pl.ds(level(-2, 0), 2 * LEVEL)]),
            Message(PARTNER, fsend.at[s], frecv.at[s]),
        ]

    def send_fields(fld, s):
        copies = field_messages(fld, s)
        copies[0].start()
        copies[1].start()
        for f in range(FIELDS):
            fsend[s, f * 8 : f * 8 + 8, :] = own_plane(fld, f)
        copies[2].start()
        return copies

    def gather(plane, who=0):
        index = idx[who]
        column = index & 127
        block = index >> 7
        out = jnp.zeros((8, 128), F32)
        for r in range(8):
            one = jnp.broadcast_to(plane[r : r + 1, :], (8, 128))
            out = jnp.where(block == r, jnp.take_along_axis(one, column, axis=1), out)
        return out

    def spread(ghost, base):
        other = swap(ghost)
        even = jnp.where(half8, ghost, other)
        odd = jnp.where(half8, other, ghost)
        zero = jnp.zeros_like(ghost)
        for side in range(2):
            on = fine if side else jnp.logical_not(fine)
            xg[side, pl.ds(base, 8, stride=2), :] = jnp.where(on, even, zero)
            xg[side, pl.ds(base + 1, 8, stride=2), :] = jnp.where(on, odd, zero)

    def x_sides(v, at, slot):
        base = slot * 48
        turned = swap(v)
        turns[base + 8 : base + 40, :] = turned
        turns[base + 7 : base + 8, :] = xg[0, pl.ds(at, 1), :]
        turns[base + 40 : base + 41, :] = xg[1, pl.ds(at, 1), :]
        down = turns[base + 7 : base + 39, :]
        up = turns[base + 9 : base + 41, :]
        return turned, jnp.where(half0, down, up)

    def y_sides(v):
        north = jnp.where(y_last, 0.0, pltpu.roll(v, 127, 1))
        south = jnp.where(y_first, 0.0, pltpu.roll(v, 1, 1))
        return north, south

    XG = 48
    TAIL = XG + FIELDS * 16

    def tendency_plane(fld, k, finish):
        c = [fld[rows(level(k, f), PLANE), :] for f in range(FIELDS)]
        reaction = burning[rows(k * PLANE, PLANE), :] * c[3] * c[4]
        source = EXPANSION * reaction
        half = jnp.where(half0, 0.5, -0.5)
        cx = c[0] * (half * -COURANT)
        cy = c[1] * (-0.5 * COURANT)
        cz = c[2] * (-COURANT * 2.0 / 3.0)
        cz2 = c[2] * (COURANT / 12.0)
        for f in range(FIELDS):
            above = fld[rows(level(k + 1, f), PLANE), :]
            below = fld[rows(level(k - 1, f), PLANE), :]
            above2 = fld[rows(level(k + 2, f), PLANE), :]
            below2 = fld[rows(level(k - 2, f), PLANE), :]
            inner, outer = x_sides(c[f], XG + f * 16 + k, f)
            north, south = y_sides(c[f])
            dx = inner - outer
            dy = north - south
            dz = above - below
            total = (inner + outer) + (north + south) + (above + below)
            change = (DIFFUSION * total + cx * dx) + (cy * dy + cz * dz) + cz2 * (above2 - below2)
            if f == 0:
                source = source - half * dx
            elif f == 1:
                source = source - 0.5 * dy
            elif f == 2:
                source = source - 0.5 * dz
            elif f == 3:
                change = change - reaction
            else:
                change = change - STOICHIOMETRY * reaction
            finish(k, f, c[f] * (1.0 - 6.0 * DIFFUSION) + change)
        src[rows(k * PLANE, PLANE), :] = source

    def z_forward(into):
        @pl.loop(0, 4)
        def _(t):
            v = [src[rows(k * PLANE + t * 8, 8), :] for k in range(CZ)]
            even = [v[k] + v[15 - k] for k in range(8)]
            odd = [v[k] - v[15 - k] for k in range(8)]
            for c in range(CZ):
                part = odd if c % 2 else even
                total = part[0] * F32(S16[c, 0])
                for k in range(1, 8):
                    total = total + part[k] * F32(S16[c, k])
                into[rows(c * PLANE + t * 8, 8), :] = total

    def z_inverse(spec, into, base):
        @pl.loop(0, 4)
        def _(t):
            v = [spec[rows(c * PLANE + t * 8, 8), :] for c in range(CZ)]
            for k in range(8):
                even = v[0] * F32(S16[0, k])
                odd = v[1] * F32(S16[1, k])
                for c in range(1, 8):
                    even = even + v[2 * c] * F32(S16[2 * c, k])
                    odd = odd + v[2 * c + 1] * F32(S16[2 * c + 1, k])
                into[rows(base + k * PLANE + t * 8, 8), :] = even + odd
                into[rows(base + (15 - k) * PLANE + t * 8, 8), :] = even - odd

    def y_matrix():
        return bh[B_Y : B_Y + 128, :], bl[B_Y : B_Y + 128, :]

    def y_transform(v):
        return dot_right(v, *y_matrix())

    def x_forward(a, b):
        even = jnp.where(half0, a, swap(b))
        odd = jnp.where(half0, swap(a), b)
        v = jnp.concatenate([even, odd], axis=0)
        return dot_left(bh[B_XF : B_XF + 64, :64], bl[B_XF : B_XF + 64, :64], v)

    def x_inverse(v):
        v = dot_left(bh[B_XI : B_XI + 64, :64], bl[B_XI : B_XI + 64, :64], v)
        even, odd = v[:PLANE], v[PLANE:]
        return jnp.where(half0, even, swap(odd)), jnp.where(half0, swap(even), odd)

    def z_plane(v):
        other = swap(v)
        out = jnp.zeros((8, 128), F32)
        for p in range(8):
            out = out + tab[T_Z1 + p * 8 : T_Z1 + p * 8 + 8, :] * v[p : p + 1, :]
            out = out + tab[T_Z2 + p * 8 : T_Z2 + p * 8 + 8, :] * other[p : p + 1, :]
        return out

    def side_x(at=T_SX):
        return tab[rows(at + g * 64, 64), :]

    def weight(k, p):
        return tab[T_W + 8 * k + p : T_W + 8 * k + p + 1, :]

    def modes(p):
        return tab[T_IM + p * 64 : T_IM + p * 64 + 64, :]

    def block(ref, p):
        return ref[p * 64 : p * 64 + 64, :]

    def first_of(acc):
        return acc + swap(acc)

    def last_of(acc):
        other = swap(acc)
        return jnp.where(half64, acc - other, other - acc)

    def z_layers(spec, k):
        acc = weight(k, 0) * block(spec, 0)
        for p in range(1, 8):
            acc = acc + weight(k, p) * block(spec, p)
        return acc

    def x_planes(spec, at):
        sx = side_x(at)
        return jnp.concatenate(
            [jnp.sum(sx * block(spec, p), axis=0, keepdims=True) for p in range(8)], axis=0
        )

    def narrow(v):
        return jnp.where(half0, v[:PLANE], v[PLANE:])

    def widen(v):
        other = swap(v)
        return jnp.concatenate(
            [jnp.where(half0, v, other), jnp.where(half0, other, v)], axis=0
        )

    def z_ghosts(below, above):
        return below + jnp.where(half64, above, -above)

    def layer_response(both, ghost):
        acc = tab[T_ALPHA : T_ALPHA + 64, :] * both
        for p in range(8):
            acc = acc + resp[rows(g * 512 + p * 64, 64), :] * ghost[p : p + 1, :]
        return acc

    def plane_response(both, ghost):
        side = jnp.concatenate(
            [
                jnp.sum(resp[rows((1 - g) * 512 + p * 64, 64), :] * both, axis=0, keepdims=True)
                for p in range(8)
            ],
            axis=0,
        )
        return side + tab[T_GAMMA : T_GAMMA + 8, :] * ghost

    Z_HIGH, Z_LOW, Z_HIGH2, Z_LOW2, Z_DLOW, Z_DHIGH = range(6)

    def solve(s):
        own = prs.at[s]
        z_forward(ybuf)
        ybuf[...] = y_transform(ybuf[...])
        for p in range(8):
            v = x_forward(
                ybuf[2 * p * PLANE : (2 * p + 1) * PLANE, :],
                ybuf[(2 * p + 1) * PLANE : (2 * p + 2) * PLANE, :],
            )
            hat1[p * 64 : p * 64 + 64, :] = v * modes(p)
        acc = z_layers(hat1, 0)
        first, last = first_of(acc), last_of(acc)
        plane = z_plane(y_transform(x_planes(hat1, T_SX)))
        zsend[s, 0, 0:PLANE, :] = narrow(first)
        zsend[s, 1, 0:PLANE, :] = narrow(last)
        zsend[s, 0, PLANE : PLANE + 8, :] = plane
        zsend[s, 1, PLANE : PLANE + 8, :] = plane

        def layer(side):
            return zsend.at[s, side, pl.ds(0, PLANE)]

        def into(slot):
            return zrecv.at[s, slot, pl.ds(0, PLANE)]

        copies = [
            Message(LOW, layer(0), into(Z_HIGH)),
            Message(HIGH, layer(1), into(Z_LOW)),
            Message(DLOW, zsend.at[s, 0], zrecv.at[s, Z_DHIGH]),
            Message(DHIGH, zsend.at[s, 1], zrecv.at[s, Z_DLOW]),
            Message(LOW2, layer(0), into(Z_HIGH2)),
            Message(HIGH2, layer(1), into(Z_LOW2)),
            Message(PARTNER, zsend.at[s, 0, pl.ds(PLANE, 8)], qrecv.at[s, 3]),
        ]
        for copy in copies:
            copy.start()
        mine = z_plane(gather(plane, 1))
        for copy in copies:
            copy.wait_recv()

        def got(slot):
            return zrecv[s, slot, 0:PLANE, :]

        def got_plane(slot):
            return zrecv[s, slot, PLANE : PLANE + 8, :]

        ghosts = y_transform(
            jnp.concatenate(
                [mine, z_plane(gather(got_plane(Z_DLOW), 2)), z_plane(gather(got_plane(Z_DHIGH), 3))],
                axis=0,
            )
        )
        partner = plane_response(
            z_ghosts(widen(got(Z_DLOW)), widen(got(Z_DHIGH))), ghosts[0:8]
        )
        partner = qrecv[s, 3] + z_plane(y_transform(partner))
        ghost = y_transform(z_plane(gather(partner)))
        above = got(Z_HIGH) + narrow(
            first_of(layer_response(z_ghosts(last, widen(got(Z_HIGH2))), ghosts[16:24]))
        )
        below = got(Z_LOW) + narrow(
            last_of(layer_response(z_ghosts(widen(got(Z_LOW2)), first), ghosts[8:16]))
        )
        above = jnp.where(has_high, above, 0.0)
        below = jnp.where(has_low, below, 0.0)
        both = z_ghosts(widen(below), widen(above))
        sx = side_x()
        for p in range(8):
            extra = weight(0, p) * both + sx * ghost[p : p + 1, :]
            hat[p * 64 : p * 64 + 64, :] = block(hat1, p) + extra * modes(p)
        depth = 3 if s == 0 else 1
        planes = [x_planes(hat, T_SX)]
        if s == 0:
            planes.append(x_planes(hat, T_SX2))
        planes = y_transform(jnp.concatenate(planes, axis=0))
        for i in range(len(planes) // 8):
            qsend[s, i * 8 : i * 8 + 8, :] = z_plane(planes[i * 8 : i * 8 + 8])
        for k in range(depth):
            acc = z_layers(hat, k)
            a, b = x_inverse(jnp.where(half64, first_of(acc), last_of(acc)))
            psend[s, 0, k * PLANE : (k + 1) * PLANE, :] = y_transform(a)
            at = depth - 1 - k
            psend[s, 1, at * PLANE : (at + 1) * PLANE, :] = y_transform(b)
        size = depth * PLANE
        copies = [
            Message(LOW, psend.at[s, 0, pl.ds(0, size)], own.at[pl.ds((CZ + 3) * PLANE, size)]),
            Message(HIGH, psend.at[s, 1, pl.ds(0, size)], own.at[pl.ds((3 - depth) * PLANE, size)]),
        ]
        if s == 0:
            copies += [
                Message(DLOW, qsend.at[s, pl.ds(0, 8)], qrecv.at[s, 2]),
                Message(DHIGH, qsend.at[s, pl.ds(0, 8)], qrecv.at[s, 1]),
                Message(PARTNER, qsend.at[s], psel.at[0]),
            ]
        else:
            copies.append(Message(PARTNER, qsend.at[s, pl.ds(0, 8)], qrecv.at[s, 0]))
        for copy in copies:
            copy.start()
        for p in range(8):
            a, b = x_inverse(block(hat, p))
            ybuf[2 * p * PLANE : (2 * p + 1) * PLANE, :] = a
            ybuf[(2 * p + 1) * PLANE : (2 * p + 2) * PLANE, :] = b
        ybuf[...] = y_transform(ybuf[...])
        z_inverse(ybuf, own, 3 * PLANE)
        return copies

    def correct_plane(s, k, into, at_of):
        own = prs.at[s]
        p = own[rows((k + 3) * PLANE, PLANE), :]
        above = own[rows((k + 4) * PLANE, PLANE), :]
        below = own[rows((k + 2) * PLANE, PLANE), :]
        inner, outer = x_sides(p, 16 + k, 0)
        north, south = y_sides(p)
        half = jnp.where(half0, 0.5, -0.5)
        for f, v in enumerate(
            (half * (inner - outer), 0.5 * (north - south), 0.5 * (above - below))
        ):
            at = rows(at_of(k, f), PLANE)
            into[at, :] = into[at, :] - v

    for f in range(FIELDS):
        fsend[0, f * 8 : f * 8 + 8, :] = own_plane(fld0, f)
    table_loads[0].wait()
    pl.semaphore_wait(barrier, count)
    early = field_messages(fld0, 0)
    maps = [
        Message(PARTNER, idx.at[0], idx.at[1]),
        Message(HIGH, idx.at[0], idx.at[2]),
        Message(LOW, idx.at[0], idx.at[3]),
    ]
    for copy in early + maps:
        copy.start()
    loads[FIELDS].wait()

    def load_burn(b, lanes):
        return bnn[b * 8 : b * 8 + 8, lanes]

    def store_burn(k, r, v):
        burning[rows(k * PLANE + r, 8), :] = v

    to_layers(load_burn, store_burn)
    for copy in table_loads[1:]:
        copy.wait()
    for side in range(2):
        sx = tab[T_SX + side * 64 : T_SX + side * 64 + 64, :]
        for p in range(8):
            start = side * 512 + p * 64
            resp[start : start + 64, :] = modes(p) * weight(0, p) * sx

    def finish0(k, f, v):
        fld1[rows(level(k, f), PLANE), :] = v

    early[2].wait_recv()
    for f in range(FIELDS):
        spread(gather(frecv[0, f * 8 : f * 8 + 8, :]), XG + f * 16)

    @pl.loop(2, CZ - 2)
    def _(k):
        tendency_plane(fld0, k, finish0)

    early[0].wait_recv()
    early[1].wait_recv()

    @pl.loop(0, 4)
    def _(i):
        tendency_plane(fld0, i + (CZ - 4) * (i // 2), finish0)

    early = send_fields(fld1, 1)
    for copy in maps:
        copy.wait_recv()
    final = solve(0)

    final[4].wait_recv()
    early[2].wait_recv()
    near = psel[0, 0:8, :]
    beside = psel[0, 8:16, :]
    spread(gather(near), 16)
    sides = gather(qsend[0, 0:8, :], 1)
    sign = jnp.where(fine, -0.5, 0.5)
    new0 = frecv[1, 0:8, :] - sign * (sides - beside)
    lane8 = lax.broadcasted_iota(jnp.int32, (8, 128), 1)
    north = jnp.where((lane8 == 63) | (lane8 == 127), 0.0, pltpu.roll(near, 127, 1))
    south = jnp.where((lane8 == 0) | (lane8 == 64), 0.0, pltpu.roll(near, 1, 1))
    new1 = frecv[1, 8:16, :] - 0.5 * (north - south)
    other = swap(near)
    up = jnp.where(sub8 == 7, 0.0, pltpu.roll(other, 7, 0))
    down = jnp.where(sub8 == 0, 0.0, pltpu.roll(other, 1, 0))
    above = jnp.where(half8, other, up)
    below = jnp.where(half8, down, other)
    new2 = frecv[1, 16:24, :] - 0.5 * (above - below)
    for f, v in enumerate((new0, new1, new2, frecv[1, 24:32, :], frecv[1, 32:40, :])):
        spread(gather(v), XG + f * 16)
    for copy in early:
        copy.wait_send()

    @pl.loop(1, CZ - 1)
    def _(k):
        correct_plane(0, k, fld1, level)

    def finish1(k, f, v):
        start = fld0[rows(level(k, f), PLANE), :]
        fields[rows((k * FIELDS + f) * PLANE, PLANE), :] = 0.5 * (start + v)

    @pl.loop(3, CZ - 3)
    def _(k):
        tendency_plane(fld1, k, finish1)

    for copy in final[:4] + early[:2]:
        copy.wait_recv()
    spread(gather(qrecv[0, 1], 2), 0)
    spread(gather(qrecv[0, 2], 3), 32)
    over = jnp.broadcast_to(swap(qrecv[0, 2])[0:1, :], (8, 128))
    under = jnp.broadcast_to(swap(qrecv[0, 1])[7:8, :], (8, 128))
    rest = jnp.where(
        half8,
        jnp.where(sub8 == 0, 0.5 * under, 0.0),
        jnp.where(sub8 == 7, -0.5 * over, 0.0),
    )
    spread(gather(rest), TAIL)
    spread(gather(new2 + rest), XG + 2 * 16)

    @pl.loop(0, 2)
    def _(i):
        correct_plane(0, i * (CZ - 1), fld1, level)

    @pl.when(has_low)
    def _():
        @pl.loop(-2, 0)
        def _(k):
            correct_plane(0, k, fld1, level)

    @pl.when(has_high)
    def _():
        @pl.loop(CZ, CZ + 2)
        def _(k):
            correct_plane(0, k, fld1, level)

    @pl.loop(3, CZ - 3)
    def _(k):
        west, east = xg[0, pl.ds(TAIL + k, 1), :], xg[1, pl.ds(TAIL + k, 1), :]
        at = jnp.where(fine, PLANE - 1, 0)
        c = fld1[pl.ds(level(k, 0) + at, 1), :]
        add = 0.5 * (DIFFUSION * (east + west) - (0.5 * COURANT) * c * (east - west))
        lanes = lax.broadcasted_iota(jnp.int32, (1, 128), 1)
        here = jnp.where(fine, lanes, 127 - lanes) >= 64
        row_at = pl.ds((k * FIELDS + 2) * PLANE + at, 1)
        fields[row_at, :] = fields[row_at, :] + jnp.where(here, add, 0.0)

    @pl.loop(0, 6)
    def _(i):
        tendency_plane(fld1, i + (CZ - 6) * (i // 3), finish1)

    final = solve(1)
    final[2].wait_recv()
    spread(gather(qrecv[1, 0]), 16)

    def place(k, f):
        return (k * FIELDS + f) * PLANE

    @pl.loop(1, CZ - 1)
    def _(k):
        correct_plane(1, k, fields, place)

    def store_head(b, lanes, v):
        out_p[b * 8 : b * 8 + 8, lanes] = v

    to_native(lambda k, r: prs[1, rows((k + 3) * PLANE + r, 8), :], store_head)

    def put_field(f):
        def load_field(k, r):
            return fields[rows(place(k, f) + r, 8), :]

        def store_field(b, lanes, v):
            out_s[f, b * 8 : b * 8 + 8, lanes] = v

        to_native(load_field, store_field)

    for f in range(3, FIELDS):
        put_field(f)
    for copy in final[:2]:
        copy.wait_recv()

    @pl.loop(0, 2)
    def _(i):
        correct_plane(1, i * (CZ - 1), fields, place)

    for f in range(3):
        put_field(f)
    for copy in messages:
        copy.wait_send()


def finish_kernel(fields, head, out_s, out_p, sems):
    copies = [
        pltpu.make_async_copy(fields, out_s, sems.at[0]),
        pltpu.make_async_copy(head, out_p, sems.at[1]),
    ]
    for copy in copies:
        copy.start()
    for copy in copies:
        copy.wait()


def write_out(fields, head):
    hbm = pl.BlockSpec(memory_space=pltpu.HBM)
    vmem = pl.BlockSpec(memory_space=pltpu.VMEM)
    return pl.pallas_call(
        finish_kernel,
        out_shape=(
            jax.ShapeDtypeStruct(fields.shape, F32),
            jax.ShapeDtypeStruct(head.shape, F32),
        ),
        in_specs=[vmem, vmem],
        out_specs=(hbm, hbm),
        scratch_shapes=[pltpu.SemaphoreType.DMA((2,))],
        compiler_params=pltpu.CompilerParams(vmem_limit_bytes=1 << 20),
        name="write_out",
    )(fields, head)


def step(state, burn, fmap):
    hbm = pl.BlockSpec(memory_space=pltpu.HBM)
    vmem = pl.BlockSpec(memory_space=pltpu.VMEM)
    tab, bh, bl = tables()
    vm = pltpu.VMEM
    layers = (CZ + 2 * HALO) * LEVEL
    return pl.pallas_call(
        kernel,
        out_shape=(
            jax.ShapeDtypeStruct((FIELDS, CZ, NX * NY), F32),
            jax.ShapeDtypeStruct((CZ, NX * NY), F32),
        ),
        in_specs=[hbm] * 6,
        out_specs=(vmem, vmem),
        scratch_shapes=[
            vm((FIELDS, CZ, NX * NY), F32),
            vm((CZ, NX * NY), F32),
            vm((layers, 128), F32),
            vm((layers, 128), F32),
            vm((CZ * LEVEL, 128), F32),
            vm((CZ * PLANE, 128), F32),
            vm((CZ * PLANE, 128), F32),
            vm((CZ * PLANE, 128), F32),
            vm((CZ * PLANE, 128), F32),
            vm((CZ * PLANE, 128), F32),
            vm((SECTIONS, (CZ + 6) * PLANE, 128), F32),
            vm((1024, 128), F32),
            vm((FIELDS * 48, 128), F32),
            vm((2, 64 + FIELDS * 16, 128), F32),
            vm((SECTIONS, 2, PLANE + 8, 128), F32),
            vm((SECTIONS, 6, PLANE + 8, 128), F32),
            vm((SECTIONS, 2, 3 * PLANE, 128), F32),
            vm((SECTIONS, 16, 128), F32),
            vm((SECTIONS, 4, 8, 128), F32),
            vm((SECTIONS, FIELDS * 8, 128), F32),
            vm((SECTIONS, FIELDS * 8, 128), F32),
            vm((1, 16, 128), F32),
            vm((T_ROWS, 128), F32),
            vm((B_ROWS, 128), BF16),
            vm((B_ROWS, 128), BF16),
            vm((4, 8, 128), jnp.int32),
            pltpu.SemaphoreType.DMA((FIELDS + 1,)),
            pltpu.SemaphoreType.DMA((4,)),
            pltpu.SemaphoreType.DMA((40,)),
            pltpu.SemaphoreType.DMA((40,)),
        ],
        compiler_params=pltpu.CompilerParams(
            collective_id=0, has_side_effects=True, vmem_limit_bytes=40 << 20
        ),
        name="fire_step",
    )(*[pltpu.with_memory_space_constraint(v, pltpu.HBM) for v in (state, burn, fmap, jnp.asarray(tab), jnp.asarray(bh), jnp.asarray(bl))])


def shards(state, burn_rate, face_map):
    fields, head = write_out(*step(state[0], burn_rate[0], face_map.reshape(8, 128)))
    return fields[None], head[None]


def solution(mesh):
    placed = (P("grp", None, "mesh", None), P("grp", "mesh", None), P("grp", "mesh", None))
    return jax.shard_map(
        shards,
        mesh=mesh,
        in_specs=placed,
        out_specs=(P("grp", None, "mesh", None), P("grp", "mesh", None)),
        check_vma=False,
    )
```

```python
import math

import jax
import jax.numpy as jnp
import numpy as np
from jax import lax
from jax.experimental import pallas as pl
from jax.experimental.pallas import tpu as pltpu
from jax.sharding import PartitionSpec as P

NX = 64
NY = 64
CZ = 16
FIELDS = 5
SECTIONS = 2
ITERS = 3
COURANT = 0.1
DIFFUSION = 0.05
STOICHIOMETRY = 2.0
EXPANSION = 1.0

PLANE = 32
LEVEL = FIELDS * PLANE
HALO = 2
MESH = pl.DeviceIdType.MESH
F32 = jnp.float32
BF16 = jnp.bfloat16


def sine(n):
    i = np.arange(n, dtype=np.float64) + 1.0
    return np.sin(np.pi * i[:, None] * i[None, :] / (n + 1)) * math.sqrt(2.0 / (n + 1))


def eigen(n):
    i = np.arange(n, dtype=np.float64) + 1.0
    return 2.0 - 2.0 * np.cos(np.pi * i / (n + 1))


T_IM = 0
T_Z1 = 512
T_Z2 = 576
T_W = 640
T_GAMMA = 664
T_ALPHA = 672
T_SX = 736
T_SX2 = 864
T_ZF = 992
T_ROWS = 1056
B_Y = 0
B_XF = 128
B_XI = 192
B_ROWS = 256


def tables():
    s16, s64 = sine(CZ), sine(NX)
    tab = np.zeros((T_ROWS, 128))
    modes = eigen(CZ)[:, None, None] + eigen(NX)[None, :, None] + eigen(NY)[None, None, :]
    inv = 1.0 / modes
    tab[T_IM : T_IM + 512] = (
        inv.reshape(8, 2, 64, 64).transpose(0, 2, 1, 3).reshape(512, 128)
    )
    for p in range(8):
        for h in range(2):
            lanes = slice(64 * h, 64 * h + 64)
            for r in range(8):
                tab[T_Z1 + p * 8 + r, lanes] = s16[2 * p + h, 2 * r + h]
                tab[T_Z2 + p * 8 + r, lanes] = s16[2 * p + 1 - h, 2 * r + h]
            for k in range(8):
                tab[T_ZF + p * 8 + k, lanes] = s16[2 * p + h, k] * (-1.0) ** h
            for k in range(3):
                tab[T_W + 8 * k + p, lanes] = s16[2 * p + h, k]
    for at, places in ((T_SX, (63, 0)), (T_SX2, (62, 1))):
        for side, place in enumerate(places):
            tab[at + 64 * side : at + 64 * side + 64] = s64[:, place][:, None]
    packed = tab[T_IM : T_IM + 512].reshape(8, 64, 128)
    tab[T_ALPHA : T_ALPHA + 64] = (packed * tab[T_W : T_W + 8, None, :] ** 2).sum(0)
    tab[T_GAMMA : T_GAMMA + 8] = (packed * tab[None, T_SX : T_SX + 64] ** 2).sum(1)
    mat = np.zeros((B_ROWS, 128))
    mat[B_Y : B_Y + 128] = np.kron(np.eye(2), s64)
    order = np.concatenate([np.arange(0, 64, 2), np.arange(1, 64, 2)])
    mat[B_XF : B_XF + 64, :64] = s64[:, order]
    mat[B_XI : B_XI + 64, :64] = s64[order, :]
    mat = mat.astype(np.float32)
    high = mat.astype(jnp.bfloat16)
    low = (mat - high.astype(np.float32)).astype(jnp.bfloat16)
    return tab.astype(np.float32), high, low


S16 = sine(CZ)


def split(v):
    high = v.astype(BF16)
    return high, (v - high.astype(F32)).astype(BF16)


def dot(a, b):
    return jnp.dot(a, b, preferred_element_type=F32)


def dot_right(v, th, tl):
    vh, vl = split(v)
    return dot(vh, th) + (dot(vl, th) + dot(vh, tl))


def dot_left(th, tl, v):
    vh, vl = split(v)
    return dot(th, vh) + (dot(th, vl) + dot(tl, vh))


def kernel(
    state, burn, fmap, tab_h, bh_h, bl_h, out_s, out_p,
    stn, bnn, fld0, fld1, fields, burning, src, ybuf, hat1, hat, prs, resp,
    turns, xg, zsend, zrecv, psend, qsend, qrecv, fsend, frecv, psel, tab, bh, bl, idx,
    in_sem, t_sem, send_sem, recv_sem,
):
    g = lax.axis_index("grp")
    m = lax.axis_index("mesh")
    n = lax.axis_size("mesh")
    fine = g == 0
    LOW, HIGH, PARTNER, LOW2, HIGH2, DLOW, DHIGH = range(7)
    back = (HIGH, LOW, PARTNER, HIGH2, LOW2, DHIGH, DLOW)
    has_low, has_high = m > 0, m < n - 1
    exists = (has_low, has_high, None, m > 1, m < n - 2, has_low, has_high)
    steps = (-1, 1, 0, -2, 2, -1, 1)
    where_to = [
        {"grp": 1 - g if to in (PARTNER, DLOW, DHIGH) else g, "mesh": lax.rem(m + n + steps[to], n)}
        for to in range(7)
    ]
    count = 1
    for to in range(7):
        if exists[to] is not None:
            count = count + exists[to].astype(jnp.int32)

    def guarded(condition, action):
        if condition is None:
            action()
        else:
            pl.when(condition)(action)

    loads = [
        pltpu.make_async_copy(state.at[f], stn.at[f], in_sem.at[f]) for f in range(FIELDS)
    ]
    loads.append(pltpu.make_async_copy(burn, bnn, in_sem.at[FIELDS]))
    for copy in loads:
        copy.start()
    table_loads = [
        pltpu.make_async_copy(a, b, t_sem.at[i])
        for i, (a, b) in enumerate(((fmap, idx.at[0]), (tab_h, tab), (bh_h, bh), (bl_h, bl)))
    ]
    for copy in table_loads:
        copy.start()

    def clear(ref, start, size):
        ref[start : start + size, :] = jnp.zeros((size, 128), F32)

    @pl.when(jnp.logical_not(has_low))
    def _():
        clear(fld0, 0, 2 * LEVEL)
        clear(fld1, 0, 2 * LEVEL)
        for s in range(SECTIONS):
            clear(prs.at[s], 0, 3 * PLANE)
            for part in (1, 4):
                clear(zrecv.at[s, part], 0, PLANE + 8)
            clear(qrecv.at[s, 1], 0, 8)

    @pl.when(jnp.logical_not(has_high))
    def _():
        clear(fld0, (CZ + 2) * LEVEL, 2 * LEVEL)
        clear(fld1, (CZ + 2) * LEVEL, 2 * LEVEL)
        for s in range(SECTIONS):
            clear(prs.at[s], (CZ + 3) * PLANE, 3 * PLANE)
            for part in (0, 5):
                clear(zrecv.at[s, part], 0, PLANE + 8)
            clear(qrecv.at[s, 2], 0, 8)

    @pl.when(m < 2)
    def _():
        for s in range(SECTIONS):
            clear(zrecv.at[s, 3], 0, PLANE + 8)

    @pl.when(m > n - 3)
    def _():
        for s in range(SECTIONS):
            clear(zrecv.at[s, 2], 0, PLANE + 8)

    barrier = pltpu.get_barrier_semaphore()
    for to in range(7):
        guarded(
            exists[to],
            lambda to=to: pl.semaphore_signal(
                barrier, inc=1, device_id=where_to[to], device_id_type=MESH
            ),
        )

    messages = []

    class Message:
        def __init__(self, to, a, b):
            slot = len(messages)
            messages.append(self)
            self.to = to
            self.copy = pltpu.make_async_remote_copy(
                src_ref=a, dst_ref=b, send_sem=send_sem.at[slot], recv_sem=recv_sem.at[slot],
                device_id=where_to[to], device_id_type=MESH,
            )
            self.sent = False

        def start(self):
            guarded(exists[self.to], self.copy.start)

        def wait_recv(self):
            guarded(exists[back[self.to]], self.copy.wait_recv)

        def wait_send(self):
            if not self.sent:
                self.sent = True
                guarded(exists[self.to], self.copy.wait_send)

    lane = lax.broadcasted_iota(jnp.int32, (PLANE, 128), 1)
    half0 = lane < 64
    y_last = (lane == 63) | (lane == 127)
    y_first = (lane == 0) | (lane == 64)
    half8 = lax.broadcasted_iota(jnp.int32, (8, 128), 1) < 64
    half64 = lax.broadcasted_iota(jnp.int32, (64, 128), 1) < 64
    sub8 = lax.broadcasted_iota(jnp.int32, (8, 128), 0)

    def swap(v):
        return pltpu.roll(v, 64, 1)

    def rows(start, size):
        return pl.ds(pl.multiple_of(start, 8), size)

    def level(k, f):
        return ((k + HALO) * FIELDS + f) * PLANE

    def to_layers(load, store):
        for b in range(2):
            for t in range(4):
                tiles = jnp.stack([load(b, pl.ds((t * 8 + i) * 128, 128)) for i in range(8)])
                turned = jnp.swapaxes(tiles, 0, 1)
                for i in range(8):
                    store(b * 8 + i, t * 8, turned[i])

    def to_native(load, store):
        for b in range(2):
            for t in range(4):
                tiles = jnp.stack([load(b * 8 + i, t * 8) for i in range(8)])
                turned = jnp.swapaxes(tiles, 0, 1)
                for i in range(8):
                    store(b, pl.ds((t * 8 + i) * 128, 128), turned[i])

    for f in range(FIELDS):
        loads[f].wait()

        def load_state(b, lanes, f=f):
            return stn[f, b * 8 : b * 8 + 8, lanes]

        def store_state(k, r, v, f=f):
            fld0[rows(level(k, f) + r, 8), :] = v

        to_layers(load_state, store_state)

    def own_plane(fld, f):
        at = jnp.where(fine, PLANE - 1, 0)
        tiles = []
        for odd in range(2):
            tile = jnp.zeros((8, 128), F32)
            for r in range(8):
                one = fld[pl.ds(level(2 * r + odd, f) + at, 1), :]
                tile = jnp.where(sub8 == r, jnp.broadcast_to(one, (8, 128)), tile)
            tiles.append(tile)
        even, odd = tiles
        return jnp.where(
            fine, jnp.where(half8, swap(even), odd), jnp.where(half8, even, swap(odd))
        )

    def field_messages(fld, s):
        return [
            Message(LOW, fld.at[pl.ds(level(0, 0), 2 * LEVEL)],
                    fld.at[pl.ds(level(CZ, 0), 2 * LEVEL)]),
            Message(HIGH, fld.at[pl.ds(level(CZ - 2, 0), 2 * LEVEL)],
                    fld.at[pl.ds(level(-2, 0), 2 * LEVEL)]),
            Message(PARTNER, fsend.at[s], frecv.at[s]),
        ]

    def send_fields(fld, s):
        copies = field_messages(fld, s)
        copies[0].start()
        copies[1].start()
        for f in range(FIELDS):
            fsend[s, f * 8 : f * 8 + 8, :] = own_plane(fld, f)
        copies[2].start()
        return copies

    def gather(plane, who=0):
        index = idx[who]
        column = index & 127
        block = index >> 7
        out = jnp.zeros((8, 128), F32)
        for r in range(8):
            one = jnp.broadcast_to(plane[r : r + 1, :], (8, 128))
            out = jnp.where(block == r, jnp.take_along_axis(one, column, axis=1), out)
        return out

    def spread(ghost, base):
        other = swap(ghost)
        even = jnp.where(half8, ghost, other)
        odd = jnp.where(half8, other, ghost)
        zero = jnp.zeros_like(ghost)
        for side in range(2):
            on = fine if side else jnp.logical_not(fine)
            xg[side, pl.ds(base, 8, stride=2), :] = jnp.where(on, even, zero)
            xg[side, pl.ds(base + 1, 8, stride=2), :] = jnp.where(on, odd, zero)

    def x_sides(v, at, slot):
        base = slot * 48
        turned = swap(v)
        turns[base + 8 : base + 40, :] = turned
        turns[base + 7 : base + 8, :] = xg[0, pl.ds(at, 1), :]
        turns[base + 40 : base + 41, :] = xg[1, pl.ds(at, 1), :]
        down = turns[base + 7 : base + 39, :]
        up = turns[base + 9 : base + 41, :]
        return turned, jnp.where(half0, down, up)

    def y_sides(v):
        north = jnp.where(y_last, 0.0, pltpu.roll(v, 127, 1))
        south = jnp.where(y_first, 0.0, pltpu.roll(v, 1, 1))
        return north, south

    XG = 48
    TAIL = XG + FIELDS * 16

    def tendency_plane(fld, k, finish, u=0):
        c = [fld[rows(level(k, f), PLANE), :] for f in range(FIELDS)]
        reaction = burning[rows(k * PLANE, PLANE), :] * c[3] * c[4]
        source = EXPANSION * reaction
        half = jnp.where(half0, 0.5, -0.5)
        cx = c[0] * (half * -COURANT)
        cy = c[1] * (-0.5 * COURANT)
        cz = c[2] * (-COURANT * 2.0 / 3.0)
        cz2 = c[2] * (COURANT / 12.0)
        for f in range(FIELDS):
            above = fld[rows(level(k + 1, f), PLANE), :]
            below = fld[rows(level(k - 1, f), PLANE), :]
            above2 = fld[rows(level(k + 2, f), PLANE), :]
            below2 = fld[rows(level(k - 2, f), PLANE), :]
            inner, outer = x_sides(c[f], XG + f * 16 + k, u * FIELDS + f)
            north, south = y_sides(c[f])
            dx = inner - outer
            dy = north - south
            dz = above - below
            total = (inner + outer) + (north + south) + (above + below)
            change = (DIFFUSION * total + cx * dx) + (cy * dy + cz * dz) + cz2 * (above2 - below2)
            if f == 0:
                source = source - half * dx
            elif f == 1:
                source = source - 0.5 * dy
            elif f == 2:
                source = source - 0.5 * dz
            elif f == 3:
                change = change - reaction
            else:
                change = change - STOICHIOMETRY * reaction
            finish(k, f, c[f] * (1.0 - 6.0 * DIFFUSION) + change)
        src[rows(k * PLANE, PLANE), :] = source

    def z_inverse(spec, into, base):
        @pl.loop(0, 4)
        def _(t):
            v = [spec[rows(c * PLANE + t * 8, 8), :] for c in range(CZ)]
            for k in range(8):
                even = v[0] * F32(S16[0, k])
                odd = v[1] * F32(S16[1, k])
                for c in range(1, 8):
                    even = even + v[2 * c] * F32(S16[2 * c, k])
                    odd = odd + v[2 * c + 1] * F32(S16[2 * c + 1, k])
                into[rows(base + k * PLANE + t * 8, 8), :] = even + odd
                into[rows(base + (15 - k) * PLANE + t * 8, 8), :] = even - odd

    def y_matrix():
        return bh[B_Y : B_Y + 128, :], bl[B_Y : B_Y + 128, :]

    def y_transform(v):
        return dot_right(v, *y_matrix())

    def x_forward(a, b):
        even = jnp.where(half0, a, swap(b))
        odd = jnp.where(half0, swap(a), b)
        v = jnp.concatenate([even, odd], axis=0)
        return dot_left(bh[B_XF : B_XF + 64, :64], bl[B_XF : B_XF + 64, :64], v)

    def transform(first, last):
        pairs = range(first, 8) if last == 0 else range(last)
        if last == 0:
            v = y_transform(src[first * PLANE : (CZ - first) * PLANE, :])
            planes = {k: v[(k - first) * PLANE : (k - first + 1) * PLANE] for k in range(first, CZ - first)}
        else:
            v = y_transform(
                jnp.concatenate(
                    [src[: last * PLANE, :], src[(CZ - last) * PLANE : CZ * PLANE, :]], axis=0
                )
            )
            planes = {k: v[k * PLANE : (k + 1) * PLANE] for k in range(last)}
            for i in range(last):
                planes[CZ - last + i] = v[(last + i) * PLANE : (last + i + 1) * PLANE]
        for k in pairs:
            ybuf[k * 64 : k * 64 + 64, :] = x_forward(planes[k], planes[CZ - 1 - k])

    def x_inverse(v):
        v = dot_left(bh[B_XI : B_XI + 64, :64], bl[B_XI : B_XI + 64, :64], v)
        even, odd = v[:PLANE], v[PLANE:]
        return jnp.where(half0, even, swap(odd)), jnp.where(half0, swap(even), odd)

    def z_plane(v):
        other = swap(v)
        parts = []
        for p in range(8):
            parts.append(tab[T_Z1 + p * 8 : T_Z1 + p * 8 + 8, :] * v[p : p + 1, :])
            parts.append(tab[T_Z2 + p * 8 : T_Z2 + p * 8 + 8, :] * other[p : p + 1, :])
        while len(parts) > 1:
            parts = [a + b for a, b in zip(parts[::2], parts[1::2])]
        return parts[0]

    def side_x(at=T_SX):
        return tab[rows(at + g * 64, 64), :]

    def weight(k, p):
        return tab[T_W + 8 * k + p : T_W + 8 * k + p + 1, :]

    def modes(p):
        return tab[T_IM + p * 64 : T_IM + p * 64 + 64, :]

    def block(ref, p):
        return ref[p * 64 : p * 64 + 64, :]

    def first_of(acc):
        return acc + swap(acc)

    def last_of(acc):
        other = swap(acc)
        return jnp.where(half64, acc - other, other - acc)

    def z_layers(spec, k):
        acc = weight(k, 0) * block(spec, 0)
        for p in range(1, 8):
            acc = acc + weight(k, p) * block(spec, p)
        return acc

    def x_planes(spec, at):
        sx = side_x(at)
        return jnp.concatenate(
            [jnp.sum(sx * block(spec, p), axis=0, keepdims=True) for p in range(8)], axis=0
        )

    def narrow(v):
        return jnp.where(half0, v[:PLANE], v[PLANE:])

    def widen(v):
        other = swap(v)
        return jnp.concatenate(
            [jnp.where(half0, v, other), jnp.where(half0, other, v)], axis=0
        )

    def z_ghosts(below, above):
        return below + jnp.where(half64, above, -above)

    def layer_response(both, ghost):
        acc = tab[T_ALPHA : T_ALPHA + 64, :] * both
        for p in range(8):
            acc = acc + resp[rows(g * 512 + p * 64, 64), :] * ghost[p : p + 1, :]
        return acc

    def plane_response(both, ghost):
        side = jnp.concatenate(
            [
                jnp.sum(resp[rows((1 - g) * 512 + p * 64, 64), :] * both, axis=0, keepdims=True)
                for p in range(8)
            ],
            axis=0,
        )
        return side + tab[T_GAMMA : T_GAMMA + 8, :] * ghost

    Z_HIGH, Z_LOW, Z_HIGH2, Z_LOW2, Z_DLOW, Z_DHIGH = range(6)

    def solve(s):
        own = prs.at[s]
        for r in range(8):
            pairs = []
            for p in range(8):
                v = ybuf[p * 64 + r * 8 : p * 64 + r * 8 + 8, :]
                pairs.append(v + jnp.where(half8, swap(v), -swap(v)))
            for q in range(8):
                parts = [
                    tab[T_ZF + q * 8 + p : T_ZF + q * 8 + p + 1, :] * pairs[p] for p in range(8)
                ]
                while len(parts) > 1:
                    parts = [a + b for a, b in zip(parts[::2], parts[1::2])]
                at = q * 64 + r * 8
                hat1[at : at + 8, :] = parts[0] * tab[T_IM + at : T_IM + at + 8, :]
        acc = z_layers(hat1, 0)
        first, last = first_of(acc), last_of(acc)
        plane = z_plane(y_transform(x_planes(hat1, T_SX)))
        zsend[s, 0, 0:PLANE, :] = narrow(first)
        zsend[s, 1, 0:PLANE, :] = narrow(last)
        zsend[s, 0, PLANE : PLANE + 8, :] = plane
        zsend[s, 1, PLANE : PLANE + 8, :] = plane

        def layer(side):
            return zsend.at[s, side, pl.ds(0, PLANE)]

        def into(slot):
            return zrecv.at[s, slot, pl.ds(0, PLANE)]

        copies = [
            Message(LOW, layer(0), into(Z_HIGH)),
            Message(HIGH, layer(1), into(Z_LOW)),
            Message(DLOW, zsend.at[s, 0], zrecv.at[s, Z_DHIGH]),
            Message(DHIGH, zsend.at[s, 1], zrecv.at[s, Z_DLOW]),
            Message(LOW2, layer(0), into(Z_HIGH2)),
            Message(HIGH2, layer(1), into(Z_LOW2)),
            Message(PARTNER, zsend.at[s, 0, pl.ds(PLANE, 8)], qrecv.at[s, 3]),
        ]
        for copy in copies:
            copy.start()
        mine = y_transform(z_plane(gather(plane, 1)))
        for copy in copies:
            copy.wait_recv()

        def got(slot):
            return zrecv[s, slot, 0:PLANE, :]

        def got_plane(slot):
            return zrecv[s, slot, PLANE : PLANE + 8, :]

        ghosts = y_transform(
            jnp.concatenate(
                [z_plane(gather(got_plane(Z_DLOW), 2)), z_plane(gather(got_plane(Z_DHIGH), 3))],
                axis=0,
            )
        )
        partner = plane_response(
            z_ghosts(widen(got(Z_DLOW)), widen(got(Z_DHIGH))), mine
        )
        partner = qrecv[s, 3] + z_plane(y_transform(partner))
        ghost = y_transform(z_plane(gather(partner)))
        above = got(Z_HIGH) + narrow(
            first_of(layer_response(z_ghosts(last, widen(got(Z_HIGH2))), ghosts[8:16]))
        )
        below = got(Z_LOW) + narrow(
            last_of(layer_response(z_ghosts(widen(got(Z_LOW2)), first), ghosts[0:8]))
        )
        above = jnp.where(has_high, above, 0.0)
        below = jnp.where(has_low, below, 0.0)
        both = z_ghosts(widen(below), widen(above))
        sx = side_x()
        for p in range(8):
            extra = weight(0, p) * both + sx * ghost[p : p + 1, :]
            hat[p * 64 : p * 64 + 64, :] = block(hat1, p) + extra * modes(p)
        depth = 3 if s == 0 else 1
        planes = [x_planes(hat, T_SX)]
        if s == 0:
            planes.append(x_planes(hat, T_SX2))
        planes = y_transform(jnp.concatenate(planes, axis=0))
        for i in range(len(planes) // 8):
            qsend[s, i * 8 : i * 8 + 8, :] = z_plane(planes[i * 8 : i * 8 + 8])
        for k in range(depth):
            acc = z_layers(hat, k)
            a, b = x_inverse(jnp.where(half64, first_of(acc), last_of(acc)))
            psend[s, 0, k * PLANE : (k + 1) * PLANE, :] = y_transform(a)
            at = depth - 1 - k
            psend[s, 1, at * PLANE : (at + 1) * PLANE, :] = y_transform(b)
        size = depth * PLANE
        copies = [
            Message(LOW, psend.at[s, 0, pl.ds(0, size)], own.at[pl.ds((CZ + 3) * PLANE, size)]),
            Message(HIGH, psend.at[s, 1, pl.ds(0, size)], own.at[pl.ds((3 - depth) * PLANE, size)]),
        ]
        if s == 0:
            copies += [
                Message(DLOW, qsend.at[s, pl.ds(0, 8)], qrecv.at[s, 2]),
                Message(DHIGH, qsend.at[s, pl.ds(0, 8)], qrecv.at[s, 1]),
                Message(PARTNER, qsend.at[s], psel.at[0]),
            ]
        else:
            copies.append(Message(PARTNER, qsend.at[s, pl.ds(0, 8)], qrecv.at[s, 0]))
        for copy in copies:
            copy.start()
        for p in range(8):
            a, b = x_inverse(block(hat, p))
            ybuf[2 * p * PLANE : (2 * p + 1) * PLANE, :] = a
            ybuf[(2 * p + 1) * PLANE : (2 * p + 2) * PLANE, :] = b
        ybuf[...] = y_transform(ybuf[...])
        z_inverse(ybuf, own, 3 * PLANE)
        return copies

    def correct_plane(s, k, into, at_of, u=0):
        own = prs.at[s]
        p = own[rows((k + 3) * PLANE, PLANE), :]
        above = own[rows((k + 4) * PLANE, PLANE), :]
        below = own[rows((k + 2) * PLANE, PLANE), :]
        inner, outer = x_sides(p, 16 + k, u)
        north, south = y_sides(p)
        half = jnp.where(half0, 0.5, -0.5)
        for f, v in enumerate(
            (half * (inner - outer), 0.5 * (north - south), 0.5 * (above - below))
        ):
            at = rows(at_of(k, f), PLANE)
            into[at, :] = into[at, :] - v

    for f in range(FIELDS):
        fsend[0, f * 8 : f * 8 + 8, :] = own_plane(fld0, f)
    table_loads[0].wait()
    pl.semaphore_wait(barrier, count)
    early = field_messages(fld0, 0)
    maps = [
        Message(PARTNER, idx.at[0], idx.at[1]),
        Message(HIGH, idx.at[0], idx.at[2]),
        Message(LOW, idx.at[0], idx.at[3]),
    ]
    for copy in early + maps:
        copy.start()
    loads[FIELDS].wait()

    def load_burn(b, lanes):
        return bnn[b * 8 : b * 8 + 8, lanes]

    def store_burn(k, r, v):
        burning[rows(k * PLANE + r, 8), :] = v

    to_layers(load_burn, store_burn)
    for copy in table_loads[1:]:
        copy.wait()
    for side in range(2):
        sx = tab[T_SX + side * 64 : T_SX + side * 64 + 64, :]
        for p in range(8):
            start = side * 512 + p * 64
            resp[start : start + 64, :] = modes(p) * weight(0, p) * sx

    def finish0(k, f, v):
        fld1[rows(level(k, f), PLANE), :] = v

    early[2].wait_recv()
    for f in range(FIELDS):
        spread(gather(frecv[0, f * 8 : f * 8 + 8, :]), XG + f * 16)

    @pl.loop(0, 6)
    def _(i):
        for u in range(2):
            tendency_plane(fld0, 2 + 2 * i + u, finish0, u)

    transform(2, 0)

    early[0].wait_recv()
    early[1].wait_recv()

    @pl.loop(0, 2)
    def _(i):
        for u in range(2):
            tendency_plane(fld0, i * (CZ - 2) + u, finish0, u)

    early = send_fields(fld1, 1)
    for copy in maps:
        copy.wait_recv()
    transform(0, 2)
    final = solve(0)

    final[4].wait_recv()
    early[2].wait_recv()
    near = psel[0, 0:8, :]
    beside = psel[0, 8:16, :]
    spread(gather(near), 16)
    sides = gather(qsend[0, 0:8, :], 1)
    sign = jnp.where(fine, -0.5, 0.5)
    new0 = frecv[1, 0:8, :] - sign * (sides - beside)
    lane8 = lax.broadcasted_iota(jnp.int32, (8, 128), 1)
    north = jnp.where((lane8 == 63) | (lane8 == 127), 0.0, pltpu.roll(near, 127, 1))
    south = jnp.where((lane8 == 0) | (lane8 == 64), 0.0, pltpu.roll(near, 1, 1))
    new1 = frecv[1, 8:16, :] - 0.5 * (north - south)
    other = swap(near)
    up = jnp.where(sub8 == 7, 0.0, pltpu.roll(other, 7, 0))
    down = jnp.where(sub8 == 0, 0.0, pltpu.roll(other, 1, 0))
    above = jnp.where(half8, other, up)
    below = jnp.where(half8, down, other)
    new2 = frecv[1, 16:24, :] - 0.5 * (above - below)
    for f, v in enumerate((new0, new1, new2, frecv[1, 24:32, :], frecv[1, 32:40, :])):
        spread(gather(v), XG + f * 16)
    for copy in early:
        copy.wait_send()

    @pl.loop(0, 2)
    def _(i):
        for u in range(7):
            correct_plane(0, 1 + 7 * i + u, fld1, level, u)

    def finish1(k, f, v):
        start = fld0[rows(level(k, f), PLANE), :]
        fields[rows((k * FIELDS + f) * PLANE, PLANE), :] = 0.5 * (start + v)

    @pl.loop(0, 5)
    def _(i):
        for u in range(2):
            tendency_plane(fld1, 3 + 2 * i + u, finish1, u)

    transform(3, 0)

    for copy in final[:4] + early[:2]:
        copy.wait_recv()
    spread(gather(qrecv[0, 1], 2), 0)
    spread(gather(qrecv[0, 2], 3), 32)
    over = jnp.broadcast_to(swap(qrecv[0, 2])[0:1, :], (8, 128))
    under = jnp.broadcast_to(swap(qrecv[0, 1])[7:8, :], (8, 128))
    rest = jnp.where(
        half8,
        jnp.where(sub8 == 0, 0.5 * under, 0.0),
        jnp.where(sub8 == 7, -0.5 * over, 0.0),
    )
    spread(gather(rest), TAIL)
    spread(gather(new2 + rest), XG + 2 * 16)

    for u in range(2):
        correct_plane(0, u * (CZ - 1), fld1, level, u)

    @pl.when(has_low)
    def _():
        for u in range(2):
            correct_plane(0, u - 2, fld1, level, u)

    @pl.when(has_high)
    def _():
        for u in range(2):
            correct_plane(0, CZ + u, fld1, level, u)

    for k in range(3, CZ - 3):
        west, east = xg[0, pl.ds(TAIL + k, 1), :], xg[1, pl.ds(TAIL + k, 1), :]
        at = jnp.where(fine, PLANE - 1, 0)
        c = fld1[pl.ds(level(k, 0) + at, 1), :]
        add = 0.5 * (DIFFUSION * (east + west) - (0.5 * COURANT) * c * (east - west))
        lanes = lax.broadcasted_iota(jnp.int32, (1, 128), 1)
        here = jnp.where(fine, lanes, 127 - lanes) >= 64
        row_at = pl.ds((k * FIELDS + 2) * PLANE + at, 1)
        fields[row_at, :] = fields[row_at, :] + jnp.where(here, add, 0.0)

    @pl.loop(0, 2)
    def _(i):
        for u in range(3):
            tendency_plane(fld1, i * (CZ - 3) + u, finish1, u)

    transform(0, 3)
    final = solve(1)
    final[2].wait_recv()
    spread(gather(qrecv[1, 0]), 16)

    def place(k, f):
        return (k * FIELDS + f) * PLANE

    @pl.loop(0, 2)
    def _(i):
        for u in range(7):
            correct_plane(1, 1 + 7 * i + u, fields, place, u)

    def store_head(b, lanes, v):
        out_p[b * 8 : b * 8 + 8, lanes] = v

    to_native(lambda k, r: prs[1, rows((k + 3) * PLANE + r, 8), :], store_head)

    def put_field(f):
        def load_field(k, r):
            return fields[rows(place(k, f) + r, 8), :]

        def store_field(b, lanes, v):
            out_s[f, b * 8 : b * 8 + 8, lanes] = v

        to_native(load_field, store_field)

    for f in range(3, FIELDS):
        put_field(f)
    for copy in final[:2]:
        copy.wait_recv()

    for u in range(2):
        correct_plane(1, u * (CZ - 1), fields, place, u)

    for f in range(3):
        put_field(f)
    for copy in messages:
        copy.wait_send()


def finish_kernel(fields, head, out_s, out_p, sems):
    copies = [
        pltpu.make_async_copy(fields, out_s, sems.at[0]),
        pltpu.make_async_copy(head, out_p, sems.at[1]),
    ]
    for copy in copies:
        copy.start()
    for copy in copies:
        copy.wait()


def write_out(fields, head):
    hbm = pl.BlockSpec(memory_space=pltpu.HBM)
    vmem = pl.BlockSpec(memory_space=pltpu.VMEM)
    return pl.pallas_call(
        finish_kernel,
        out_shape=(
            jax.ShapeDtypeStruct(fields.shape, F32),
            jax.ShapeDtypeStruct(head.shape, F32),
        ),
        in_specs=[vmem, vmem],
        out_specs=(hbm, hbm),
        scratch_shapes=[pltpu.SemaphoreType.DMA((2,))],
        compiler_params=pltpu.CompilerParams(vmem_limit_bytes=1 << 20),
        name="write_out",
    )(fields, head)


def step(state, burn, fmap):
    hbm = pl.BlockSpec(memory_space=pltpu.HBM)
    vmem = pl.BlockSpec(memory_space=pltpu.VMEM)
    tab, bh, bl = tables()
    vm = pltpu.VMEM
    layers = (CZ + 2 * HALO) * LEVEL
    return pl.pallas_call(
        kernel,
        out_shape=(
            jax.ShapeDtypeStruct((FIELDS, CZ, NX * NY), F32),
            jax.ShapeDtypeStruct((CZ, NX * NY), F32),
        ),
        in_specs=[hbm] * 6,
        out_specs=(vmem, vmem),
        scratch_shapes=[
            vm((FIELDS, CZ, NX * NY), F32),
            vm((CZ, NX * NY), F32),
            vm((layers, 128), F32),
            vm((layers, 128), F32),
            vm((CZ * LEVEL, 128), F32),
            vm((CZ * PLANE, 128), F32),
            vm((CZ * PLANE, 128), F32),
            vm((CZ * PLANE, 128), F32),
            vm((CZ * PLANE, 128), F32),
            vm((CZ * PLANE, 128), F32),
            vm((SECTIONS, (CZ + 6) * PLANE, 128), F32),
            vm((1024, 128), F32),
            vm((3 * FIELDS * 48, 128), F32),
            vm((2, 64 + FIELDS * 16, 128), F32),
            vm((SECTIONS, 2, PLANE + 8, 128), F32),
            vm((SECTIONS, 6, PLANE + 8, 128), F32),
            vm((SECTIONS, 2, 3 * PLANE, 128), F32),
            vm((SECTIONS, 16, 128), F32),
            vm((SECTIONS, 4, 8, 128), F32),
            vm((SECTIONS, FIELDS * 8, 128), F32),
            vm((SECTIONS, FIELDS * 8, 128), F32),
            vm((1, 16, 128), F32),
            vm((T_ROWS, 128), F32),
            vm((B_ROWS, 128), BF16),
            vm((B_ROWS, 128), BF16),
            vm((4, 8, 128), jnp.int32),
            pltpu.SemaphoreType.DMA((FIELDS + 1,)),
            pltpu.SemaphoreType.DMA((4,)),
            pltpu.SemaphoreType.DMA((40,)),
            pltpu.SemaphoreType.DMA((40,)),
        ],
        compiler_params=pltpu.CompilerParams(
            collective_id=0, has_side_effects=True, vmem_limit_bytes=40 << 20
        ),
        name="fire_step",
    )(*[pltpu.with_memory_space_constraint(v, pltpu.HBM) for v in (state, burn, fmap, jnp.asarray(tab), jnp.asarray(bh), jnp.asarray(bl))])


def shards(state, burn_rate, face_map):
    fields, head = write_out(*step(state[0], burn_rate[0], face_map.reshape(8, 128)))
    return fields[None], head[None]


def solution(mesh):
    placed = (P("grp", None, "mesh", None), P("grp", "mesh", None), P("grp", "mesh", None))
    return jax.shard_map(
        shards,
        mesh=mesh,
        in_specs=placed,
        out_specs=(P("grp", None, "mesh", None), P("grp", "mesh", None)),
        check_vma=False,
    )
```

```python
import math

import jax
import jax.numpy as jnp
import numpy as np
from jax import lax
from jax.experimental import pallas as pl
from jax.experimental.pallas import tpu as pltpu
from jax.sharding import PartitionSpec as P

NX = 64
NY = 64
CZ = 16
FIELDS = 5
SECTIONS = 2
ITERS = 3
COURANT = 0.1
DIFFUSION = 0.05
STOICHIOMETRY = 2.0
EXPANSION = 1.0

PLANE = 32
LEVEL = FIELDS * PLANE
HALO = 2
MESH = pl.DeviceIdType.MESH
F32 = jnp.float32
BF16 = jnp.bfloat16


def sine(n):
    i = np.arange(n, dtype=np.float64) + 1.0
    return np.sin(np.pi * i[:, None] * i[None, :] / (n + 1)) * math.sqrt(2.0 / (n + 1))


def eigen(n):
    i = np.arange(n, dtype=np.float64) + 1.0
    return 2.0 - 2.0 * np.cos(np.pi * i / (n + 1))


T_IM = 0
T_Z1 = 512
T_Z2 = 576
T_W = 640
T_GAMMA = 664
T_ALPHA = 672
T_SX = 736
T_SX2 = 864
T_ZF = 992
T_ROWS = 1056
B_Y = 0
B_XF = 128
B_XI = 192
B_ROWS = 256


def tables():
    s16, s64 = sine(CZ), sine(NX)
    tab = np.zeros((T_ROWS, 128))
    modes = eigen(CZ)[:, None, None] + eigen(NX)[None, :, None] + eigen(NY)[None, None, :]
    inv = 1.0 / modes
    tab[T_IM : T_IM + 512] = (
        inv.reshape(8, 2, 64, 64).transpose(0, 2, 1, 3).reshape(512, 128)
    )
    for p in range(8):
        for h in range(2):
            lanes = slice(64 * h, 64 * h + 64)
            for r in range(8):
                tab[T_Z1 + p * 8 + r, lanes] = s16[2 * p + h, 2 * r + h]
                tab[T_Z2 + p * 8 + r, lanes] = s16[2 * p + 1 - h, 2 * r + h]
            for k in range(8):
                tab[T_ZF + p * 8 + k, lanes] = s16[2 * p + h, k] * (-1.0) ** h
            for k in range(3):
                tab[T_W + 8 * k + p, lanes] = s16[2 * p + h, k]
    for at, places in ((T_SX, (63, 0)), (T_SX2, (62, 1))):
        for side, place in enumerate(places):
            tab[at + 64 * side : at + 64 * side + 64] = s64[:, place][:, None]
    packed = tab[T_IM : T_IM + 512].reshape(8, 64, 128)
    tab[T_ALPHA : T_ALPHA + 64] = (packed * tab[T_W : T_W + 8, None, :] ** 2).sum(0)
    tab[T_GAMMA : T_GAMMA + 8] = (packed * tab[None, T_SX : T_SX + 64] ** 2).sum(1)
    mat = np.zeros((B_ROWS, 128))
    mat[B_Y : B_Y + 128] = np.kron(np.eye(2), s64)
    order = np.concatenate([np.arange(0, 64, 2), np.arange(1, 64, 2)])
    mat[B_XF : B_XF + 64, :64] = s64[:, order]
    mat[B_XI : B_XI + 64, :64] = s64[order, :]
    mat = mat.astype(np.float32)
    high = mat.astype(jnp.bfloat16)
    low = (mat - high.astype(np.float32)).astype(jnp.bfloat16)
    return tab.astype(np.float32), high, low


S16 = sine(CZ)


def split(v):
    high = v.astype(BF16)
    return high, (v - high.astype(F32)).astype(BF16)


def dot(a, b):
    return jnp.dot(a, b, preferred_element_type=F32)


def dot_right(v, th, tl):
    vh, vl = split(v)
    return dot(vh, th) + (dot(vl, th) + dot(vh, tl))


def dot_left(th, tl, v):
    vh, vl = split(v)
    return dot(th, vh) + (dot(th, vl) + dot(tl, vh))


def kernel(
    state, burn, fmap, tab_h, bh_h, bl_h, out_s, out_p,
    stn, bnn, fld0, fld1, fields, burning, src, ybuf, hat1, hat, prs, resp,
    turns, xg, zsend, zrecv, dsend, drecv, psend, qsend, qrecv, fsend, frecv, psel, tab, bh, bl, idx,
    in_sem, t_sem, send_sem, recv_sem,
):
    g = lax.axis_index("grp")
    m = lax.axis_index("mesh")
    n = lax.axis_size("mesh")
    fine = g == 0
    LOW, HIGH, PARTNER, LOW2, HIGH2, DLOW, DHIGH = range(7)
    back = (HIGH, LOW, PARTNER, HIGH2, LOW2, DHIGH, DLOW)
    has_low, has_high = m > 0, m < n - 1
    exists = (has_low, has_high, None, m > 1, m < n - 2, has_low, has_high)
    steps = (-1, 1, 0, -2, 2, -1, 1)
    where_to = [
        {"grp": 1 - g if to in (PARTNER, DLOW, DHIGH) else g, "mesh": lax.rem(m + n + steps[to], n)}
        for to in range(7)
    ]
    count = 1
    for to in range(7):
        if exists[to] is not None:
            count = count + exists[to].astype(jnp.int32)

    def guarded(condition, action):
        if condition is None:
            action()
        else:
            pl.when(condition)(action)

    loads = [
        pltpu.make_async_copy(state.at[f], stn.at[f], in_sem.at[f]) for f in range(FIELDS)
    ]
    loads.append(pltpu.make_async_copy(burn, bnn, in_sem.at[FIELDS]))
    for copy in loads:
        copy.start()
    table_loads = [
        pltpu.make_async_copy(a, b, t_sem.at[i])
        for i, (a, b) in enumerate(((fmap, idx.at[0]), (tab_h, tab), (bh_h, bh), (bl_h, bl)))
    ]
    for copy in table_loads:
        copy.start()

    def clear(ref, start, size):
        ref[start : start + size, :] = jnp.zeros((size, 128), F32)

    def level(k, f):
        return (f * (CZ + 2 * HALO) + k + HALO) * PLANE

    @pl.when(jnp.logical_not(has_low))
    def _():
        for f in range(FIELDS):
            clear(fld0, level(-2, f), 2 * PLANE)
            clear(fld1, level(-2, f), 2 * PLANE)
        for s in range(SECTIONS):
            clear(prs.at[s], 0, 3 * PLANE)
            clear(zrecv.at[s, 1], 0, PLANE)
            clear(drecv.at[s, 0], 0, 16)
            clear(qrecv.at[s, 1], 0, 8)

    @pl.when(jnp.logical_not(has_high))
    def _():
        for f in range(FIELDS):
            clear(fld0, level(CZ, f), 2 * PLANE)
            clear(fld1, level(CZ, f), 2 * PLANE)
        for s in range(SECTIONS):
            clear(prs.at[s], (CZ + 3) * PLANE, 3 * PLANE)
            clear(zrecv.at[s, 0], 0, PLANE)
            clear(drecv.at[s, 1], 0, 16)
            clear(qrecv.at[s, 2], 0, 8)

    @pl.when(m < 2)
    def _():
        for s in range(SECTIONS):
            clear(zrecv.at[s, 3], 0, PLANE)

    @pl.when(m > n - 3)
    def _():
        for s in range(SECTIONS):
            clear(zrecv.at[s, 2], 0, PLANE)

    barrier = pltpu.get_barrier_semaphore()
    for to in range(7):
        guarded(
            exists[to],
            lambda to=to: pl.semaphore_signal(
                barrier, inc=1, device_id=where_to[to], device_id_type=MESH
            ),
        )

    messages = []

    class Message:
        def __init__(self, to, a, b):
            slot = len(messages)
            messages.append(self)
            self.to = to
            self.copy = pltpu.make_async_remote_copy(
                src_ref=a, dst_ref=b, send_sem=send_sem.at[slot], recv_sem=recv_sem.at[slot],
                device_id=where_to[to], device_id_type=MESH,
            )
            self.sent = False

        def start(self):
            guarded(exists[self.to], self.copy.start)

        def wait_recv(self):
            guarded(exists[back[self.to]], self.copy.wait_recv)

        def wait_send(self):
            if not self.sent:
                self.sent = True
                guarded(exists[self.to], self.copy.wait_send)

    lane = lax.broadcasted_iota(jnp.int32, (PLANE, 128), 1)
    half0 = lane < 64
    y_last = (lane == 63) | (lane == 127)
    y_first = (lane == 0) | (lane == 64)
    half8 = lax.broadcasted_iota(jnp.int32, (8, 128), 1) < 64
    half64 = lax.broadcasted_iota(jnp.int32, (64, 128), 1) < 64
    sub8 = lax.broadcasted_iota(jnp.int32, (8, 128), 0)

    def swap(v):
        return pltpu.roll(v, 64, 1)

    def rows(start, size):
        return pl.ds(pl.multiple_of(start, 8), size)

    def to_layers(load, store):
        for b in range(2):
            for t in range(4):
                tiles = jnp.stack([load(b, pl.ds((t * 8 + i) * 128, 128)) for i in range(8)])
                turned = jnp.swapaxes(tiles, 0, 1)
                for i in range(8):
                    store(b * 8 + i, t * 8, turned[i])

    def to_native(load, store):
        for b in range(2):
            for t in range(4):
                tiles = jnp.stack([load(b * 8 + i, t * 8) for i in range(8)])
                turned = jnp.swapaxes(tiles, 0, 1)
                for i in range(8):
                    store(b, pl.ds((t * 8 + i) * 128, 128), turned[i])

    def own_plane(fld, f):
        at = jnp.where(fine, PLANE - 1, 0)
        tiles = []
        for odd in range(2):
            tile = jnp.zeros((8, 128), F32)
            for r in range(8):
                one = fld[pl.ds(level(2 * r + odd, f) + at, 1), :]
                tile = jnp.where(sub8 == r, jnp.broadcast_to(one, (8, 128)), tile)
            tiles.append(tile)
        even, odd = tiles
        return jnp.where(
            fine, jnp.where(half8, swap(even), odd), jnp.where(half8, even, swap(odd))
        )

    def halo_messages(fld, f):
        return [
            Message(LOW, fld.at[pl.ds(level(0, f), 2 * PLANE)],
                    fld.at[pl.ds(level(CZ, f), 2 * PLANE)]),
            Message(HIGH, fld.at[pl.ds(level(CZ - 2, f), 2 * PLANE)],
                    fld.at[pl.ds(level(-2, f), 2 * PLANE)]),
        ]

    def gather(plane, who=0):
        index = idx[who]
        column = index & 127
        block = index >> 7
        out = jnp.zeros((8, 128), F32)
        for r in range(8):
            one = jnp.broadcast_to(plane[r : r + 1, :], (8, 128))
            out = jnp.where(block == r, jnp.take_along_axis(one, column, axis=1), out)
        return out

    def spread(ghost, base):
        other = swap(ghost)
        even = jnp.where(half8, ghost, other)
        odd = jnp.where(half8, other, ghost)
        zero = jnp.zeros_like(ghost)
        for side in range(2):
            on = fine if side else jnp.logical_not(fine)
            xg[side, pl.ds(base, 8, stride=2), :] = jnp.where(on, even, zero)
            xg[side, pl.ds(base + 1, 8, stride=2), :] = jnp.where(on, odd, zero)

    def x_sides(v, at, slot):
        base = slot * 48
        turned = swap(v)
        turns[base + 8 : base + 40, :] = turned
        turns[base + 7 : base + 8, :] = xg[0, pl.ds(at, 1), :]
        turns[base + 40 : base + 41, :] = xg[1, pl.ds(at, 1), :]
        down = turns[base + 7 : base + 39, :]
        up = turns[base + 9 : base + 41, :]
        return turned, jnp.where(half0, down, up)

    def y_sides(v):
        north = jnp.where(y_last, 0.0, pltpu.roll(v, 127, 1))
        south = jnp.where(y_first, 0.0, pltpu.roll(v, 1, 1))
        return north, south

    XG = 48
    TAIL = XG + FIELDS * 16

    def tendency_plane(fld, k, finish, u=0):
        c = [fld[rows(level(k, f), PLANE), :] for f in range(FIELDS)]
        reaction = burning[rows(k * PLANE, PLANE), :] * c[3] * c[4]
        source = EXPANSION * reaction
        half = jnp.where(half0, 0.5, -0.5)
        cx = c[0] * (half * -COURANT)
        cy = c[1] * (-0.5 * COURANT)
        cz = c[2] * (-COURANT * 2.0 / 3.0)
        cz2 = c[2] * (COURANT / 12.0)
        for f in range(FIELDS):
            above = fld[rows(level(k + 1, f), PLANE), :]
            below = fld[rows(level(k - 1, f), PLANE), :]
            above2 = fld[rows(level(k + 2, f), PLANE), :]
            below2 = fld[rows(level(k - 2, f), PLANE), :]
            inner, outer = x_sides(c[f], XG + f * 16 + k, u * FIELDS + f)
            north, south = y_sides(c[f])
            dx = inner - outer
            dy = north - south
            dz = above - below
            total = (inner + outer) + (north + south) + (above + below)
            change = (DIFFUSION * total + cx * dx) + (cy * dy + cz * dz) + cz2 * (above2 - below2)
            if f == 0:
                source = source - half * dx
            elif f == 1:
                source = source - 0.5 * dy
            elif f == 2:
                source = source - 0.5 * dz
            elif f == 3:
                change = change - reaction
            else:
                change = change - STOICHIOMETRY * reaction
            finish(k, f, c[f] * (1.0 - 6.0 * DIFFUSION) + change)
        src[rows(k * PLANE, PLANE), :] = source

    def z_inverse(spec, into, base):
        @pl.loop(0, 4)
        def _(t):
            v = [spec[rows(c * PLANE + t * 8, 8), :] for c in range(CZ)]
            for k in range(8):
                even = v[0] * F32(S16[0, k])
                odd = v[1] * F32(S16[1, k])
                for c in range(1, 8):
                    even = even + v[2 * c] * F32(S16[2 * c, k])
                    odd = odd + v[2 * c + 1] * F32(S16[2 * c + 1, k])
                into[rows(base + k * PLANE + t * 8, 8), :] = even + odd
                into[rows(base + (15 - k) * PLANE + t * 8, 8), :] = even - odd

    def y_matrix():
        return bh[B_Y : B_Y + 128, :], bl[B_Y : B_Y + 128, :]

    def y_transform(v):
        return dot_right(v, *y_matrix())

    def x_forward(a, b):
        even = jnp.where(half0, a, swap(b))
        odd = jnp.where(half0, swap(a), b)
        v = jnp.concatenate([even, odd], axis=0)
        return dot_left(bh[B_XF : B_XF + 64, :64], bl[B_XF : B_XF + 64, :64], v)

    def transform(first, last):
        pairs = range(first, 8) if last == 0 else range(last)
        if last == 0:
            v = y_transform(src[first * PLANE : (CZ - first) * PLANE, :])
            planes = {k: v[(k - first) * PLANE : (k - first + 1) * PLANE] for k in range(first, CZ - first)}
        else:
            v = y_transform(
                jnp.concatenate(
                    [src[: last * PLANE, :], src[(CZ - last) * PLANE : CZ * PLANE, :]], axis=0
                )
            )
            planes = {k: v[k * PLANE : (k + 1) * PLANE] for k in range(last)}
            for i in range(last):
                planes[CZ - last + i] = v[(last + i) * PLANE : (last + i + 1) * PLANE]
        for k in pairs:
            ybuf[k * 64 : k * 64 + 64, :] = x_forward(planes[k], planes[CZ - 1 - k])

    def x_inverse(v):
        v = dot_left(bh[B_XI : B_XI + 64, :64], bl[B_XI : B_XI + 64, :64], v)
        even, odd = v[:PLANE], v[PLANE:]
        return jnp.where(half0, even, swap(odd)), jnp.where(half0, swap(even), odd)

    def z_plane(v):
        other = swap(v)
        parts = []
        for p in range(8):
            parts.append(tab[T_Z1 + p * 8 : T_Z1 + p * 8 + 8, :] * v[p : p + 1, :])
            parts.append(tab[T_Z2 + p * 8 : T_Z2 + p * 8 + 8, :] * other[p : p + 1, :])
        while len(parts) > 1:
            parts = [a + b for a, b in zip(parts[::2], parts[1::2])]
        return parts[0]

    def side_x(at=T_SX):
        return tab[rows(at + g * 64, 64), :]

    def weight(k, p):
        return tab[T_W + 8 * k + p : T_W + 8 * k + p + 1, :]

    def modes(p):
        return tab[T_IM + p * 64 : T_IM + p * 64 + 64, :]

    def block(ref, p):
        return ref[p * 64 : p * 64 + 64, :]

    def first_of(acc):
        return acc + swap(acc)

    def last_of(acc):
        other = swap(acc)
        return jnp.where(half64, acc - other, other - acc)

    def z_layers(spec, k):
        acc = weight(k, 0) * block(spec, 0)
        for p in range(1, 8):
            acc = acc + weight(k, p) * block(spec, p)
        return acc

    def x_planes(spec, at):
        sx = side_x(at)
        return jnp.concatenate(
            [jnp.sum(sx * block(spec, p), axis=0, keepdims=True) for p in range(8)], axis=0
        )

    def narrow(v):
        return jnp.where(half0, v[:PLANE], v[PLANE:])

    def widen(v):
        other = swap(v)
        return jnp.concatenate(
            [jnp.where(half0, v, other), jnp.where(half0, other, v)], axis=0
        )

    def z_ghosts(below, above):
        return below + jnp.where(half64, above, -above)

    def layer_response(both, ghost):
        acc = tab[T_ALPHA : T_ALPHA + 64, :] * both
        for p in range(8):
            acc = acc + block(resp, p) * ghost[p : p + 1, :]
        return acc

    def plane_response(layer):
        return jnp.concatenate(
            [jnp.sum(block(resp, p) * layer, axis=0, keepdims=True) for p in range(8)], axis=0
        )

    Z_HIGH, Z_LOW, Z_HIGH2, Z_LOW2 = range(4)

    def solve(s):
        own = prs.at[s]
        for r in range(8):
            pairs = []
            for p in range(8):
                v = ybuf[p * 64 + r * 8 : p * 64 + r * 8 + 8, :]
                pairs.append(v + jnp.where(half8, swap(v), -swap(v)))
            for q in range(8):
                parts = [
                    tab[T_ZF + q * 8 + p : T_ZF + q * 8 + p + 1, :] * pairs[p] for p in range(8)
                ]
                while len(parts) > 1:
                    parts = [a + b for a, b in zip(parts[::2], parts[1::2])]
                at = q * 64 + r * 8
                hat1[at : at + 8, :] = parts[0] * tab[T_IM + at : T_IM + at + 8, :]
        acc = z_layers(hat1, 0)
        first, last = first_of(acc), last_of(acc)
        zsend[s, 0] = narrow(first)
        zsend[s, 1] = narrow(last)
        copies = [
            Message(LOW2, zsend.at[s, 0], zrecv.at[s, Z_HIGH2]),
            Message(HIGH2, zsend.at[s, 1], zrecv.at[s, Z_LOW2]),
            Message(LOW, zsend.at[s, 0], zrecv.at[s, Z_HIGH]),
            Message(HIGH, zsend.at[s, 1], zrecv.at[s, Z_LOW]),
        ]
        for copy in copies:
            copy.start()
        plane = z_plane(y_transform(x_planes(hat1, T_SX)))
        dsend[s, 0, 0:8, :] = plane
        dsend[s, 1, 0:8, :] = plane
        dsend[s, 0, 8:16, :] = plane_response(first)
        dsend[s, 1, 8:16, :] = plane_response(last)
        sides = [
            Message(DLOW, dsend.at[s, 0], drecv.at[s, 1]),
            Message(DHIGH, dsend.at[s, 1], drecv.at[s, 0]),
            Message(PARTNER, dsend.at[s, 0, pl.ds(0, 8)], qrecv.at[s, 3]),
        ]
        for copy in sides:
            copy.start()
        if s == 0:
            for f in range(FIELDS):
                fsend[1, f * 8 : f * 8 + 8, :] = own_plane(fld1, f)
            early.append(Message(PARTNER, fsend.at[1], frecv.at[1]))
            for f in range(FIELDS):
                early.extend(halo_messages(fld1, f))
            for copy in early:
                copy.start()
            for copy in maps[1:]:
                copy.wait_recv()
        mine = y_transform(z_plane(gather(plane, 1)))
        mine = tab[T_GAMMA : T_GAMMA + 8, :] * mine
        for copy in sides:
            copy.wait_recv()
        response = drecv[s, 0, 8:16, :] + jnp.where(
            half8, drecv[s, 1, 8:16, :], -drecv[s, 1, 8:16, :]
        )
        partner = qrecv[s, 3] + z_plane(y_transform(response + mine))
        ghost = z_plane(gather(partner))
        ghosts = y_transform(
            jnp.concatenate(
                [
                    z_plane(gather(drecv[s, 0, 0:8, :], 2)),
                    z_plane(gather(drecv[s, 1, 0:8, :], 3)),
                    ghost,
                ],
                axis=0,
            )
        )
        ghost = ghosts[16:24]
        for copy in copies:
            copy.wait_recv()

        def got(slot):
            return zrecv[s, slot]

        above = got(Z_HIGH) + narrow(
            first_of(layer_response(z_ghosts(last, widen(got(Z_HIGH2))), ghosts[8:16]))
        )
        below = got(Z_LOW) + narrow(
            last_of(layer_response(z_ghosts(widen(got(Z_LOW2)), first), ghosts[0:8]))
        )
        above = jnp.where(has_high, above, 0.0)
        below = jnp.where(has_low, below, 0.0)
        both = z_ghosts(widen(below), widen(above))
        sx = side_x()
        for p in range(8):
            extra = weight(0, p) * both + sx * ghost[p : p + 1, :]
            hat[p * 64 : p * 64 + 64, :] = block(hat1, p) + extra * modes(p)
        depth = 3 if s == 0 else 1
        planes = [x_planes(hat, T_SX)]
        if s == 0:
            planes.append(x_planes(hat, T_SX2))
        planes = y_transform(jnp.concatenate(planes, axis=0))
        for i in range(len(planes) // 8):
            qsend[s, i * 8 : i * 8 + 8, :] = z_plane(planes[i * 8 : i * 8 + 8])
        for k in range(depth):
            acc = z_layers(hat, k)
            a, b = x_inverse(jnp.where(half64, first_of(acc), last_of(acc)))
            psend[s, 0, k * PLANE : (k + 1) * PLANE, :] = y_transform(a)
            at = depth - 1 - k
            psend[s, 1, at * PLANE : (at + 1) * PLANE, :] = y_transform(b)
        size = depth * PLANE
        copies = [
            Message(LOW, psend.at[s, 0, pl.ds(0, size)], own.at[pl.ds((CZ + 3) * PLANE, size)]),
            Message(HIGH, psend.at[s, 1, pl.ds(0, size)], own.at[pl.ds((3 - depth) * PLANE, size)]),
        ]
        if s == 0:
            copies += [
                Message(DLOW, qsend.at[s, pl.ds(0, 8)], qrecv.at[s, 2]),
                Message(DHIGH, qsend.at[s, pl.ds(0, 8)], qrecv.at[s, 1]),
                Message(PARTNER, qsend.at[s], psel.at[0]),
            ]
        else:
            copies.append(Message(PARTNER, qsend.at[s, pl.ds(0, 8)], qrecv.at[s, 0]))
        for copy in copies:
            copy.start()
        for p in range(8):
            a, b = x_inverse(block(hat, p))
            ybuf[2 * p * PLANE : (2 * p + 1) * PLANE, :] = a
            ybuf[(2 * p + 1) * PLANE : (2 * p + 2) * PLANE, :] = b
        ybuf[...] = y_transform(ybuf[...])
        z_inverse(ybuf, own, 3 * PLANE)
        return copies

    def correct_plane(s, k, into, at_of, u=0):
        own = prs.at[s]
        p = own[rows((k + 3) * PLANE, PLANE), :]
        above = own[rows((k + 4) * PLANE, PLANE), :]
        below = own[rows((k + 2) * PLANE, PLANE), :]
        inner, outer = x_sides(p, 16 + k, u)
        north, south = y_sides(p)
        half = jnp.where(half0, 0.5, -0.5)
        for f, v in enumerate(
            (half * (inner - outer), 0.5 * (north - south), 0.5 * (above - below))
        ):
            at = rows(at_of(k, f), PLANE)
            into[at, :] = into[at, :] - v

    early = []
    for f in range(FIELDS):
        loads[f].wait()

        def load_state(b, lanes, f=f):
            return stn[f, b * 8 : b * 8 + 8, lanes]

        def store_state(k, r, v, f=f):
            fld0[rows(level(k, f) + r, 8), :] = v

        to_layers(load_state, store_state)
        if f == 0:
            pl.semaphore_wait(barrier, count)
        copies = halo_messages(fld0, f)
        for copy in copies:
            copy.start()
        early.extend(copies)
    for f in range(FIELDS):
        fsend[0, f * 8 : f * 8 + 8, :] = own_plane(fld0, f)
    table_loads[0].wait()
    maps = [
        Message(PARTNER, fsend.at[0], frecv.at[0]),
        Message(PARTNER, idx.at[0], idx.at[1]),
        Message(HIGH, idx.at[0], idx.at[2]),
        Message(LOW, idx.at[0], idx.at[3]),
    ]
    for copy in maps:
        copy.start()
    loads[FIELDS].wait()

    def load_burn(b, lanes):
        return bnn[b * 8 : b * 8 + 8, lanes]

    def store_burn(k, r, v):
        burning[rows(k * PLANE + r, 8), :] = v

    to_layers(load_burn, store_burn)
    for copy in table_loads[1:]:
        copy.wait()
    for p in range(8):
        resp[p * 64 : p * 64 + 64, :] = modes(p) * weight(0, p) * side_x()

    def finish0(k, f, v):
        fld1[rows(level(k, f), PLANE), :] = v

    maps[0].wait_recv()
    for f in range(FIELDS):
        spread(gather(frecv[0, f * 8 : f * 8 + 8, :]), XG + f * 16)

    @pl.loop(0, 6)
    def _(i):
        for u in range(2):
            tendency_plane(fld0, 2 + 2 * i + u, finish0, u)

    transform(2, 0)

    for copy in early:
        copy.wait_recv()

    @pl.loop(0, 2)
    def _(i):
        for u in range(2):
            tendency_plane(fld0, i * (CZ - 2) + u, finish0, u)

    early = []
    transform(0, 2)
    final = solve(0)

    final[4].wait_recv()
    early[0].wait_recv()
    near = psel[0, 0:8, :]
    beside = psel[0, 8:16, :]
    spread(gather(near), 16)
    sides = gather(qsend[0, 0:8, :], 1)
    sign = jnp.where(fine, -0.5, 0.5)
    new0 = frecv[1, 0:8, :] - sign * (sides - beside)
    lane8 = lax.broadcasted_iota(jnp.int32, (8, 128), 1)
    north = jnp.where((lane8 == 63) | (lane8 == 127), 0.0, pltpu.roll(near, 127, 1))
    south = jnp.where((lane8 == 0) | (lane8 == 64), 0.0, pltpu.roll(near, 1, 1))
    new1 = frecv[1, 8:16, :] - 0.5 * (north - south)
    other = swap(near)
    up = jnp.where(sub8 == 7, 0.0, pltpu.roll(other, 7, 0))
    down = jnp.where(sub8 == 0, 0.0, pltpu.roll(other, 1, 0))
    above = jnp.where(half8, other, up)
    below = jnp.where(half8, down, other)
    new2 = frecv[1, 16:24, :] - 0.5 * (above - below)
    for f, v in enumerate((new0, new1, new2, frecv[1, 24:32, :], frecv[1, 32:40, :])):
        spread(gather(v), XG + f * 16)
    for copy in early:
        copy.wait_send()

    @pl.loop(0, 2)
    def _(i):
        for u in range(7):
            correct_plane(0, 1 + 7 * i + u, fld1, level, u)

    def finish1(k, f, v):
        start = fld0[rows(level(k, f), PLANE), :]
        fields[rows((k * FIELDS + f) * PLANE, PLANE), :] = 0.5 * (start + v)

    @pl.loop(0, 5)
    def _(i):
        for u in range(2):
            tendency_plane(fld1, 3 + 2 * i + u, finish1, u)

    transform(3, 0)

    for copy in final[:4] + early[1:]:
        copy.wait_recv()
    spread(gather(qrecv[0, 1], 2), 0)
    spread(gather(qrecv[0, 2], 3), 32)
    over = jnp.broadcast_to(swap(qrecv[0, 2])[0:1, :], (8, 128))
    under = jnp.broadcast_to(swap(qrecv[0, 1])[7:8, :], (8, 128))
    rest = jnp.where(
        half8,
        jnp.where(sub8 == 0, 0.5 * under, 0.0),
        jnp.where(sub8 == 7, -0.5 * over, 0.0),
    )
    spread(gather(rest), TAIL)
    spread(gather(new2 + rest), XG + 2 * 16)

    for u in range(2):
        correct_plane(0, u * (CZ - 1), fld1, level, u)

    @pl.when(has_low)
    def _():
        for u in range(2):
            correct_plane(0, u - 2, fld1, level, u)

    @pl.when(has_high)
    def _():
        for u in range(2):
            correct_plane(0, CZ + u, fld1, level, u)

    for k in range(3, CZ - 3):
        west, east = xg[0, pl.ds(TAIL + k, 1), :], xg[1, pl.ds(TAIL + k, 1), :]
        at = jnp.where(fine, PLANE - 1, 0)
        c = fld1[pl.ds(level(k, 0) + at, 1), :]
        add = 0.5 * (DIFFUSION * (east + west) - (0.5 * COURANT) * c * (east - west))
        lanes = lax.broadcasted_iota(jnp.int32, (1, 128), 1)
        here = jnp.where(fine, lanes, 127 - lanes) >= 64
        row_at = pl.ds((k * FIELDS + 2) * PLANE + at, 1)
        fields[row_at, :] = fields[row_at, :] + jnp.where(here, add, 0.0)

    @pl.loop(0, 2)
    def _(i):
        for u in range(3):
            tendency_plane(fld1, i * (CZ - 3) + u, finish1, u)

    transform(0, 3)
    final = solve(1)
    final[2].wait_recv()
    spread(gather(qrecv[1, 0]), 16)

    def place(k, f):
        return (k * FIELDS + f) * PLANE

    @pl.loop(0, 2)
    def _(i):
        for u in range(7):
            correct_plane(1, 1 + 7 * i + u, fields, place, u)

    def store_head(b, lanes, v):
        out_p[b * 8 : b * 8 + 8, lanes] = v

    to_native(lambda k, r: prs[1, rows((k + 3) * PLANE + r, 8), :], store_head)

    def put_field(f):
        def load_field(k, r):
            return fields[rows(place(k, f) + r, 8), :]

        def store_field(b, lanes, v):
            out_s[f, b * 8 : b * 8 + 8, lanes] = v

        to_native(load_field, store_field)

    for f in range(3, FIELDS):
        put_field(f)
    for copy in final[:2]:
        copy.wait_recv()

    for u in range(2):
        correct_plane(1, u * (CZ - 1), fields, place, u)

    for f in range(3):
        put_field(f)
    for copy in messages:
        copy.wait_send()


def finish_kernel(fields, head, out_s, out_p, sems):
    copies = [
        pltpu.make_async_copy(fields, out_s, sems.at[0]),
        pltpu.make_async_copy(head, out_p, sems.at[1]),
    ]
    for copy in copies:
        copy.start()
    for copy in copies:
        copy.wait()


def write_out(fields, head):
    hbm = pl.BlockSpec(memory_space=pltpu.HBM)
    vmem = pl.BlockSpec(memory_space=pltpu.VMEM)
    return pl.pallas_call(
        finish_kernel,
        out_shape=(
            jax.ShapeDtypeStruct(fields.shape, F32),
            jax.ShapeDtypeStruct(head.shape, F32),
        ),
        in_specs=[vmem, vmem],
        out_specs=(hbm, hbm),
        scratch_shapes=[pltpu.SemaphoreType.DMA((2,))],
        compiler_params=pltpu.CompilerParams(vmem_limit_bytes=1 << 20),
        name="write_out",
    )(fields, head)


def step(state, burn, fmap):
    hbm = pl.BlockSpec(memory_space=pltpu.HBM)
    vmem = pl.BlockSpec(memory_space=pltpu.VMEM)
    tab, bh, bl = tables()
    vm = pltpu.VMEM
    layers = (CZ + 2 * HALO) * LEVEL
    return pl.pallas_call(
        kernel,
        out_shape=(
            jax.ShapeDtypeStruct((FIELDS, CZ, NX * NY), F32),
            jax.ShapeDtypeStruct((CZ, NX * NY), F32),
        ),
        in_specs=[hbm] * 6,
        out_specs=(vmem, vmem),
        scratch_shapes=[
            vm((FIELDS, CZ, NX * NY), F32),
            vm((CZ, NX * NY), F32),
            vm((layers, 128), F32),
            vm((layers, 128), F32),
            vm((CZ * LEVEL, 128), F32),
            vm((CZ * PLANE, 128), F32),
            vm((CZ * PLANE, 128), F32),
            vm((CZ * PLANE, 128), F32),
            vm((CZ * PLANE, 128), F32),
            vm((CZ * PLANE, 128), F32),
            vm((SECTIONS, (CZ + 6) * PLANE, 128), F32),
            vm((512, 128), F32),
            vm((3 * FIELDS * 48, 128), F32),
            vm((2, 64 + FIELDS * 16, 128), F32),
            vm((SECTIONS, 2, PLANE, 128), F32),
            vm((SECTIONS, 4, PLANE, 128), F32),
            vm((SECTIONS, 2, 16, 128), F32),
            vm((SECTIONS, 2, 16, 128), F32),
            vm((SECTIONS, 2, 3 * PLANE, 128), F32),
            vm((SECTIONS, 16, 128), F32),
            vm((SECTIONS, 4, 8, 128), F32),
            vm((SECTIONS, FIELDS * 8, 128), F32),
            vm((SECTIONS, FIELDS * 8, 128), F32),
            vm((1, 16, 128), F32),
            vm((T_ROWS, 128), F32),
            vm((B_ROWS, 128), BF16),
            vm((B_ROWS, 128), BF16),
            vm((4, 8, 128), jnp.int32),
            pltpu.SemaphoreType.DMA((FIELDS + 1,)),
            pltpu.SemaphoreType.DMA((4,)),
            pltpu.SemaphoreType.DMA((48,)),
            pltpu.SemaphoreType.DMA((48,)),
        ],
        compiler_params=pltpu.CompilerParams(
            collective_id=0, has_side_effects=True, vmem_limit_bytes=40 << 20
        ),
        name="fire_step",
    )(*[pltpu.with_memory_space_constraint(v, pltpu.HBM) for v in (state, burn, fmap, jnp.asarray(tab), jnp.asarray(bh), jnp.asarray(bl))])


def shards(state, burn_rate, face_map):
    fields, head = write_out(*step(state[0], burn_rate[0], face_map.reshape(8, 128)))
    return fields[None], head[None]


def solution(mesh):
    placed = (P("grp", None, "mesh", None), P("grp", "mesh", None), P("grp", "mesh", None))
    return jax.shard_map(
        shards,
        mesh=mesh,
        in_specs=placed,
        out_specs=(P("grp", None, "mesh", None), P("grp", "mesh", None)),
        check_vma=False,
    )
```

```python
import math

import jax
import jax.numpy as jnp
import numpy as np
from jax import lax
from jax.experimental import pallas as pl
from jax.experimental.pallas import tpu as pltpu
from jax.sharding import PartitionSpec as P

NX = 64
NY = 64
CZ = 16
FIELDS = 5
SECTIONS = 2
ITERS = 3
COURANT = 0.1
DIFFUSION = 0.05
STOICHIOMETRY = 2.0
EXPANSION = 1.0

PLANE = 32
LEVEL = FIELDS * PLANE
HALO = 2
MESH = pl.DeviceIdType.MESH
F32 = jnp.float32
BF16 = jnp.bfloat16


def sine(n):
    i = np.arange(n, dtype=np.float64) + 1.0
    return np.sin(np.pi * i[:, None] * i[None, :] / (n + 1)) * math.sqrt(2.0 / (n + 1))


def eigen(n):
    i = np.arange(n, dtype=np.float64) + 1.0
    return 2.0 - 2.0 * np.cos(np.pi * i / (n + 1))


T_IM = 0
T_Z1 = 512
T_Z2 = 576
T_W = 640
T_GAMMA = 664
T_ALPHA = 672
T_SX = 736
T_SX2 = 864
T_ZF = 992
T_ROWS = 1056
B_Y = 0
B_XF = 128
B_XI = 192
B_ROWS = 256


def tables():
    s16, s64 = sine(CZ), sine(NX)
    tab = np.zeros((T_ROWS, 128))
    modes = eigen(CZ)[:, None, None] + eigen(NX)[None, :, None] + eigen(NY)[None, None, :]
    inv = 1.0 / modes
    tab[T_IM : T_IM + 512] = (
        inv.reshape(8, 2, 64, 64).transpose(0, 2, 1, 3).reshape(512, 128)
    )
    for p in range(8):
        for h in range(2):
            lanes = slice(64 * h, 64 * h + 64)
            for r in range(8):
                tab[T_Z1 + p * 8 + r, lanes] = s16[2 * p + h, 2 * r + h]
                tab[T_Z2 + p * 8 + r, lanes] = s16[2 * p + 1 - h, 2 * r + h]
            for k in range(8):
                tab[T_ZF + p * 8 + k, lanes] = s16[2 * p + h, k] * (-1.0) ** h
            for k in range(3):
                tab[T_W + 8 * k + p, lanes] = s16[2 * p + h, k]
    for at, places in ((T_SX, (63, 0)), (T_SX2, (62, 1))):
        for side, place in enumerate(places):
            tab[at + 64 * side : at + 64 * side + 64] = s64[:, place][:, None]
    packed = tab[T_IM : T_IM + 512].reshape(8, 64, 128)
    tab[T_ALPHA : T_ALPHA + 64] = (packed * tab[T_W : T_W + 8, None, :] ** 2).sum(0)
    tab[T_GAMMA : T_GAMMA + 8] = (packed * tab[None, T_SX : T_SX + 64] ** 2).sum(1)
    mat = np.zeros((B_ROWS, 128))
    mat[B_Y : B_Y + 128] = np.kron(np.eye(2), s64)
    order = np.concatenate([np.arange(0, 64, 2), np.arange(1, 64, 2)])
    mat[B_XF : B_XF + 64, :64] = s64[:, order]
    mat[B_XI : B_XI + 64, :64] = s64[order, :]
    mat = mat.astype(np.float32)
    high = mat.astype(jnp.bfloat16)
    low = (mat - high.astype(np.float32)).astype(jnp.bfloat16)
    return tab.astype(np.float32), high, low


S16 = sine(CZ)


def split(v):
    high = v.astype(BF16)
    return high, (v - high.astype(F32)).astype(BF16)


def dot(a, b):
    return jnp.dot(a, b, preferred_element_type=F32)


def dot_right(v, th, tl):
    vh, vl = split(v)
    return dot(vh, th) + (dot(vl, th) + dot(vh, tl))


def dot_left(th, tl, v):
    vh, vl = split(v)
    return dot(th, vh) + (dot(th, vl) + dot(tl, vh))


def kernel(
    state, burn, fmap, tab_h, bh_h, bl_h, out_s, out_p,
    stn, bnn, fld0, fld1, fields, burning, src, ybuf, hat1, hat, prs, resp,
    turns, xg, zsend, zrecv, dsend, drecv, psend, qsend, qrecv, fsend, frecv, psel, tab, bh, bl, idx,
    in_sem, t_sem, send_sem, recv_sem,
):
    g = lax.axis_index("grp")
    m = lax.axis_index("mesh")
    n = lax.axis_size("mesh")
    fine = g == 0
    LOW, HIGH, PARTNER, LOW2, HIGH2, DLOW, DHIGH = range(7)
    back = (HIGH, LOW, PARTNER, HIGH2, LOW2, DHIGH, DLOW)
    has_low, has_high = m > 0, m < n - 1
    exists = (has_low, has_high, None, m > 1, m < n - 2, has_low, has_high)
    steps = (-1, 1, 0, -2, 2, -1, 1)
    where_to = [
        {"grp": 1 - g if to in (PARTNER, DLOW, DHIGH) else g, "mesh": lax.rem(m + n + steps[to], n)}
        for to in range(7)
    ]
    count = 1
    for to in range(7):
        if exists[to] is not None:
            count = count + exists[to].astype(jnp.int32)

    def guarded(condition, action):
        if condition is None:
            action()
        else:
            pl.when(condition)(action)

    loads = [
        pltpu.make_async_copy(state.at[f], stn.at[f], in_sem.at[f]) for f in range(FIELDS)
    ]
    loads.append(pltpu.make_async_copy(burn, bnn, in_sem.at[FIELDS]))
    for copy in loads:
        copy.start()
    table_loads = [
        pltpu.make_async_copy(a, b, t_sem.at[i])
        for i, (a, b) in enumerate(((fmap, idx.at[0]), (tab_h, tab), (bh_h, bh), (bl_h, bl)))
    ]
    for copy in table_loads:
        copy.start()

    def clear(ref, start, size):
        ref[start : start + size, :] = jnp.zeros((size, 128), F32)

    def level(k, f):
        return (f * (CZ + 2 * HALO) + k + HALO) * PLANE

    @pl.when(jnp.logical_not(has_low))
    def _():
        for f in range(FIELDS):
            clear(fld0, level(-2, f), 2 * PLANE)
            clear(fld1, level(-2, f), 2 * PLANE)
        for s in range(SECTIONS):
            clear(prs.at[s], 0, 3 * PLANE)
            clear(zrecv.at[s, 1], 0, PLANE)
            clear(drecv.at[s, 0], 0, 16)
            clear(qrecv.at[s, 1], 0, 8)

    @pl.when(jnp.logical_not(has_high))
    def _():
        for f in range(FIELDS):
            clear(fld0, level(CZ, f), 2 * PLANE)
            clear(fld1, level(CZ, f), 2 * PLANE)
        for s in range(SECTIONS):
            clear(prs.at[s], (CZ + 3) * PLANE, 3 * PLANE)
            clear(zrecv.at[s, 0], 0, PLANE)
            clear(drecv.at[s, 1], 0, 16)
            clear(qrecv.at[s, 2], 0, 8)

    @pl.when(m < 2)
    def _():
        for s in range(SECTIONS):
            clear(zrecv.at[s, 3], 0, PLANE)

    @pl.when(m > n - 3)
    def _():
        for s in range(SECTIONS):
            clear(zrecv.at[s, 2], 0, PLANE)

    barrier = pltpu.get_barrier_semaphore()
    for to in range(7):
        guarded(
            exists[to],
            lambda to=to: pl.semaphore_signal(
                barrier, inc=1, device_id=where_to[to], device_id_type=MESH
            ),
        )

    messages = []

    class Message:
        def __init__(self, to, a, b):
            slot = len(messages)
            messages.append(self)
            self.to = to
            self.copy = pltpu.make_async_remote_copy(
                src_ref=a, dst_ref=b, send_sem=send_sem.at[slot], recv_sem=recv_sem.at[slot],
                device_id=where_to[to], device_id_type=MESH,
            )
            self.sent = False

        def start(self):
            guarded(exists[self.to], self.copy.start)

        def wait_recv(self):
            guarded(exists[back[self.to]], self.copy.wait_recv)

        def wait_send(self):
            if not self.sent:
                self.sent = True
                guarded(exists[self.to], self.copy.wait_send)

    lane = lax.broadcasted_iota(jnp.int32, (PLANE, 128), 1)
    half0 = lane < 64
    y_last = (lane == 63) | (lane == 127)
    y_first = (lane == 0) | (lane == 64)
    half8 = lax.broadcasted_iota(jnp.int32, (8, 128), 1) < 64
    half64 = lax.broadcasted_iota(jnp.int32, (64, 128), 1) < 64
    sub8 = lax.broadcasted_iota(jnp.int32, (8, 128), 0)

    def swap(v):
        return pltpu.roll(v, 64, 1)

    def rows(start, size):
        return pl.ds(pl.multiple_of(start, 8), size)

    def to_layers(load, store):
        for b in range(2):
            for t in range(4):
                tiles = jnp.stack([load(b, pl.ds((t * 8 + i) * 128, 128)) for i in range(8)])
                turned = jnp.swapaxes(tiles, 0, 1)
                for i in range(8):
                    store(b * 8 + i, t * 8, turned[i])

    def to_native(load, store):
        for b in range(2):
            for t in range(4):
                tiles = jnp.stack([load(b * 8 + i, t * 8) for i in range(8)])
                turned = jnp.swapaxes(tiles, 0, 1)
                for i in range(8):
                    store(b, pl.ds((t * 8 + i) * 128, 128), turned[i])

    def own_plane(fld, f):
        at = jnp.where(fine, PLANE - 1, 0)
        tiles = []
        for odd in range(2):
            tile = jnp.zeros((8, 128), F32)
            for r in range(8):
                one = fld[pl.ds(level(2 * r + odd, f) + at, 1), :]
                tile = jnp.where(sub8 == r, jnp.broadcast_to(one, (8, 128)), tile)
            tiles.append(tile)
        even, odd = tiles
        return jnp.where(
            fine, jnp.where(half8, swap(even), odd), jnp.where(half8, even, swap(odd))
        )

    def halo_messages(fld, f):
        return [
            Message(LOW, fld.at[pl.ds(level(0, f), 2 * PLANE)],
                    fld.at[pl.ds(level(CZ, f), 2 * PLANE)]),
            Message(HIGH, fld.at[pl.ds(level(CZ - 2, f), 2 * PLANE)],
                    fld.at[pl.ds(level(-2, f), 2 * PLANE)]),
        ]

    def gather(plane, who=0):
        index = idx[who]
        column = index & 127
        block = index >> 7
        out = jnp.zeros((8, 128), F32)
        for r in range(8):
            one = jnp.broadcast_to(plane[r : r + 1, :], (8, 128))
            out = jnp.where(block == r, jnp.take_along_axis(one, column, axis=1), out)
        return out

    def spread(ghost, base):
        other = swap(ghost)
        even = jnp.where(half8, ghost, other)
        odd = jnp.where(half8, other, ghost)
        zero = jnp.zeros_like(ghost)
        for side in range(2):
            on = fine if side else jnp.logical_not(fine)
            xg[side, pl.ds(base, 8, stride=2), :] = jnp.where(on, even, zero)
            xg[side, pl.ds(base + 1, 8, stride=2), :] = jnp.where(on, odd, zero)

    def x_sides(v, at, slot):
        base = slot * 48
        turned = swap(v)
        turns[base + 8 : base + 40, :] = turned
        turns[base + 7 : base + 8, :] = xg[0, pl.ds(at, 1), :]
        turns[base + 40 : base + 41, :] = xg[1, pl.ds(at, 1), :]
        down = turns[base + 7 : base + 39, :]
        up = turns[base + 9 : base + 41, :]
        return turned, jnp.where(half0, down, up)

    def y_sides(v):
        north = jnp.where(y_last, 0.0, pltpu.roll(v, 127, 1))
        south = jnp.where(y_first, 0.0, pltpu.roll(v, 1, 1))
        return north, south

    XG = 48
    TAIL = XG + FIELDS * 16

    def tendency_plane(fld, k, finish, u=0):
        c = [fld[rows(level(k, f), PLANE), :] for f in range(FIELDS)]
        reaction = burning[rows(k * PLANE, PLANE), :] * c[3] * c[4]
        source = EXPANSION * reaction
        half = jnp.where(half0, 0.5, -0.5)
        cx = c[0] * (half * -COURANT)
        cy = c[1] * (-0.5 * COURANT)
        cz = c[2] * (-COURANT * 2.0 / 3.0)
        cz2 = c[2] * (COURANT / 12.0)
        for f in range(FIELDS):
            above = fld[rows(level(k + 1, f), PLANE), :]
            below = fld[rows(level(k - 1, f), PLANE), :]
            above2 = fld[rows(level(k + 2, f), PLANE), :]
            below2 = fld[rows(level(k - 2, f), PLANE), :]
            inner, outer = x_sides(c[f], XG + f * 16 + k, u * FIELDS + f)
            north, south = y_sides(c[f])
            dx = inner - outer
            dy = north - south
            dz = above - below
            total = (inner + outer) + (north + south) + (above + below)
            change = (DIFFUSION * total + cx * dx) + (cy * dy + cz * dz) + cz2 * (above2 - below2)
            if f == 0:
                source = source - half * dx
            elif f == 1:
                source = source - 0.5 * dy
            elif f == 2:
                source = source - 0.5 * dz
            elif f == 3:
                change = change - reaction
            else:
                change = change - STOICHIOMETRY * reaction
            finish(k, f, c[f] * (1.0 - 6.0 * DIFFUSION) + change)
        src[rows(k * PLANE, PLANE), :] = source

    def z_inverse(spec, into, base):
        @pl.loop(0, 4)
        def _(t):
            v = [spec[rows(c * PLANE + t * 8, 8), :] for c in range(CZ)]
            for k in range(8):
                even = v[0] * F32(S16[0, k])
                odd = v[1] * F32(S16[1, k])
                for c in range(1, 8):
                    even = even + v[2 * c] * F32(S16[2 * c, k])
                    odd = odd + v[2 * c + 1] * F32(S16[2 * c + 1, k])
                into[rows(base + k * PLANE + t * 8, 8), :] = even + odd
                into[rows(base + (15 - k) * PLANE + t * 8, 8), :] = even - odd

    def y_matrix():
        return bh[B_Y : B_Y + 128, :], bl[B_Y : B_Y + 128, :]

    def y_transform(v):
        return dot_right(v, *y_matrix())

    def x_forward(a, b):
        even = jnp.where(half0, a, swap(b))
        odd = jnp.where(half0, swap(a), b)
        v = jnp.concatenate([even, odd], axis=0)
        return dot_left(bh[B_XF : B_XF + 64, :64], bl[B_XF : B_XF + 64, :64], v)

    def transform(first, last):
        pairs = range(first, 8) if last == 0 else range(last)
        if last == 0:
            v = y_transform(src[first * PLANE : (CZ - first) * PLANE, :])
            planes = {k: v[(k - first) * PLANE : (k - first + 1) * PLANE] for k in range(first, CZ - first)}
        else:
            v = y_transform(
                jnp.concatenate(
                    [src[: last * PLANE, :], src[(CZ - last) * PLANE : CZ * PLANE, :]], axis=0
                )
            )
            planes = {k: v[k * PLANE : (k + 1) * PLANE] for k in range(last)}
            for i in range(last):
                planes[CZ - last + i] = v[(last + i) * PLANE : (last + i + 1) * PLANE]
        for k in pairs:
            ybuf[k * 64 : k * 64 + 64, :] = x_forward(planes[k], planes[CZ - 1 - k])

    def x_inverse(v):
        v = dot_left(bh[B_XI : B_XI + 64, :64], bl[B_XI : B_XI + 64, :64], v)
        even, odd = v[:PLANE], v[PLANE:]
        return jnp.where(half0, even, swap(odd)), jnp.where(half0, swap(even), odd)

    def z_plane(v):
        other = swap(v)
        parts = []
        for p in range(8):
            parts.append(tab[T_Z1 + p * 8 : T_Z1 + p * 8 + 8, :] * v[p : p + 1, :])
            parts.append(tab[T_Z2 + p * 8 : T_Z2 + p * 8 + 8, :] * other[p : p + 1, :])
        while len(parts) > 1:
            parts = [a + b for a, b in zip(parts[::2], parts[1::2])]
        return parts[0]

    def side_x(at=T_SX):
        return tab[rows(at + g * 64, 64), :]

    def weight(k, p):
        return tab[T_W + 8 * k + p : T_W + 8 * k + p + 1, :]

    def modes(p):
        return tab[T_IM + p * 64 : T_IM + p * 64 + 64, :]

    def block(ref, p):
        return ref[p * 64 : p * 64 + 64, :]

    def first_of(acc):
        return acc + swap(acc)

    def last_of(acc):
        other = swap(acc)
        return jnp.where(half64, acc - other, other - acc)

    def z_layers(spec, k):
        acc = weight(k, 0) * block(spec, 0)
        for p in range(1, 8):
            acc = acc + weight(k, p) * block(spec, p)
        return acc

    def x_planes(spec, at):
        sx = side_x(at)
        return jnp.concatenate(
            [jnp.sum(sx * block(spec, p), axis=0, keepdims=True) for p in range(8)], axis=0
        )

    def narrow(v):
        return jnp.where(half0, v[:PLANE], v[PLANE:])

    def widen(v):
        other = swap(v)
        return jnp.concatenate(
            [jnp.where(half0, v, other), jnp.where(half0, other, v)], axis=0
        )

    def z_ghosts(below, above):
        return below + jnp.where(half64, above, -above)

    def layer_response(both, ghost):
        acc = tab[T_ALPHA : T_ALPHA + 64, :] * both
        for p in range(8):
            acc = acc + block(resp, p) * ghost[p : p + 1, :]
        return acc

    def plane_response(layer):
        return jnp.concatenate(
            [jnp.sum(block(resp, p) * layer, axis=0, keepdims=True) for p in range(8)], axis=0
        )

    Z_HIGH, Z_LOW, Z_HIGH2, Z_LOW2 = range(4)

    def solve(s):
        own = prs.at[s]
        for r in range(8):
            pairs = []
            for p in range(8):
                v = ybuf[p * 64 + r * 8 : p * 64 + r * 8 + 8, :]
                pairs.append(v + jnp.where(half8, swap(v), -swap(v)))
            for q in range(8):
                parts = [
                    tab[T_ZF + q * 8 + p : T_ZF + q * 8 + p + 1, :] * pairs[p] for p in range(8)
                ]
                while len(parts) > 1:
                    parts = [a + b for a, b in zip(parts[::2], parts[1::2])]
                at = q * 64 + r * 8
                hat1[at : at + 8, :] = parts[0] * tab[T_IM + at : T_IM + at + 8, :]
        acc = z_layers(hat1, 0)
        first, last = first_of(acc), last_of(acc)
        zsend[s, 0] = narrow(first)
        zsend[s, 1] = narrow(last)
        copies = [
            Message(LOW2, zsend.at[s, 0], zrecv.at[s, Z_HIGH2]),
            Message(HIGH2, zsend.at[s, 1], zrecv.at[s, Z_LOW2]),
            Message(LOW, zsend.at[s, 0], zrecv.at[s, Z_HIGH]),
            Message(HIGH, zsend.at[s, 1], zrecv.at[s, Z_LOW]),
        ]
        for copy in copies:
            copy.start()
        start = x_planes(hat1, T_SX)
        plane = z_plane(y_transform(start))
        dsend[s, 0, 0:8, :] = plane
        dsend[s, 1, 0:8, :] = plane
        dsend[s, 0, 8:16, :] = plane_response(first)
        dsend[s, 1, 8:16, :] = plane_response(last)
        sides = [
            Message(DLOW, dsend.at[s, 0], drecv.at[s, 1]),
            Message(DHIGH, dsend.at[s, 1], drecv.at[s, 0]),
            Message(PARTNER, dsend.at[s, 0, pl.ds(0, 8)], qrecv.at[s, 3]),
        ]
        for copy in sides:
            copy.start()
        if s == 0:
            for f in range(FIELDS):
                fsend[1, f * 8 : f * 8 + 8, :] = own_plane(fld1, f)
            early.append(Message(PARTNER, fsend.at[1], frecv.at[1]))
            for f in range(FIELDS):
                early.extend(halo_messages(fld1, f))
            for copy in early:
                copy.start()
            for copy in maps[1:]:
                copy.wait_recv()
        mine = y_transform(z_plane(gather(plane, 1)))
        mine = tab[T_GAMMA : T_GAMMA + 8, :] * mine
        for copy in sides:
            copy.wait_recv()
        response = drecv[s, 0, 8:16, :] + jnp.where(
            half8, drecv[s, 1, 8:16, :], -drecv[s, 1, 8:16, :]
        )
        partner = qrecv[s, 3] + z_plane(y_transform(response + mine))
        ghost = z_plane(gather(partner))
        ghosts = y_transform(
            jnp.concatenate(
                [
                    z_plane(gather(drecv[s, 0, 0:8, :], 2)),
                    z_plane(gather(drecv[s, 1, 0:8, :], 3)),
                    ghost,
                ],
                axis=0,
            )
        )
        ghost = ghosts[16:24]
        for copy in copies:
            copy.wait_recv()

        def got(slot):
            return zrecv[s, slot]

        above = got(Z_HIGH) + narrow(
            first_of(layer_response(z_ghosts(last, widen(got(Z_HIGH2))), ghosts[8:16]))
        )
        below = got(Z_LOW) + narrow(
            last_of(layer_response(z_ghosts(widen(got(Z_LOW2)), first), ghosts[0:8]))
        )
        above = jnp.where(has_high, above, 0.0)
        below = jnp.where(has_low, below, 0.0)
        both = z_ghosts(widen(below), widen(above))
        depth = 3 if s == 0 else 1
        size = depth * PLANE

        def spectrum():
            sx = side_x()
            for p in range(8):
                extra = weight(0, p) * both + sx * ghost[p : p + 1, :]
                hat[p * 64 : p * 64 + 64, :] = block(hat1, p) + extra * modes(p)

        def layers_out(k, acc):
            a, b = x_inverse(jnp.where(half64, first_of(acc), last_of(acc)))
            psend[s, 0, k * PLANE : (k + 1) * PLANE, :] = y_transform(a)
            at = depth - 1 - k
            psend[s, 1, at * PLANE : (at + 1) * PLANE, :] = y_transform(b)

        stack = [
            Message(LOW, psend.at[s, 0, pl.ds(0, size)], own.at[pl.ds((CZ + 3) * PLANE, size)]),
            Message(HIGH, psend.at[s, 1, pl.ds(0, size)], own.at[pl.ds((3 - depth) * PLANE, size)]),
        ]
        if s == 0:
            spectrum()
            planes = y_transform(
                jnp.concatenate([x_planes(hat, T_SX), x_planes(hat, T_SX2)], axis=0)
            )
            for i in range(2):
                qsend[s, i * 8 : i * 8 + 8, :] = z_plane(planes[i * 8 : i * 8 + 8])
            copies = [
                Message(DLOW, qsend.at[s, pl.ds(0, 8)], qrecv.at[s, 2]),
                Message(DHIGH, qsend.at[s, pl.ds(0, 8)], qrecv.at[s, 1]),
                Message(PARTNER, qsend.at[s], psel.at[0]),
            ]
            for copy in copies:
                copy.start()
            for k in range(depth):
                layers_out(k, z_layers(hat, k))
            for copy in stack:
                copy.start()
        else:
            layers_out(0, acc + layer_response(both, ghost))
            for copy in stack:
                copy.start()
            plane = start + plane_response(both) + tab[T_GAMMA : T_GAMMA + 8, :] * ghost
            qsend[s, 0:8, :] = z_plane(y_transform(plane))
            copies = [Message(PARTNER, qsend.at[s, pl.ds(0, 8)], qrecv.at[s, 0])]
            for copy in copies:
                copy.start()
            spectrum()
        copies = stack + copies
        for p in range(8):
            a, b = x_inverse(block(hat, p))
            ybuf[2 * p * PLANE : (2 * p + 1) * PLANE, :] = a
            ybuf[(2 * p + 1) * PLANE : (2 * p + 2) * PLANE, :] = b
        ybuf[...] = y_transform(ybuf[...])
        z_inverse(ybuf, own, 3 * PLANE)
        return copies

    def correct_z(s, k, into, at_of):
        own = prs.at[s]
        above = own[rows((k + 4) * PLANE, PLANE), :]
        below = own[rows((k + 2) * PLANE, PLANE), :]
        at = rows(at_of(k, 2), PLANE)
        into[at, :] = into[at, :] - 0.5 * (above - below)

    def correct_plane(s, k, into, at_of, u=0, along_z=True):
        p = prs[s, rows((k + 3) * PLANE, PLANE), :]
        inner, outer = x_sides(p, 16 + k, u)
        north, south = y_sides(p)
        half = jnp.where(half0, 0.5, -0.5)
        for f, v in enumerate((half * (inner - outer), 0.5 * (north - south))):
            at = rows(at_of(k, f), PLANE)
            into[at, :] = into[at, :] - v
        if along_z:
            correct_z(s, k, into, at_of)

    early = []
    for f in range(FIELDS):
        loads[f].wait()

        def load_state(b, lanes, f=f):
            return stn[f, b * 8 : b * 8 + 8, lanes]

        def store_state(k, r, v, f=f):
            fld0[rows(level(k, f) + r, 8), :] = v

        to_layers(load_state, store_state)
        if f == 0:
            pl.semaphore_wait(barrier, count)
        copies = halo_messages(fld0, f)
        for copy in copies:
            copy.start()
        early.extend(copies)
    for f in range(FIELDS):
        fsend[0, f * 8 : f * 8 + 8, :] = own_plane(fld0, f)
    table_loads[0].wait()
    maps = [
        Message(PARTNER, fsend.at[0], frecv.at[0]),
        Message(PARTNER, idx.at[0], idx.at[1]),
        Message(HIGH, idx.at[0], idx.at[2]),
        Message(LOW, idx.at[0], idx.at[3]),
    ]
    for copy in maps:
        copy.start()
    loads[FIELDS].wait()

    def load_burn(b, lanes):
        return bnn[b * 8 : b * 8 + 8, lanes]

    def store_burn(k, r, v):
        burning[rows(k * PLANE + r, 8), :] = v

    to_layers(load_burn, store_burn)
    for copy in table_loads[1:]:
        copy.wait()
    for p in range(8):
        resp[p * 64 : p * 64 + 64, :] = modes(p) * weight(0, p) * side_x()

    def finish0(k, f, v):
        fld1[rows(level(k, f), PLANE), :] = v

    maps[0].wait_recv()
    for f in range(FIELDS):
        spread(gather(frecv[0, f * 8 : f * 8 + 8, :]), XG + f * 16)

    @pl.loop(0, 6)
    def _(i):
        for u in range(2):
            tendency_plane(fld0, 2 + 2 * i + u, finish0, u)

    transform(2, 0)

    for copy in early:
        copy.wait_recv()

    @pl.loop(0, 2)
    def _(i):
        for u in range(2):
            tendency_plane(fld0, i * (CZ - 2) + u, finish0, u)

    early = []
    transform(0, 2)
    final = solve(0)

    final[4].wait_recv()
    early[0].wait_recv()
    near = psel[0, 0:8, :]
    beside = psel[0, 8:16, :]
    spread(gather(near), 16)
    sides = gather(qsend[0, 0:8, :], 1)
    sign = jnp.where(fine, -0.5, 0.5)
    new0 = frecv[1, 0:8, :] - sign * (sides - beside)
    lane8 = lax.broadcasted_iota(jnp.int32, (8, 128), 1)
    north = jnp.where((lane8 == 63) | (lane8 == 127), 0.0, pltpu.roll(near, 127, 1))
    south = jnp.where((lane8 == 0) | (lane8 == 64), 0.0, pltpu.roll(near, 1, 1))
    new1 = frecv[1, 8:16, :] - 0.5 * (north - south)
    other = swap(near)
    up = jnp.where(sub8 == 7, 0.0, pltpu.roll(other, 7, 0))
    down = jnp.where(sub8 == 0, 0.0, pltpu.roll(other, 1, 0))
    above = jnp.where(half8, other, up)
    below = jnp.where(half8, down, other)
    new2 = frecv[1, 16:24, :] - 0.5 * (above - below)
    for f, v in enumerate((new0, new1, new2, frecv[1, 24:32, :], frecv[1, 32:40, :])):
        spread(gather(v), XG + f * 16)
    for copy in early:
        copy.wait_send()

    @pl.loop(0, 2)
    def _(i):
        for u in range(7):
            correct_plane(0, 1 + 7 * i + u, fld1, level, u)

    def finish1(k, f, v):
        start = fld0[rows(level(k, f), PLANE), :]
        fields[rows((k * FIELDS + f) * PLANE, PLANE), :] = 0.5 * (start + v)

    @pl.loop(0, 5)
    def _(i):
        for u in range(2):
            tendency_plane(fld1, 3 + 2 * i + u, finish1, u)

    transform(3, 0)

    for copy in final[:4] + early[1:]:
        copy.wait_recv()
    spread(gather(qrecv[0, 1], 2), 0)
    spread(gather(qrecv[0, 2], 3), 32)
    over = jnp.broadcast_to(swap(qrecv[0, 2])[0:1, :], (8, 128))
    under = jnp.broadcast_to(swap(qrecv[0, 1])[7:8, :], (8, 128))
    rest = jnp.where(
        half8,
        jnp.where(sub8 == 0, 0.5 * under, 0.0),
        jnp.where(sub8 == 7, -0.5 * over, 0.0),
    )
    spread(gather(rest), TAIL)
    spread(gather(new2 + rest), XG + 2 * 16)

    for u in range(2):
        correct_plane(0, u * (CZ - 1), fld1, level, u)

    @pl.when(has_low)
    def _():
        for u in range(2):
            correct_plane(0, u - 2, fld1, level, u)

    @pl.when(has_high)
    def _():
        for u in range(2):
            correct_plane(0, CZ + u, fld1, level, u)

    for k in range(3, CZ - 3):
        west, east = xg[0, pl.ds(TAIL + k, 1), :], xg[1, pl.ds(TAIL + k, 1), :]
        at = jnp.where(fine, PLANE - 1, 0)
        c = fld1[pl.ds(level(k, 0) + at, 1), :]
        add = 0.5 * (DIFFUSION * (east + west) - (0.5 * COURANT) * c * (east - west))
        lanes = lax.broadcasted_iota(jnp.int32, (1, 128), 1)
        here = jnp.where(fine, lanes, 127 - lanes) >= 64
        row_at = pl.ds((k * FIELDS + 2) * PLANE + at, 1)
        fields[row_at, :] = fields[row_at, :] + jnp.where(here, add, 0.0)

    @pl.loop(0, 2)
    def _(i):
        for u in range(3):
            tendency_plane(fld1, i * (CZ - 3) + u, finish1, u)

    transform(0, 3)
    final = solve(1)
    final[2].wait_recv()
    spread(gather(qrecv[1, 0]), 16)

    def place(k, f):
        return (k * FIELDS + f) * PLANE

    @pl.loop(0, 2)
    def _(i):
        for u in range(7):
            correct_plane(1, 1 + 7 * i + u, fields, place, u)

    for u in range(2):
        correct_plane(1, u * (CZ - 1), fields, place, u, along_z=False)

    def store_head(b, lanes, v):
        out_p[b * 8 : b * 8 + 8, lanes] = v

    to_native(lambda k, r: prs[1, rows((k + 3) * PLANE + r, 8), :], store_head)

    def put_field(f):
        def load_field(k, r):
            return fields[rows(place(k, f) + r, 8), :]

        def store_field(b, lanes, v):
            out_s[f, b * 8 : b * 8 + 8, lanes] = v

        to_native(load_field, store_field)

    for f in (0, 1, 3, 4):
        put_field(f)
    for copy in final[:2]:
        copy.wait_recv()
    for u in range(2):
        correct_z(1, u * (CZ - 1), fields, place)
    put_field(2)
    for copy in messages:
        copy.wait_send()


def finish_kernel(fields, head, out_s, out_p, sems):
    copies = [
        pltpu.make_async_copy(fields, out_s, sems.at[0]),
        pltpu.make_async_copy(head, out_p, sems.at[1]),
    ]
    for copy in copies:
        copy.start()
    for copy in copies:
        copy.wait()


def write_out(fields, head):
    hbm = pl.BlockSpec(memory_space=pltpu.HBM)
    vmem = pl.BlockSpec(memory_space=pltpu.VMEM)
    return pl.pallas_call(
        finish_kernel,
        out_shape=(
            jax.ShapeDtypeStruct(fields.shape, F32),
            jax.ShapeDtypeStruct(head.shape, F32),
        ),
        in_specs=[vmem, vmem],
        out_specs=(hbm, hbm),
        scratch_shapes=[pltpu.SemaphoreType.DMA((2,))],
        compiler_params=pltpu.CompilerParams(vmem_limit_bytes=1 << 20),
        name="write_out",
    )(fields, head)


def step(state, burn, fmap):
    hbm = pl.BlockSpec(memory_space=pltpu.HBM)
    vmem = pl.BlockSpec(memory_space=pltpu.VMEM)
    tab, bh, bl = tables()
    vm = pltpu.VMEM
    layers = (CZ + 2 * HALO) * LEVEL
    return pl.pallas_call(
        kernel,
        out_shape=(
            jax.ShapeDtypeStruct((FIELDS, CZ, NX * NY), F32),
            jax.ShapeDtypeStruct((CZ, NX * NY), F32),
        ),
        in_specs=[hbm] * 6,
        out_specs=(vmem, vmem),
        scratch_shapes=[
            vm((FIELDS, CZ, NX * NY), F32),
            vm((CZ, NX * NY), F32),
            vm((layers, 128), F32),
            vm((layers, 128), F32),
            vm((CZ * LEVEL, 128), F32),
            vm((CZ * PLANE, 128), F32),
            vm((CZ * PLANE, 128), F32),
            vm((CZ * PLANE, 128), F32),
            vm((CZ * PLANE, 128), F32),
            vm((CZ * PLANE, 128), F32),
            vm((SECTIONS, (CZ + 6) * PLANE, 128), F32),
            vm((512, 128), F32),
            vm((3 * FIELDS * 48, 128), F32),
            vm((2, 64 + FIELDS * 16, 128), F32),
            vm((SECTIONS, 2, PLANE, 128), F32),
            vm((SECTIONS, 4, PLANE, 128), F32),
            vm((SECTIONS, 2, 16, 128), F32),
            vm((SECTIONS, 2, 16, 128), F32),
            vm((SECTIONS, 2, 3 * PLANE, 128), F32),
            vm((SECTIONS, 16, 128), F32),
            vm((SECTIONS, 4, 8, 128), F32),
            vm((SECTIONS, FIELDS * 8, 128), F32),
            vm((SECTIONS, FIELDS * 8, 128), F32),
            vm((1, 16, 128), F32),
            vm((T_ROWS, 128), F32),
            vm((B_ROWS, 128), BF16),
            vm((B_ROWS, 128), BF16),
            vm((4, 8, 128), jnp.int32),
            pltpu.SemaphoreType.DMA((FIELDS + 1,)),
            pltpu.SemaphoreType.DMA((4,)),
            pltpu.SemaphoreType.DMA((48,)),
            pltpu.SemaphoreType.DMA((48,)),
        ],
        compiler_params=pltpu.CompilerParams(
            collective_id=0, has_side_effects=True, vmem_limit_bytes=40 << 20
        ),
        name="fire_step",
    )(*[pltpu.with_memory_space_constraint(v, pltpu.HBM) for v in (state, burn, fmap, jnp.asarray(tab), jnp.asarray(bh), jnp.asarray(bl))])


def shards(state, burn_rate, face_map):
    fields, head = write_out(*step(state[0], burn_rate[0], face_map.reshape(8, 128)))
    return fields[None], head[None]


def solution(mesh):
    placed = (P("grp", None, "mesh", None), P("grp", "mesh", None), P("grp", "mesh", None))
    return jax.shard_map(
        shards,
        mesh=mesh,
        in_specs=placed,
        out_specs=(P("grp", None, "mesh", None), P("grp", "mesh", None)),
        check_vma=False,
    )
```

```python
import math

import jax
import jax.numpy as jnp
import numpy as np
from jax import lax
from jax.experimental import pallas as pl
from jax.experimental.pallas import tpu as pltpu
from jax.sharding import PartitionSpec as P

NX = 64
NY = 64
CZ = 16
FIELDS = 5
SECTIONS = 2
ITERS = 3
COURANT = 0.1
DIFFUSION = 0.05
STOICHIOMETRY = 2.0
EXPANSION = 1.0

PLANE = 32
LEVEL = FIELDS * PLANE
HALO = 2
MESH = pl.DeviceIdType.MESH
F32 = jnp.float32
BF16 = jnp.bfloat16


def sine(n):
    i = np.arange(n, dtype=np.float64) + 1.0
    return np.sin(np.pi * i[:, None] * i[None, :] / (n + 1)) * math.sqrt(2.0 / (n + 1))


def eigen(n):
    i = np.arange(n, dtype=np.float64) + 1.0
    return 2.0 - 2.0 * np.cos(np.pi * i / (n + 1))


T_IM = 0
T_Z1 = 512
T_Z2 = 576
T_W = 640
T_GAMMA = 664
T_ALPHA = 672
T_SX = 736
T_SX2 = 864
T_ZF = 992
T_ROWS = 1056
B_Y = 0
B_XF = 128
B_XI = 192
B_ROWS = 256


def tables():
    s16, s64 = sine(CZ), sine(NX)
    tab = np.zeros((T_ROWS, 128))
    modes = eigen(CZ)[:, None, None] + eigen(NX)[None, :, None] + eigen(NY)[None, None, :]
    inv = 1.0 / modes
    tab[T_IM : T_IM + 512] = (
        inv.reshape(8, 2, 64, 64).transpose(0, 2, 1, 3).reshape(512, 128)
    )
    for p in range(8):
        for h in range(2):
            lanes = slice(64 * h, 64 * h + 64)
            for r in range(8):
                tab[T_Z1 + p * 8 + r, lanes] = s16[2 * p + h, 2 * r + h]
                tab[T_Z2 + p * 8 + r, lanes] = s16[2 * p + 1 - h, 2 * r + h]
            for k in range(8):
                tab[T_ZF + p * 8 + k, lanes] = s16[2 * p + h, k] * (-1.0) ** h
            for k in range(3):
                tab[T_W + 8 * k + p, lanes] = s16[2 * p + h, k]
    for at, places in ((T_SX, (63, 0)), (T_SX2, (62, 1))):
        for side, place in enumerate(places):
            tab[at + 64 * side : at + 64 * side + 64] = s64[:, place][:, None]
    packed = tab[T_IM : T_IM + 512].reshape(8, 64, 128)
    tab[T_ALPHA : T_ALPHA + 64] = (packed * tab[T_W : T_W + 8, None, :] ** 2).sum(0)
    tab[T_GAMMA : T_GAMMA + 8] = (packed * tab[None, T_SX : T_SX + 64] ** 2).sum(1)
    mat = np.zeros((B_ROWS, 128))
    mat[B_Y : B_Y + 128] = np.kron(np.eye(2), s64)
    order = np.concatenate([np.arange(0, 64, 2), np.arange(1, 64, 2)])
    mat[B_XF : B_XF + 64, :64] = s64[:, order]
    mat[B_XI : B_XI + 64, :64] = s64[order, :]
    mat = mat.astype(np.float32)
    high = mat.astype(jnp.bfloat16)
    low = (mat - high.astype(np.float32)).astype(jnp.bfloat16)
    return tab.astype(np.float32), high, low


S16 = sine(CZ)


def split(v):
    high = v.astype(BF16)
    return high, (v - high.astype(F32)).astype(BF16)


def dot(a, b):
    return jnp.dot(a, b, preferred_element_type=F32)


def dot_right(v, th, tl):
    vh, vl = split(v)
    return dot(vh, th) + (dot(vl, th) + dot(vh, tl))


def dot_left(th, tl, v):
    vh, vl = split(v)
    return dot(th, vh) + (dot(th, vl) + dot(tl, vh))


def kernel(
    state, burn, fmap, tab_h, bh_h, bl_h, out_s, out_p,
    stn, bnn, fld0, fld1, fields, burning, src, ybuf, hat1, hat, prs, resp,
    turns, xg, zsend, zrecv, dsend, drecv, psend, qsend, qrecv, fsend, frecv, psel, tab, bh, bl, idx,
    in_sem, t_sem, send_sem, recv_sem,
):
    g = lax.axis_index("grp")
    m = lax.axis_index("mesh")
    n = lax.axis_size("mesh")
    fine = g == 0
    LOW, HIGH, PARTNER, LOW2, HIGH2, DLOW, DHIGH = range(7)
    back = (HIGH, LOW, PARTNER, HIGH2, LOW2, DHIGH, DLOW)
    has_low, has_high = m > 0, m < n - 1
    exists = (has_low, has_high, None, m > 1, m < n - 2, has_low, has_high)
    steps = (-1, 1, 0, -2, 2, -1, 1)
    where_to = [
        {"grp": 1 - g if to in (PARTNER, DLOW, DHIGH) else g, "mesh": lax.rem(m + n + steps[to], n)}
        for to in range(7)
    ]
    count = 1
    for to in range(7):
        if exists[to] is not None:
            count = count + exists[to].astype(jnp.int32)

    def guarded(condition, action):
        if condition is None:
            action()
        else:
            pl.when(condition)(action)

    loads = [
        pltpu.make_async_copy(state.at[f], stn.at[f], in_sem.at[f]) for f in range(FIELDS)
    ]
    loads.append(pltpu.make_async_copy(burn, bnn, in_sem.at[FIELDS]))
    for copy in loads:
        copy.start()
    table_loads = [
        pltpu.make_async_copy(a, b, t_sem.at[i])
        for i, (a, b) in enumerate(((fmap, idx.at[0]), (tab_h, tab), (bh_h, bh), (bl_h, bl)))
    ]
    for copy in table_loads:
        copy.start()

    def clear(ref, start, size):
        ref[start : start + size, :] = jnp.zeros((size, 128), F32)

    def level(k, f):
        return (f * (CZ + 2 * HALO) + k + HALO) * PLANE

    @pl.when(jnp.logical_not(has_low))
    def _():
        for f in range(FIELDS):
            clear(fld0, level(-2, f), 2 * PLANE)
            clear(fld1, level(-2, f), 2 * PLANE)
        for s in range(SECTIONS):
            clear(prs.at[s], 0, 3 * PLANE)
            clear(zrecv.at[s, 1], 0, PLANE)
            clear(drecv.at[s, 0], 0, 16)
            clear(qrecv.at[s, 1], 0, 8)

    @pl.when(jnp.logical_not(has_high))
    def _():
        for f in range(FIELDS):
            clear(fld0, level(CZ, f), 2 * PLANE)
            clear(fld1, level(CZ, f), 2 * PLANE)
        for s in range(SECTIONS):
            clear(prs.at[s], (CZ + 3) * PLANE, 3 * PLANE)
            clear(zrecv.at[s, 0], 0, PLANE)
            clear(drecv.at[s, 1], 0, 16)
            clear(qrecv.at[s, 2], 0, 8)

    @pl.when(m < 2)
    def _():
        for s in range(SECTIONS):
            clear(zrecv.at[s, 3], 0, PLANE)

    @pl.when(m > n - 3)
    def _():
        for s in range(SECTIONS):
            clear(zrecv.at[s, 2], 0, PLANE)

    barrier = pltpu.get_barrier_semaphore()
    for to in range(7):
        guarded(
            exists[to],
            lambda to=to: pl.semaphore_signal(
                barrier, inc=1, device_id=where_to[to], device_id_type=MESH
            ),
        )

    messages = []

    class Message:
        def __init__(self, to, a, b):
            slot = len(messages)
            messages.append(self)
            self.to = to
            self.copy = pltpu.make_async_remote_copy(
                src_ref=a, dst_ref=b, send_sem=send_sem.at[slot], recv_sem=recv_sem.at[slot],
                device_id=where_to[to], device_id_type=MESH,
            )
            self.sent = False

        def start(self):
            guarded(exists[self.to], self.copy.start)

        def wait_recv(self):
            guarded(exists[back[self.to]], self.copy.wait_recv)

        def wait_send(self):
            if not self.sent:
                self.sent = True
                guarded(exists[self.to], self.copy.wait_send)

    lane = lax.broadcasted_iota(jnp.int32, (PLANE, 128), 1)
    half0 = lane < 64
    y_last = (lane == 63) | (lane == 127)
    y_first = (lane == 0) | (lane == 64)
    half8 = lax.broadcasted_iota(jnp.int32, (8, 128), 1) < 64
    half64 = lax.broadcasted_iota(jnp.int32, (64, 128), 1) < 64
    sub8 = lax.broadcasted_iota(jnp.int32, (8, 128), 0)

    def swap(v):
        return pltpu.roll(v, 64, 1)

    def rows(start, size):
        return pl.ds(pl.multiple_of(start, 8), size)

    def to_layers(load, store):
        for b in range(2):
            for t in range(4):
                tiles = jnp.stack([load(b, pl.ds((t * 8 + i) * 128, 128)) for i in range(8)])
                turned = jnp.swapaxes(tiles, 0, 1)
                for i in range(8):
                    store(b * 8 + i, t * 8, turned[i])

    def to_native(load, store):
        for b in range(2):
            for t in range(4):
                tiles = jnp.stack([load(b * 8 + i, t * 8) for i in range(8)])
                turned = jnp.swapaxes(tiles, 0, 1)
                for i in range(8):
                    store(b, pl.ds((t * 8 + i) * 128, 128), turned[i])

    def own_plane(fld, f):
        at = jnp.where(fine, PLANE - 1, 0)
        tiles = []
        for odd in range(2):
            tile = jnp.zeros((8, 128), F32)
            for r in range(8):
                one = fld[pl.ds(level(2 * r + odd, f) + at, 1), :]
                tile = jnp.where(sub8 == r, jnp.broadcast_to(one, (8, 128)), tile)
            tiles.append(tile)
        even, odd = tiles
        return jnp.where(
            fine, jnp.where(half8, swap(even), odd), jnp.where(half8, even, swap(odd))
        )

    def halo_messages(fld, f):
        return [
            Message(LOW, fld.at[pl.ds(level(0, f), 2 * PLANE)],
                    fld.at[pl.ds(level(CZ, f), 2 * PLANE)]),
            Message(HIGH, fld.at[pl.ds(level(CZ - 2, f), 2 * PLANE)],
                    fld.at[pl.ds(level(-2, f), 2 * PLANE)]),
        ]

    def gather(plane, who=0):
        index = idx[who]
        column = index & 127
        block = index >> 7
        out = jnp.zeros((8, 128), F32)
        for r in range(8):
            one = jnp.broadcast_to(plane[r : r + 1, :], (8, 128))
            out = jnp.where(block == r, jnp.take_along_axis(one, column, axis=1), out)
        return out

    def spread(ghost, base):
        other = swap(ghost)
        even = jnp.where(half8, ghost, other)
        odd = jnp.where(half8, other, ghost)
        zero = jnp.zeros_like(ghost)
        for side in range(2):
            on = fine if side else jnp.logical_not(fine)
            xg[side, pl.ds(base, 8, stride=2), :] = jnp.where(on, even, zero)
            xg[side, pl.ds(base + 1, 8, stride=2), :] = jnp.where(on, odd, zero)

    def x_sides(v, at, slot):
        base = slot * 48
        turned = swap(v)
        turns[base + 8 : base + 40, :] = turned
        turns[base + 7 : base + 8, :] = xg[0, pl.ds(at, 1), :]
        turns[base + 40 : base + 41, :] = xg[1, pl.ds(at, 1), :]
        down = turns[base + 7 : base + 39, :]
        up = turns[base + 9 : base + 41, :]
        return turned, jnp.where(half0, down, up)

    def y_sides(v):
        north = jnp.where(y_last, 0.0, pltpu.roll(v, 127, 1))
        south = jnp.where(y_first, 0.0, pltpu.roll(v, 1, 1))
        return north, south

    XG = 48
    TAIL = XG + FIELDS * 16

    def tendency_plane(fld, k, finish, u=0):
        c = [fld[rows(level(k, f), PLANE), :] for f in range(FIELDS)]
        reaction = burning[rows(k * PLANE, PLANE), :] * c[3] * c[4]
        source = EXPANSION * reaction
        half = jnp.where(half0, 0.5, -0.5)
        cx = c[0] * (half * -COURANT)
        cy = c[1] * (-0.5 * COURANT)
        cz = c[2] * (-COURANT * 2.0 / 3.0)
        cz2 = c[2] * (COURANT / 12.0)
        for f in range(FIELDS):
            above = fld[rows(level(k + 1, f), PLANE), :]
            below = fld[rows(level(k - 1, f), PLANE), :]
            above2 = fld[rows(level(k + 2, f), PLANE), :]
            below2 = fld[rows(level(k - 2, f), PLANE), :]
            inner, outer = x_sides(c[f], XG + f * 16 + k, u * FIELDS + f)
            north, south = y_sides(c[f])
            dx = inner - outer
            dy = north - south
            dz = above - below
            total = (inner + outer) + (north + south) + (above + below)
            change = (DIFFUSION * total + cx * dx) + (cy * dy + cz * dz) + cz2 * (above2 - below2)
            if f == 0:
                source = source - half * dx
            elif f == 1:
                source = source - 0.5 * dy
            elif f == 2:
                source = source - 0.5 * dz
            elif f == 3:
                change = change - reaction
            else:
                change = change - STOICHIOMETRY * reaction
            finish(k, f, c[f] * (1.0 - 6.0 * DIFFUSION) + change)
        src[rows(k * PLANE, PLANE), :] = source

    def z_inverse(spec, into, base):
        @pl.loop(0, 4)
        def _(t):
            v = [spec[rows(c * PLANE + t * 8, 8), :] for c in range(CZ)]
            for k in range(8):
                even = v[0] * F32(S16[0, k])
                odd = v[1] * F32(S16[1, k])
                for c in range(1, 8):
                    even = even + v[2 * c] * F32(S16[2 * c, k])
                    odd = odd + v[2 * c + 1] * F32(S16[2 * c + 1, k])
                into[rows(base + k * PLANE + t * 8, 8), :] = even + odd
                into[rows(base + (15 - k) * PLANE + t * 8, 8), :] = even - odd

    def y_matrix():
        return bh[B_Y : B_Y + 128, :], bl[B_Y : B_Y + 128, :]

    def y_transform(v):
        return dot_right(v, *y_matrix())

    def x_forward(a, b):
        even = jnp.where(half0, a, swap(b))
        odd = jnp.where(half0, swap(a), b)
        v = jnp.concatenate([even, odd], axis=0)
        return dot_left(bh[B_XF : B_XF + 64, :64], bl[B_XF : B_XF + 64, :64], v)

    def transform(first, last):
        pairs = range(first, 8) if last == 0 else range(last)
        if last == 0:
            v = y_transform(src[first * PLANE : (CZ - first) * PLANE, :])
            planes = {k: v[(k - first) * PLANE : (k - first + 1) * PLANE] for k in range(first, CZ - first)}
        else:
            v = y_transform(
                jnp.concatenate(
                    [src[: last * PLANE, :], src[(CZ - last) * PLANE : CZ * PLANE, :]], axis=0
                )
            )
            planes = {k: v[k * PLANE : (k + 1) * PLANE] for k in range(last)}
            for i in range(last):
                planes[CZ - last + i] = v[(last + i) * PLANE : (last + i + 1) * PLANE]
        for k in pairs:
            ybuf[k * 64 : k * 64 + 64, :] = x_forward(planes[k], planes[CZ - 1 - k])
        for r in range(8):
            turned = []
            for p in pairs:
                v = ybuf[p * 64 + r * 8 : p * 64 + r * 8 + 8, :]
                turned.append(v + jnp.where(half8, swap(v), -swap(v)))
            for q in range(8):
                at = q * 64 + r * 8
                parts = [
                    tab[T_ZF + q * 8 + p : T_ZF + q * 8 + p + 1, :] * v
                    for p, v in zip(pairs, turned)
                ]
                if last:
                    parts.append(hat1[at : at + 8, :])
                while len(parts) > 1:
                    parts = [a + b for a, b in zip(parts[::2], parts[1::2])] + (
                        parts[-1:] if len(parts) % 2 else []
                    )
                total = parts[0]
                if last:
                    total = total * tab[T_IM + at : T_IM + at + 8, :]
                hat1[at : at + 8, :] = total

    def x_inverse(v):
        v = dot_left(bh[B_XI : B_XI + 64, :64], bl[B_XI : B_XI + 64, :64], v)
        even, odd = v[:PLANE], v[PLANE:]
        return jnp.where(half0, even, swap(odd)), jnp.where(half0, swap(even), odd)

    def z_plane(v):
        other = swap(v)
        parts = []
        for p in range(8):
            parts.append(tab[T_Z1 + p * 8 : T_Z1 + p * 8 + 8, :] * v[p : p + 1, :])
            parts.append(tab[T_Z2 + p * 8 : T_Z2 + p * 8 + 8, :] * other[p : p + 1, :])
        while len(parts) > 1:
            parts = [a + b for a, b in zip(parts[::2], parts[1::2])]
        return parts[0]

    def side_x(at=T_SX):
        return tab[rows(at + g * 64, 64), :]

    def weight(k, p):
        return tab[T_W + 8 * k + p : T_W + 8 * k + p + 1, :]

    def modes(p):
        return tab[T_IM + p * 64 : T_IM + p * 64 + 64, :]

    def block(ref, p):
        return ref[p * 64 : p * 64 + 64, :]

    def first_of(acc):
        return acc + swap(acc)

    def last_of(acc):
        other = swap(acc)
        return jnp.where(half64, acc - other, other - acc)

    def z_layers(spec, k):
        acc = weight(k, 0) * block(spec, 0)
        for p in range(1, 8):
            acc = acc + weight(k, p) * block(spec, p)
        return acc

    def x_planes(spec, at):
        sx = side_x(at)
        return jnp.concatenate(
            [jnp.sum(sx * block(spec, p), axis=0, keepdims=True) for p in range(8)], axis=0
        )

    def narrow(v):
        return jnp.where(half0, v[:PLANE], v[PLANE:])

    def widen(v):
        other = swap(v)
        return jnp.concatenate(
            [jnp.where(half0, v, other), jnp.where(half0, other, v)], axis=0
        )

    def z_ghosts(below, above):
        return below + jnp.where(half64, above, -above)

    def layer_response(both, ghost):
        acc = tab[T_ALPHA : T_ALPHA + 64, :] * both
        for p in range(8):
            acc = acc + block(resp, p) * ghost[p : p + 1, :]
        return acc

    def plane_response(layer):
        return jnp.concatenate(
            [jnp.sum(block(resp, p) * layer, axis=0, keepdims=True) for p in range(8)], axis=0
        )

    Z_HIGH, Z_LOW, Z_HIGH2, Z_LOW2 = range(4)

    def solve(s):
        own = prs.at[s]
        acc = z_layers(hat1, 0)
        first, last = first_of(acc), last_of(acc)
        zsend[s, 0] = narrow(first)
        zsend[s, 1] = narrow(last)
        copies = [
            Message(LOW2, zsend.at[s, 0], zrecv.at[s, Z_HIGH2]),
            Message(HIGH2, zsend.at[s, 1], zrecv.at[s, Z_LOW2]),
            Message(LOW, zsend.at[s, 0], zrecv.at[s, Z_HIGH]),
            Message(HIGH, zsend.at[s, 1], zrecv.at[s, Z_LOW]),
        ]
        for copy in copies:
            copy.start()
        start = x_planes(hat1, T_SX)
        plane = z_plane(y_transform(start))
        dsend[s, 0, 0:8, :] = plane
        dsend[s, 1, 0:8, :] = plane
        dsend[s, 0, 8:16, :] = plane_response(first)
        dsend[s, 1, 8:16, :] = plane_response(last)
        sides = [
            Message(DLOW, dsend.at[s, 0], drecv.at[s, 1]),
            Message(DHIGH, dsend.at[s, 1], drecv.at[s, 0]),
            Message(PARTNER, dsend.at[s, 0, pl.ds(0, 8)], qrecv.at[s, 3]),
        ]
        for copy in sides:
            copy.start()
        if s == 0:
            for f in range(FIELDS):
                fsend[1, f * 8 : f * 8 + 8, :] = own_plane(fld1, f)
            early.append(Message(PARTNER, fsend.at[1], frecv.at[1]))
            for f in range(FIELDS):
                early.extend(halo_messages(fld1, f))
            for copy in early:
                copy.start()
            for copy in maps[1:]:
                copy.wait_recv()
        mine = y_transform(z_plane(gather(plane, 1)))
        mine = tab[T_GAMMA : T_GAMMA + 8, :] * mine
        for copy in sides:
            copy.wait_recv()
        response = drecv[s, 0, 8:16, :] + jnp.where(
            half8, drecv[s, 1, 8:16, :], -drecv[s, 1, 8:16, :]
        )
        partner = qrecv[s, 3] + z_plane(y_transform(response + mine))
        ghost = z_plane(gather(partner))
        ghosts = y_transform(
            jnp.concatenate(
                [
                    z_plane(gather(drecv[s, 0, 0:8, :], 2)),
                    z_plane(gather(drecv[s, 1, 0:8, :], 3)),
                    ghost,
                ],
                axis=0,
            )
        )
        ghost = ghosts[16:24]
        for copy in copies:
            copy.wait_recv()

        def got(slot):
            return zrecv[s, slot]

        above = got(Z_HIGH) + narrow(
            first_of(layer_response(z_ghosts(last, widen(got(Z_HIGH2))), ghosts[8:16]))
        )
        below = got(Z_LOW) + narrow(
            last_of(layer_response(z_ghosts(widen(got(Z_LOW2)), first), ghosts[0:8]))
        )
        above = jnp.where(has_high, above, 0.0)
        below = jnp.where(has_low, below, 0.0)
        both = z_ghosts(widen(below), widen(above))
        depth = 3 if s == 0 else 1
        size = depth * PLANE

        def spectrum():
            sx = side_x()
            for p in range(8):
                extra = weight(0, p) * both + sx * ghost[p : p + 1, :]
                hat[p * 64 : p * 64 + 64, :] = block(hat1, p) + extra * modes(p)

        def layers_out(k, acc):
            a, b = x_inverse(jnp.where(half64, first_of(acc), last_of(acc)))
            psend[s, 0, k * PLANE : (k + 1) * PLANE, :] = y_transform(a)
            at = depth - 1 - k
            psend[s, 1, at * PLANE : (at + 1) * PLANE, :] = y_transform(b)

        stack = [
            Message(LOW, psend.at[s, 0, pl.ds(0, size)], own.at[pl.ds((CZ + 3) * PLANE, size)]),
            Message(HIGH, psend.at[s, 1, pl.ds(0, size)], own.at[pl.ds((3 - depth) * PLANE, size)]),
        ]
        if s == 0:
            spectrum()
            planes = y_transform(
                jnp.concatenate([x_planes(hat, T_SX), x_planes(hat, T_SX2)], axis=0)
            )
            for i in range(2):
                qsend[s, i * 8 : i * 8 + 8, :] = z_plane(planes[i * 8 : i * 8 + 8])
            copies = [
                Message(DLOW, qsend.at[s, pl.ds(0, 8)], qrecv.at[s, 2]),
                Message(DHIGH, qsend.at[s, pl.ds(0, 8)], qrecv.at[s, 1]),
                Message(PARTNER, qsend.at[s], psel.at[0]),
            ]
            for copy in copies:
                copy.start()
            for k in range(depth):
                layers_out(k, z_layers(hat, k))
            for copy in stack:
                copy.start()
        else:
            layers_out(0, acc + layer_response(both, ghost))
            for copy in stack:
                copy.start()
            plane = start + plane_response(both) + tab[T_GAMMA : T_GAMMA + 8, :] * ghost
            qsend[s, 0:8, :] = z_plane(y_transform(plane))
            copies = [Message(PARTNER, qsend.at[s, pl.ds(0, 8)], qrecv.at[s, 0])]
            for copy in copies:
                copy.start()
            spectrum()
        copies = stack + copies
        for p in range(8):
            a, b = x_inverse(block(hat, p))
            ybuf[2 * p * PLANE : (2 * p + 1) * PLANE, :] = a
            ybuf[(2 * p + 1) * PLANE : (2 * p + 2) * PLANE, :] = b
        ybuf[...] = y_transform(ybuf[...])
        z_inverse(ybuf, own, 3 * PLANE)
        return copies

    def correct_z(s, k, into, at_of):
        own = prs.at[s]
        above = own[rows((k + 4) * PLANE, PLANE), :]
        below = own[rows((k + 2) * PLANE, PLANE), :]
        at = rows(at_of(k, 2), PLANE)
        into[at, :] = into[at, :] - 0.5 * (above - below)

    def correct_plane(s, k, into, at_of, u=0, along_z=True):
        p = prs[s, rows((k + 3) * PLANE, PLANE), :]
        inner, outer = x_sides(p, 16 + k, u)
        north, south = y_sides(p)
        half = jnp.where(half0, 0.5, -0.5)
        for f, v in enumerate((half * (inner - outer), 0.5 * (north - south))):
            at = rows(at_of(k, f), PLANE)
            into[at, :] = into[at, :] - v
        if along_z:
            correct_z(s, k, into, at_of)

    early = []
    for f in range(FIELDS):
        loads[f].wait()

        def load_state(b, lanes, f=f):
            return stn[f, b * 8 : b * 8 + 8, lanes]

        def store_state(k, r, v, f=f):
            fld0[rows(level(k, f) + r, 8), :] = v

        to_layers(load_state, store_state)
        if f == 0:
            pl.semaphore_wait(barrier, count)
        copies = halo_messages(fld0, f)
        for copy in copies:
            copy.start()
        early.extend(copies)
    for f in range(FIELDS):
        fsend[0, f * 8 : f * 8 + 8, :] = own_plane(fld0, f)
    table_loads[0].wait()
    maps = [
        Message(PARTNER, fsend.at[0], frecv.at[0]),
        Message(PARTNER, idx.at[0], idx.at[1]),
        Message(HIGH, idx.at[0], idx.at[2]),
        Message(LOW, idx.at[0], idx.at[3]),
    ]
    for copy in maps:
        copy.start()
    loads[FIELDS].wait()

    def load_burn(b, lanes):
        return bnn[b * 8 : b * 8 + 8, lanes]

    def store_burn(k, r, v):
        burning[rows(k * PLANE + r, 8), :] = v

    to_layers(load_burn, store_burn)
    for copy in table_loads[1:]:
        copy.wait()
    for p in range(8):
        resp[p * 64 : p * 64 + 64, :] = modes(p) * weight(0, p) * side_x()

    def finish0(k, f, v):
        fld1[rows(level(k, f), PLANE), :] = v

    maps[0].wait_recv()
    for f in range(FIELDS):
        spread(gather(frecv[0, f * 8 : f * 8 + 8, :]), XG + f * 16)

    @pl.loop(0, 6)
    def _(i):
        for u in range(2):
            tendency_plane(fld0, 2 + 2 * i + u, finish0, u)

    transform(2, 0)

    for copy in early:
        copy.wait_recv()

    for u, k in enumerate((0, 1, CZ - 2, CZ - 1)):
        tendency_plane(fld0, k, finish0, u)

    early = []
    transform(0, 2)
    final = solve(0)

    final[4].wait_recv()
    early[0].wait_recv()
    near = psel[0, 0:8, :]
    beside = psel[0, 8:16, :]
    spread(gather(near), 16)
    sides = gather(qsend[0, 0:8, :], 1)
    sign = jnp.where(fine, -0.5, 0.5)
    new0 = frecv[1, 0:8, :] - sign * (sides - beside)
    lane8 = lax.broadcasted_iota(jnp.int32, (8, 128), 1)
    north = jnp.where((lane8 == 63) | (lane8 == 127), 0.0, pltpu.roll(near, 127, 1))
    south = jnp.where((lane8 == 0) | (lane8 == 64), 0.0, pltpu.roll(near, 1, 1))
    new1 = frecv[1, 8:16, :] - 0.5 * (north - south)
    other = swap(near)
    up = jnp.where(sub8 == 7, 0.0, pltpu.roll(other, 7, 0))
    down = jnp.where(sub8 == 0, 0.0, pltpu.roll(other, 1, 0))
    above = jnp.where(half8, other, up)
    below = jnp.where(half8, down, other)
    new2 = frecv[1, 16:24, :] - 0.5 * (above - below)
    for f, v in enumerate((new0, new1, new2, frecv[1, 24:32, :], frecv[1, 32:40, :])):
        spread(gather(v), XG + f * 16)
    for copy in early:
        copy.wait_send()

    @pl.loop(0, 2)
    def _(i):
        for u in range(7):
            correct_plane(0, 1 + 7 * i + u, fld1, level, u)

    def finish1(k, f, v):
        start = fld0[rows(level(k, f), PLANE), :]
        fields[rows((k * FIELDS + f) * PLANE, PLANE), :] = 0.5 * (start + v)

    @pl.loop(0, 5)
    def _(i):
        for u in range(2):
            tendency_plane(fld1, 3 + 2 * i + u, finish1, u)

    transform(3, 0)

    for copy in final[:4] + early[1:]:
        copy.wait_recv()
    spread(gather(qrecv[0, 1], 2), 0)
    spread(gather(qrecv[0, 2], 3), 32)
    over = jnp.broadcast_to(swap(qrecv[0, 2])[0:1, :], (8, 128))
    under = jnp.broadcast_to(swap(qrecv[0, 1])[7:8, :], (8, 128))
    rest = jnp.where(
        half8,
        jnp.where(sub8 == 0, 0.5 * under, 0.0),
        jnp.where(sub8 == 7, -0.5 * over, 0.0),
    )
    spread(gather(rest), TAIL)
    spread(gather(new2 + rest), XG + 2 * 16)

    for u in range(2):
        correct_plane(0, u * (CZ - 1), fld1, level, u)

    @pl.when(has_low)
    def _():
        for u in range(2):
            correct_plane(0, u - 2, fld1, level, u)

    @pl.when(has_high)
    def _():
        for u in range(2):
            correct_plane(0, CZ + u, fld1, level, u)

    for k in range(3, CZ - 3):
        west, east = xg[0, pl.ds(TAIL + k, 1), :], xg[1, pl.ds(TAIL + k, 1), :]
        at = jnp.where(fine, PLANE - 1, 0)
        c = fld1[pl.ds(level(k, 0) + at, 1), :]
        add = 0.5 * (DIFFUSION * (east + west) - (0.5 * COURANT) * c * (east - west))
        lanes = lax.broadcasted_iota(jnp.int32, (1, 128), 1)
        here = jnp.where(fine, lanes, 127 - lanes) >= 64
        row_at = pl.ds((k * FIELDS + 2) * PLANE + at, 1)
        fields[row_at, :] = fields[row_at, :] + jnp.where(here, add, 0.0)

    @pl.loop(0, 2)
    def _(i):
        for u in range(3):
            tendency_plane(fld1, i * (CZ - 3) + u, finish1, u)

    transform(0, 3)
    final = solve(1)
    final[2].wait_recv()
    spread(gather(qrecv[1, 0]), 16)

    def place(k, f):
        return (k * FIELDS + f) * PLANE

    @pl.loop(0, 2)
    def _(i):
        for u in range(7):
            correct_plane(1, 1 + 7 * i + u, fields, place, u)

    for u in range(2):
        correct_plane(1, u * (CZ - 1), fields, place, u, along_z=False)

    def store_head(b, lanes, v):
        out_p[b * 8 : b * 8 + 8, lanes] = v

    to_native(lambda k, r: prs[1, rows((k + 3) * PLANE + r, 8), :], store_head)

    def put_field(f):
        def load_field(k, r):
            return fields[rows(place(k, f) + r, 8), :]

        def store_field(b, lanes, v):
            out_s[f, b * 8 : b * 8 + 8, lanes] = v

        to_native(load_field, store_field)

    for f in (0, 1, 3, 4):
        put_field(f)
    for copy in final[:2]:
        copy.wait_recv()
    for u in range(2):
        correct_z(1, u * (CZ - 1), fields, place)
    put_field(2)
    for copy in messages:
        copy.wait_send()


def finish_kernel(fields, head, out_s, out_p, sems):
    copies = [
        pltpu.make_async_copy(fields, out_s, sems.at[0]),
        pltpu.make_async_copy(head, out_p, sems.at[1]),
    ]
    for copy in copies:
        copy.start()
    for copy in copies:
        copy.wait()


def write_out(fields, head):
    hbm = pl.BlockSpec(memory_space=pltpu.HBM)
    vmem = pl.BlockSpec(memory_space=pltpu.VMEM)
    return pl.pallas_call(
        finish_kernel,
        out_shape=(
            jax.ShapeDtypeStruct(fields.shape, F32),
            jax.ShapeDtypeStruct(head.shape, F32),
        ),
        in_specs=[vmem, vmem],
        out_specs=(hbm, hbm),
        scratch_shapes=[pltpu.SemaphoreType.DMA((2,))],
        compiler_params=pltpu.CompilerParams(vmem_limit_bytes=1 << 20),
        name="write_out",
    )(fields, head)


def step(state, burn, fmap):
    hbm = pl.BlockSpec(memory_space=pltpu.HBM)
    vmem = pl.BlockSpec(memory_space=pltpu.VMEM)
    tab, bh, bl = tables()
    vm = pltpu.VMEM
    layers = (CZ + 2 * HALO) * LEVEL
    return pl.pallas_call(
        kernel,
        out_shape=(
            jax.ShapeDtypeStruct((FIELDS, CZ, NX * NY), F32),
            jax.ShapeDtypeStruct((CZ, NX * NY), F32),
        ),
        in_specs=[hbm] * 6,
        out_specs=(vmem, vmem),
        scratch_shapes=[
            vm((FIELDS, CZ, NX * NY), F32),
            vm((CZ, NX * NY), F32),
            vm((layers, 128), F32),
            vm((layers, 128), F32),
            vm((CZ * LEVEL, 128), F32),
            vm((CZ * PLANE, 128), F32),
            vm((CZ * PLANE, 128), F32),
            vm((CZ * PLANE, 128), F32),
            vm((CZ * PLANE, 128), F32),
            vm((CZ * PLANE, 128), F32),
            vm((SECTIONS, (CZ + 6) * PLANE, 128), F32),
            vm((512, 128), F32),
            vm((7 * FIELDS * 48, 128), F32),
            vm((2, 64 + FIELDS * 16, 128), F32),
            vm((SECTIONS, 2, PLANE, 128), F32),
            vm((SECTIONS, 4, PLANE, 128), F32),
            vm((SECTIONS, 2, 16, 128), F32),
            vm((SECTIONS, 2, 16, 128), F32),
            vm((SECTIONS, 2, 3 * PLANE, 128), F32),
            vm((SECTIONS, 16, 128), F32),
            vm((SECTIONS, 4, 8, 128), F32),
            vm((SECTIONS, FIELDS * 8, 128), F32),
            vm((SECTIONS, FIELDS * 8, 128), F32),
            vm((1, 16, 128), F32),
            vm((T_ROWS, 128), F32),
            vm((B_ROWS, 128), BF16),
            vm((B_ROWS, 128), BF16),
            vm((4, 8, 128), jnp.int32),
            pltpu.SemaphoreType.DMA((FIELDS + 1,)),
            pltpu.SemaphoreType.DMA((4,)),
            pltpu.SemaphoreType.DMA((48,)),
            pltpu.SemaphoreType.DMA((48,)),
        ],
        compiler_params=pltpu.CompilerParams(
            collective_id=0, has_side_effects=True, vmem_limit_bytes=40 << 20
        ),
        name="fire_step",
    )(*[pltpu.with_memory_space_constraint(v, pltpu.HBM) for v in (state, burn, fmap, jnp.asarray(tab), jnp.asarray(bh), jnp.asarray(bl))])


def shards(state, burn_rate, face_map):
    fields, head = write_out(*step(state[0], burn_rate[0], face_map.reshape(8, 128)))
    return fields[None], head[None]


def solution(mesh):
    placed = (P("grp", None, "mesh", None), P("grp", "mesh", None), P("grp", "mesh", None))
    return jax.shard_map(
        shards,
        mesh=mesh,
        in_specs=placed,
        out_specs=(P("grp", None, "mesh", None), P("grp", "mesh", None)),
        check_vma=False,
    )
```

```python
import math

import jax
import jax.numpy as jnp
import numpy as np
from jax import lax
from jax.experimental import pallas as pl
from jax.experimental.pallas import tpu as pltpu
from jax.sharding import PartitionSpec as P

NX = 64
NY = 64
CZ = 16
FIELDS = 5
SECTIONS = 2
ITERS = 3
COURANT = 0.1
DIFFUSION = 0.05
STOICHIOMETRY = 2.0
EXPANSION = 1.0

PLANE = 32
LEVEL = FIELDS * PLANE
HALO = 2
MESH = pl.DeviceIdType.MESH
F32 = jnp.float32
BF16 = jnp.bfloat16


def sine(n):
    i = np.arange(n, dtype=np.float64) + 1.0
    return np.sin(np.pi * i[:, None] * i[None, :] / (n + 1)) * math.sqrt(2.0 / (n + 1))


def eigen(n):
    i = np.arange(n, dtype=np.float64) + 1.0
    return 2.0 - 2.0 * np.cos(np.pi * i / (n + 1))


T_IM = 0
T_Z1 = 512
T_Z2 = 576
T_W = 640
T_GAMMA = 664
T_ALPHA = 672
T_SX = 736
T_SX2 = 864
T_ZF = 992
T_ROWS = 1056
B_Y = 0
B_XF = 128
B_XI = 192
B_ROWS = 256


def tables():
    s16, s64 = sine(CZ), sine(NX)
    tab = np.zeros((T_ROWS, 128))
    modes = eigen(CZ)[:, None, None] + eigen(NX)[None, :, None] + eigen(NY)[None, None, :]
    inv = 1.0 / modes
    tab[T_IM : T_IM + 512] = (
        inv.reshape(8, 2, 64, 64).transpose(0, 2, 1, 3).reshape(512, 128)
    )
    for p in range(8):
        for h in range(2):
            lanes = slice(64 * h, 64 * h + 64)
            for r in range(8):
                tab[T_Z1 + p * 8 + r, lanes] = s16[2 * p + h, 2 * r + h]
                tab[T_Z2 + p * 8 + r, lanes] = s16[2 * p + 1 - h, 2 * r + h]
            for k in range(8):
                tab[T_ZF + p * 8 + k, lanes] = s16[2 * p + h, k] * (-1.0) ** h
            for k in range(3):
                tab[T_W + 8 * k + p, lanes] = s16[2 * p + h, k]
    for at, places in ((T_SX, (63, 0)), (T_SX2, (62, 1))):
        for side, place in enumerate(places):
            tab[at + 64 * side : at + 64 * side + 64] = s64[:, place][:, None]
    packed = tab[T_IM : T_IM + 512].reshape(8, 64, 128)
    tab[T_ALPHA : T_ALPHA + 64] = (packed * tab[T_W : T_W + 8, None, :] ** 2).sum(0)
    tab[T_GAMMA : T_GAMMA + 8] = (packed * tab[None, T_SX : T_SX + 64] ** 2).sum(1)
    mat = np.zeros((B_ROWS, 128))
    mat[B_Y : B_Y + 128] = np.kron(np.eye(2), s64)
    order = np.concatenate([np.arange(0, 64, 2), np.arange(1, 64, 2)])
    mat[B_XF : B_XF + 64, :64] = s64[:, order]
    mat[B_XI : B_XI + 64, :64] = s64[order, :]
    mat = mat.astype(np.float32)
    high = mat.astype(jnp.bfloat16)
    low = (mat - high.astype(np.float32)).astype(jnp.bfloat16)
    return tab.astype(np.float32), high, low


S16 = sine(CZ)


def split(v):
    high = v.astype(BF16)
    return high, (v - high.astype(F32)).astype(BF16)


def dot(a, b):
    return jnp.dot(a, b, preferred_element_type=F32)


def dot_right(v, th, tl):
    vh, vl = split(v)
    return dot(vh, th) + (dot(vl, th) + dot(vh, tl))


def dot_left(th, tl, v):
    vh, vl = split(v)
    return dot(th, vh) + (dot(th, vl) + dot(tl, vh))


def kernel(
    state, burn, fmap, tab_h, bh_h, bl_h, out_s, out_p,
    stn, bnn, fld0, fld1, fields, burning, src, ybuf, hat1, hat, prs, resp,
    turns, xg, zsend, zrecv, dsend, drecv, psend, qsend, qrecv, fsend, frecv, psel, tab, bh, bl, idx,
    in_sem, t_sem, send_sem, recv_sem,
):
    g = lax.axis_index("grp")
    m = lax.axis_index("mesh")
    n = lax.axis_size("mesh")
    fine = g == 0
    LOW, HIGH, PARTNER, LOW2, HIGH2, DLOW, DHIGH = range(7)
    back = (HIGH, LOW, PARTNER, HIGH2, LOW2, DHIGH, DLOW)
    has_low, has_high = m > 0, m < n - 1
    exists = (has_low, has_high, None, m > 1, m < n - 2, has_low, has_high)
    steps = (-1, 1, 0, -2, 2, -1, 1)
    where_to = [
        {"grp": 1 - g if to in (PARTNER, DLOW, DHIGH) else g, "mesh": lax.rem(m + n + steps[to], n)}
        for to in range(7)
    ]
    count = 1
    for to in range(7):
        if exists[to] is not None:
            count = count + exists[to].astype(jnp.int32)

    def guarded(condition, action):
        if condition is None:
            action()
        else:
            pl.when(condition)(action)

    loads = [
        pltpu.make_async_copy(state.at[f], stn.at[f], in_sem.at[f]) for f in range(FIELDS)
    ]
    loads.append(pltpu.make_async_copy(burn, bnn, in_sem.at[FIELDS]))
    for copy in loads:
        copy.start()
    table_loads = [
        pltpu.make_async_copy(a, b, t_sem.at[i])
        for i, (a, b) in enumerate(((fmap, idx.at[0]), (tab_h, tab), (bh_h, bh), (bl_h, bl)))
    ]
    for copy in table_loads:
        copy.start()

    def clear(ref, start, size):
        ref[start : start + size, :] = jnp.zeros((size, 128), F32)

    def level(k, f):
        return (f * (CZ + 2 * HALO) + k + HALO) * PLANE

    @pl.when(jnp.logical_not(has_low))
    def _():
        for f in range(FIELDS):
            clear(fld0, level(-2, f), 2 * PLANE)
            clear(fld1, level(-2, f), 2 * PLANE)
        for s in range(SECTIONS):
            clear(prs.at[s], 0, 3 * PLANE)
            clear(zrecv.at[s, 1], 0, PLANE)
            clear(drecv.at[s, 0], 0, 16)
            clear(qrecv.at[s, 1], 0, 8)

    @pl.when(jnp.logical_not(has_high))
    def _():
        for f in range(FIELDS):
            clear(fld0, level(CZ, f), 2 * PLANE)
            clear(fld1, level(CZ, f), 2 * PLANE)
        for s in range(SECTIONS):
            clear(prs.at[s], (CZ + 3) * PLANE, 3 * PLANE)
            clear(zrecv.at[s, 0], 0, PLANE)
            clear(drecv.at[s, 1], 0, 16)
            clear(qrecv.at[s, 2], 0, 8)

    @pl.when(m < 2)
    def _():
        for s in range(SECTIONS):
            clear(zrecv.at[s, 3], 0, PLANE)

    @pl.when(m > n - 3)
    def _():
        for s in range(SECTIONS):
            clear(zrecv.at[s, 2], 0, PLANE)

    barrier = pltpu.get_barrier_semaphore()
    for to in range(7):
        guarded(
            exists[to],
            lambda to=to: pl.semaphore_signal(
                barrier, inc=1, device_id=where_to[to], device_id_type=MESH
            ),
        )

    messages = []

    class Message:
        def __init__(self, to, a, b):
            slot = len(messages)
            messages.append(self)
            self.to = to
            self.copy = pltpu.make_async_remote_copy(
                src_ref=a, dst_ref=b, send_sem=send_sem.at[slot], recv_sem=recv_sem.at[slot],
                device_id=where_to[to], device_id_type=MESH,
            )
            self.sent = False

        def start(self):
            guarded(exists[self.to], self.copy.start)

        def wait_recv(self):
            guarded(exists[back[self.to]], self.copy.wait_recv)

        def wait_send(self):
            if not self.sent:
                self.sent = True
                guarded(exists[self.to], self.copy.wait_send)

    lane = lax.broadcasted_iota(jnp.int32, (PLANE, 128), 1)
    half0 = lane < 64
    y_last = (lane == 63) | (lane == 127)
    y_first = (lane == 0) | (lane == 64)
    half8 = lax.broadcasted_iota(jnp.int32, (8, 128), 1) < 64
    half64 = lax.broadcasted_iota(jnp.int32, (64, 128), 1) < 64
    sub8 = lax.broadcasted_iota(jnp.int32, (8, 128), 0)

    def swap(v):
        return pltpu.roll(v, 64, 1)

    def rows(start, size):
        return pl.ds(pl.multiple_of(start, 8), size)

    def to_layers(load, store):
        for b in range(2):
            for t in range(4):
                tiles = jnp.stack([load(b, pl.ds((t * 8 + i) * 128, 128)) for i in range(8)])
                turned = jnp.swapaxes(tiles, 0, 1)
                for i in range(8):
                    store(b * 8 + i, t * 8, turned[i])

    def to_native(load, store):
        for b in range(2):
            for t in range(4):
                tiles = jnp.stack([load(b * 8 + i, t * 8) for i in range(8)])
                turned = jnp.swapaxes(tiles, 0, 1)
                for i in range(8):
                    store(b, pl.ds((t * 8 + i) * 128, 128), turned[i])

    def own_plane(fld, f):
        at = jnp.where(fine, PLANE - 1, 0)
        tiles = []
        for odd in range(2):
            tile = jnp.zeros((8, 128), F32)
            for r in range(8):
                one = fld[pl.ds(level(2 * r + odd, f) + at, 1), :]
                tile = jnp.where(sub8 == r, jnp.broadcast_to(one, (8, 128)), tile)
            tiles.append(tile)
        even, odd = tiles
        return jnp.where(
            fine, jnp.where(half8, swap(even), odd), jnp.where(half8, even, swap(odd))
        )

    def halo_messages(fld, f):
        return [
            Message(LOW, fld.at[pl.ds(level(0, f), 2 * PLANE)],
                    fld.at[pl.ds(level(CZ, f), 2 * PLANE)]),
            Message(HIGH, fld.at[pl.ds(level(CZ - 2, f), 2 * PLANE)],
                    fld.at[pl.ds(level(-2, f), 2 * PLANE)]),
        ]

    def gather(plane, who=0):
        index = idx[who]
        column = index & 127
        block = index >> 7
        out = jnp.zeros((8, 128), F32)
        for r in range(8):
            one = jnp.broadcast_to(plane[r : r + 1, :], (8, 128))
            out = jnp.where(block == r, jnp.take_along_axis(one, column, axis=1), out)
        return out

    def spread(ghost, base):
        other = swap(ghost)
        even = jnp.where(half8, ghost, other)
        odd = jnp.where(half8, other, ghost)
        zero = jnp.zeros_like(ghost)
        for side in range(2):
            on = fine if side else jnp.logical_not(fine)
            xg[side, pl.ds(base, 8, stride=2), :] = jnp.where(on, even, zero)
            xg[side, pl.ds(base + 1, 8, stride=2), :] = jnp.where(on, odd, zero)

    def x_sides(v, at, slot):
        base = slot * 48
        turned = swap(v)
        turns[base + 8 : base + 40, :] = turned
        turns[base + 7 : base + 8, :] = xg[0, pl.ds(at, 1), :]
        turns[base + 40 : base + 41, :] = xg[1, pl.ds(at, 1), :]
        down = turns[base + 7 : base + 39, :]
        up = turns[base + 9 : base + 41, :]
        return turned, jnp.where(half0, down, up)

    def y_sides(v):
        north = jnp.where(y_last, 0.0, pltpu.roll(v, 127, 1))
        south = jnp.where(y_first, 0.0, pltpu.roll(v, 1, 1))
        return north, south

    XG = 48
    TAIL = XG + FIELDS * 16

    def tendency_plane(fld, k, finish, u=0):
        c = [fld[rows(level(k, f), PLANE), :] for f in range(FIELDS)]
        reaction = burning[rows(k * PLANE, PLANE), :] * c[3] * c[4]
        source = EXPANSION * reaction
        half = jnp.where(half0, 0.5, -0.5)
        cx = c[0] * (half * -COURANT)
        cy = c[1] * (-0.5 * COURANT)
        cz = c[2] * (-COURANT * 2.0 / 3.0)
        cz2 = c[2] * (COURANT / 12.0)
        for f in range(FIELDS):
            above = fld[rows(level(k + 1, f), PLANE), :]
            below = fld[rows(level(k - 1, f), PLANE), :]
            above2 = fld[rows(level(k + 2, f), PLANE), :]
            below2 = fld[rows(level(k - 2, f), PLANE), :]
            inner, outer = x_sides(c[f], XG + f * 16 + k, u * FIELDS + f)
            north, south = y_sides(c[f])
            dx = inner - outer
            dy = north - south
            dz = above - below
            total = (inner + outer) + (north + south) + (above + below)
            change = (DIFFUSION * total + cx * dx) + (cy * dy + cz * dz) + cz2 * (above2 - below2)
            if f == 0:
                source = source - half * dx
            elif f == 1:
                source = source - 0.5 * dy
            elif f == 2:
                source = source - 0.5 * dz
            elif f == 3:
                change = change - reaction
            else:
                change = change - STOICHIOMETRY * reaction
            finish(k, f, c[f] * (1.0 - 6.0 * DIFFUSION) + change)
        src[rows(k * PLANE, PLANE), :] = source

    def z_inverse(spec, into, base):
        @pl.loop(0, 4)
        def _(t):
            v = [spec[rows(c * PLANE + t * 8, 8), :] for c in range(CZ)]
            for k in range(8):
                even = v[0] * F32(S16[0, k])
                odd = v[1] * F32(S16[1, k])
                for c in range(1, 8):
                    even = even + v[2 * c] * F32(S16[2 * c, k])
                    odd = odd + v[2 * c + 1] * F32(S16[2 * c + 1, k])
                into[rows(base + k * PLANE + t * 8, 8), :] = even + odd
                into[rows(base + (15 - k) * PLANE + t * 8, 8), :] = even - odd

    def y_matrix():
        return bh[B_Y : B_Y + 128, :], bl[B_Y : B_Y + 128, :]

    def y_transform(v):
        return dot_right(v, *y_matrix())

    def x_forward(a, b):
        even = jnp.where(half0, a, swap(b))
        odd = jnp.where(half0, swap(a), b)
        v = jnp.concatenate([even, odd], axis=0)
        return dot_left(bh[B_XF : B_XF + 64, :64], bl[B_XF : B_XF + 64, :64], v)

    def transform(first, last):
        pairs = range(first, 8) if last == 0 else range(last)
        if last == 0:
            v = y_transform(src[first * PLANE : (CZ - first) * PLANE, :])
            planes = {k: v[(k - first) * PLANE : (k - first + 1) * PLANE] for k in range(first, CZ - first)}
        else:
            v = y_transform(
                jnp.concatenate(
                    [src[: last * PLANE, :], src[(CZ - last) * PLANE : CZ * PLANE, :]], axis=0
                )
            )
            planes = {k: v[k * PLANE : (k + 1) * PLANE] for k in range(last)}
            for i in range(last):
                planes[CZ - last + i] = v[(last + i) * PLANE : (last + i + 1) * PLANE]
        for k in pairs:
            ybuf[k * 64 : k * 64 + 64, :] = x_forward(planes[k], planes[CZ - 1 - k])
        for r in range(8):
            turned = []
            for p in pairs:
                v = ybuf[p * 64 + r * 8 : p * 64 + r * 8 + 8, :]
                turned.append(v + jnp.where(half8, swap(v), -swap(v)))
            for q in range(8):
                at = q * 64 + r * 8
                parts = [
                    tab[T_ZF + q * 8 + p : T_ZF + q * 8 + p + 1, :] * v
                    for p, v in zip(pairs, turned)
                ]
                if last:
                    parts.append(hat1[at : at + 8, :])
                while len(parts) > 1:
                    parts = [a + b for a, b in zip(parts[::2], parts[1::2])] + (
                        parts[-1:] if len(parts) % 2 else []
                    )
                total = parts[0]
                if last:
                    total = total * tab[T_IM + at : T_IM + at + 8, :]
                hat1[at : at + 8, :] = total

    def x_inverse(v):
        v = dot_left(bh[B_XI : B_XI + 64, :64], bl[B_XI : B_XI + 64, :64], v)
        even, odd = v[:PLANE], v[PLANE:]
        return jnp.where(half0, even, swap(odd)), jnp.where(half0, swap(even), odd)

    def z_plane(v):
        other = swap(v)
        parts = []
        for p in range(8):
            parts.append(tab[T_Z1 + p * 8 : T_Z1 + p * 8 + 8, :] * v[p : p + 1, :])
            parts.append(tab[T_Z2 + p * 8 : T_Z2 + p * 8 + 8, :] * other[p : p + 1, :])
        while len(parts) > 1:
            parts = [a + b for a, b in zip(parts[::2], parts[1::2])]
        return parts[0]

    def side_x(at=T_SX):
        return tab[rows(at + g * 64, 64), :]

    def weight(k, p):
        return tab[T_W + 8 * k + p : T_W + 8 * k + p + 1, :]

    def modes(p):
        return tab[T_IM + p * 64 : T_IM + p * 64 + 64, :]

    def block(ref, p):
        return ref[p * 64 : p * 64 + 64, :]

    def first_of(acc):
        return acc + swap(acc)

    def last_of(acc):
        other = swap(acc)
        return jnp.where(half64, acc - other, other - acc)

    def z_layers(spec, k):
        acc = weight(k, 0) * block(spec, 0)
        for p in range(1, 8):
            acc = acc + weight(k, p) * block(spec, p)
        return acc

    def x_planes(spec, at):
        sx = side_x(at)
        return jnp.concatenate(
            [jnp.sum(sx * block(spec, p), axis=0, keepdims=True) for p in range(8)], axis=0
        )

    def narrow(v):
        return jnp.where(half0, v[:PLANE], v[PLANE:])

    def widen(v):
        other = swap(v)
        return jnp.concatenate(
            [jnp.where(half0, v, other), jnp.where(half0, other, v)], axis=0
        )

    def z_ghosts(below, above):
        return below + jnp.where(half64, above, -above)

    def layer_response(both, ghost):
        acc = tab[T_ALPHA : T_ALPHA + 64, :] * both
        for p in range(8):
            acc = acc + block(resp, p) * ghost[p : p + 1, :]
        return acc

    def plane_response(layer):
        return jnp.concatenate(
            [jnp.sum(block(resp, p) * layer, axis=0, keepdims=True) for p in range(8)], axis=0
        )

    Z_HIGH, Z_LOW, Z_HIGH2, Z_LOW2 = range(4)

    def solve(s):
        own = prs.at[s]
        acc = z_layers(hat1, 0)
        first, last = first_of(acc), last_of(acc)
        zsend[s, 0] = narrow(first)
        zsend[s, 1] = narrow(last)
        copies = [
            Message(LOW2, zsend.at[s, 0], zrecv.at[s, Z_HIGH2]),
            Message(HIGH2, zsend.at[s, 1], zrecv.at[s, Z_LOW2]),
            Message(LOW, zsend.at[s, 0], zrecv.at[s, Z_HIGH]),
            Message(HIGH, zsend.at[s, 1], zrecv.at[s, Z_LOW]),
        ]
        for copy in copies:
            copy.start()
        start = x_planes(hat1, T_SX)
        plane = z_plane(y_transform(start))
        dsend[s, 0, 0:8, :] = plane
        dsend[s, 1, 0:8, :] = plane
        dsend[s, 0, 8:16, :] = plane_response(first)
        dsend[s, 1, 8:16, :] = plane_response(last)
        sides = [
            Message(DLOW, dsend.at[s, 0], drecv.at[s, 1]),
            Message(DHIGH, dsend.at[s, 1], drecv.at[s, 0]),
            Message(PARTNER, dsend.at[s, 0, pl.ds(0, 8)], qrecv.at[s, 3]),
        ]
        for copy in sides:
            copy.start()
        if s == 0:
            for f in range(FIELDS):
                fsend[1, f * 8 : f * 8 + 8, :] = own_plane(fld1, f)
            early.append(Message(PARTNER, fsend.at[1], frecv.at[1]))
            for f in range(FIELDS):
                early.extend(halo_messages(fld1, f))
            for copy in early:
                copy.start()
            for copy in maps[1:]:
                copy.wait_recv()
        mine = y_transform(z_plane(gather(plane, 1)))
        mine = tab[T_GAMMA : T_GAMMA + 8, :] * mine
        for copy in sides:
            copy.wait_recv()
        response = drecv[s, 0, 8:16, :] + jnp.where(
            half8, drecv[s, 1, 8:16, :], -drecv[s, 1, 8:16, :]
        )
        partner = qrecv[s, 3] + z_plane(y_transform(response + mine))
        ghost = z_plane(gather(partner))
        ghosts = y_transform(
            jnp.concatenate(
                [
                    z_plane(gather(drecv[s, 0, 0:8, :], 2)),
                    z_plane(gather(drecv[s, 1, 0:8, :], 3)),
                    ghost,
                ],
                axis=0,
            )
        )
        ghost = ghosts[16:24]
        for copy in copies:
            copy.wait_recv()

        def got(slot):
            return zrecv[s, slot]

        above = got(Z_HIGH) + narrow(
            first_of(layer_response(z_ghosts(last, widen(got(Z_HIGH2))), ghosts[8:16]))
        )
        below = got(Z_LOW) + narrow(
            last_of(layer_response(z_ghosts(widen(got(Z_LOW2)), first), ghosts[0:8]))
        )
        above = jnp.where(has_high, above, 0.0)
        below = jnp.where(has_low, below, 0.0)
        both = z_ghosts(widen(below), widen(above))
        depth = 3 if s == 0 else 1
        size = depth * PLANE

        def spectrum():
            sx = side_x()
            for p in range(8):
                extra = weight(0, p) * both + sx * ghost[p : p + 1, :]
                hat[p * 64 : p * 64 + 64, :] = block(hat1, p) + extra * modes(p)

        def layers_out(k, acc):
            a, b = x_inverse(jnp.where(half64, first_of(acc), last_of(acc)))
            psend[s, 0, k * PLANE : (k + 1) * PLANE, :] = y_transform(a)
            at = depth - 1 - k
            psend[s, 1, at * PLANE : (at + 1) * PLANE, :] = y_transform(b)

        stack = [
            Message(LOW, psend.at[s, 0, pl.ds(0, size)], own.at[pl.ds((CZ + 3) * PLANE, size)]),
            Message(HIGH, psend.at[s, 1, pl.ds(0, size)], own.at[pl.ds((3 - depth) * PLANE, size)]),
        ]
        if s == 0:
            spectrum()
            planes = y_transform(
                jnp.concatenate([x_planes(hat, T_SX), x_planes(hat, T_SX2)], axis=0)
            )
            for i in range(2):
                qsend[s, i * 8 : i * 8 + 8, :] = z_plane(planes[i * 8 : i * 8 + 8])
            copies = [
                Message(DLOW, qsend.at[s, pl.ds(0, 8)], qrecv.at[s, 2]),
                Message(DHIGH, qsend.at[s, pl.ds(0, 8)], qrecv.at[s, 1]),
                Message(PARTNER, qsend.at[s], psel.at[0]),
            ]
            for copy in copies:
                copy.start()
            for k in range(depth):
                layers_out(k, z_layers(hat, k))
            for copy in stack:
                copy.start()
        else:
            layers_out(0, acc + layer_response(both, ghost))
            for copy in stack:
                copy.start()
            plane = start + plane_response(both) + tab[T_GAMMA : T_GAMMA + 8, :] * ghost
            qsend[s, 0:8, :] = z_plane(y_transform(plane))
            copies = [Message(PARTNER, qsend.at[s, pl.ds(0, 8)], qrecv.at[s, 0])]
            for copy in copies:
                copy.start()
            spectrum()
        copies = stack + copies
        for p in range(8):
            a, b = x_inverse(block(hat, p))
            ybuf[2 * p * PLANE : (2 * p + 1) * PLANE, :] = a
            ybuf[(2 * p + 1) * PLANE : (2 * p + 2) * PLANE, :] = b
        ybuf[...] = y_transform(ybuf[...])
        z_inverse(ybuf, own, 3 * PLANE)
        return copies

    def correct_z(s, k, into, at_of):
        own = prs.at[s]
        above = own[rows((k + 4) * PLANE, PLANE), :]
        below = own[rows((k + 2) * PLANE, PLANE), :]
        at = rows(at_of(k, 2), PLANE)
        into[at, :] = into[at, :] - 0.5 * (above - below)

    def correct_plane(s, k, into, at_of, u=0, along_z=True):
        p = prs[s, rows((k + 3) * PLANE, PLANE), :]
        inner, outer = x_sides(p, 16 + k, u)
        north, south = y_sides(p)
        half = jnp.where(half0, 0.5, -0.5)
        for f, v in enumerate((half * (inner - outer), 0.5 * (north - south))):
            at = rows(at_of(k, f), PLANE)
            into[at, :] = into[at, :] - v
        if along_z:
            correct_z(s, k, into, at_of)

    early = []
    for f in range(FIELDS):
        loads[f].wait()

        def load_state(b, lanes, f=f):
            return stn[f, b * 8 : b * 8 + 8, lanes]

        def store_state(k, r, v, f=f):
            fld0[rows(level(k, f) + r, 8), :] = v

        to_layers(load_state, store_state)
        if f == 0:
            pl.semaphore_wait(barrier, count)
        copies = halo_messages(fld0, f)
        for copy in copies:
            copy.start()
        early.extend(copies)
    for f in range(FIELDS):
        fsend[0, f * 8 : f * 8 + 8, :] = own_plane(fld0, f)
    table_loads[0].wait()
    maps = [
        Message(PARTNER, fsend.at[0], frecv.at[0]),
        Message(PARTNER, idx.at[0], idx.at[1]),
        Message(HIGH, idx.at[0], idx.at[2]),
        Message(LOW, idx.at[0], idx.at[3]),
    ]
    for copy in maps:
        copy.start()
    loads[FIELDS].wait()

    def load_burn(b, lanes):
        return bnn[b * 8 : b * 8 + 8, lanes]

    def store_burn(k, r, v):
        burning[rows(k * PLANE + r, 8), :] = v

    to_layers(load_burn, store_burn)
    for copy in table_loads[1:]:
        copy.wait()
    for p in range(8):
        resp[p * 64 : p * 64 + 64, :] = modes(p) * weight(0, p) * side_x()

    def finish0(k, f, v):
        fld1[rows(level(k, f), PLANE), :] = v

    maps[0].wait_recv()
    for f in range(FIELDS):
        spread(gather(frecv[0, f * 8 : f * 8 + 8, :]), XG + f * 16)

    @pl.loop(0, 6)
    def _(i):
        for u in range(2):
            tendency_plane(fld0, 2 + 2 * i + u, finish0, u)

    transform(2, 0)

    for copy in early:
        copy.wait_recv()

    for u, k in enumerate((0, 1, CZ - 2, CZ - 1)):
        tendency_plane(fld0, k, finish0, u)

    early = []
    transform(0, 2)
    final = solve(0)

    final[4].wait_recv()
    early[0].wait_recv()
    near = psel[0, 0:8, :]
    beside = psel[0, 8:16, :]
    spread(gather(near), 16)
    sides = gather(qsend[0, 0:8, :], 1)
    sign = jnp.where(fine, -0.5, 0.5)
    new0 = frecv[1, 0:8, :] - sign * (sides - beside)
    lane8 = lax.broadcasted_iota(jnp.int32, (8, 128), 1)
    north = jnp.where((lane8 == 63) | (lane8 == 127), 0.0, pltpu.roll(near, 127, 1))
    south = jnp.where((lane8 == 0) | (lane8 == 64), 0.0, pltpu.roll(near, 1, 1))
    new1 = frecv[1, 8:16, :] - 0.5 * (north - south)
    other = swap(near)
    up = jnp.where(sub8 == 7, 0.0, pltpu.roll(other, 7, 0))
    down = jnp.where(sub8 == 0, 0.0, pltpu.roll(other, 1, 0))
    above = jnp.where(half8, other, up)
    below = jnp.where(half8, down, other)
    new2 = frecv[1, 16:24, :] - 0.5 * (above - below)
    for f, v in enumerate((new0, new1, new2, frecv[1, 24:32, :], frecv[1, 32:40, :])):
        spread(gather(v), XG + f * 16)
    for copy in early:
        copy.wait_send()

    @pl.loop(0, 2)
    def _(i):
        for u in range(7):
            correct_plane(0, 1 + 7 * i + u, fld1, level, u)

    def finish1(k, f, v):
        start = fld0[rows(level(k, f), PLANE), :]
        fields[rows((k * FIELDS + f) * PLANE, PLANE), :] = 0.5 * (start + v)

    @pl.loop(0, 5)
    def _(i):
        for u in range(2):
            tendency_plane(fld1, 3 + 2 * i + u, finish1, u)

    transform(3, 0)

    for copy in final[:4] + early[1:]:
        copy.wait_recv()
    spread(gather(qrecv[0, 1], 2), 0)
    spread(gather(qrecv[0, 2], 3), 32)
    over = jnp.broadcast_to(swap(qrecv[0, 2])[0:1, :], (8, 128))
    under = jnp.broadcast_to(swap(qrecv[0, 1])[7:8, :], (8, 128))
    rest = jnp.where(
        half8,
        jnp.where(sub8 == 0, 0.5 * under, 0.0),
        jnp.where(sub8 == 7, -0.5 * over, 0.0),
    )
    spread(gather(rest), TAIL)
    spread(gather(new2 + rest), XG + 2 * 16)

    for u in range(2):
        correct_plane(0, u * (CZ - 1), fld1, level, u)

    @pl.when(has_low)
    def _():
        for u in range(2):
            correct_plane(0, u - 2, fld1, level, u)

    @pl.when(has_high)
    def _():
        for u in range(2):
            correct_plane(0, CZ + u, fld1, level, u)

    for k in range(3, CZ - 3):
        west, east = xg[0, pl.ds(TAIL + k, 1), :], xg[1, pl.ds(TAIL + k, 1), :]
        at = jnp.where(fine, PLANE - 1, 0)
        c = fld1[pl.ds(level(k, 0) + at, 1), :]
        add = 0.5 * (DIFFUSION * (east + west) - (0.5 * COURANT) * c * (east - west))
        lanes = lax.broadcasted_iota(jnp.int32, (1, 128), 1)
        here = jnp.where(fine, lanes, 127 - lanes) >= 64
        row_at = pl.ds((k * FIELDS + 2) * PLANE + at, 1)
        fields[row_at, :] = fields[row_at, :] + jnp.where(here, add, 0.0)

    @pl.loop(0, 2)
    def _(i):
        for u in range(3):
            tendency_plane(fld1, i * (CZ - 3) + u, finish1, u)

    transform(0, 3)
    final = solve(1)
    final[2].wait_recv()
    spread(gather(qrecv[1, 0]), 16)

    def place(k, f):
        return (k * FIELDS + f) * PLANE

    @pl.loop(0, 2)
    def _(i):
        for u in range(7):
            correct_plane(1, 1 + 7 * i + u, fields, place, u)

    for u in range(2):
        correct_plane(1, u * (CZ - 1), fields, place, u, along_z=False)

    def store_head(b, lanes, v):
        out_p[b * 8 : b * 8 + 8, lanes] = v

    to_native(lambda k, r: prs[1, rows((k + 3) * PLANE + r, 8), :], store_head)

    def put_field(f):
        def load_field(k, r):
            return fields[rows(place(k, f) + r, 8), :]

        def store_field(b, lanes, v):
            out_s[f, b * 8 : b * 8 + 8, lanes] = v

        to_native(load_field, store_field)

    for f in (0, 1, 3, 4):
        put_field(f)
    for copy in final[:2]:
        copy.wait_recv()
    for u in range(2):
        correct_z(1, u * (CZ - 1), fields, place)
    put_field(2)
    for copy in messages:
        copy.wait_send()


def finish_kernel(fields, head, out_s, out_p, sems):
    copies = [
        pltpu.make_async_copy(fields, out_s, sems.at[0]),
        pltpu.make_async_copy(head, out_p, sems.at[1]),
    ]
    for copy in copies:
        copy.start()
    for copy in copies:
        copy.wait()


def write_out(fields, head):
    hbm = pl.BlockSpec(memory_space=pltpu.HBM)
    vmem = pl.BlockSpec(memory_space=pltpu.VMEM)
    return pl.pallas_call(
        finish_kernel,
        out_shape=(
            jax.ShapeDtypeStruct(fields.shape, F32),
            jax.ShapeDtypeStruct(head.shape, F32),
        ),
        in_specs=[vmem, vmem],
        out_specs=(hbm, hbm),
        scratch_shapes=[pltpu.SemaphoreType.DMA((2,))],
        compiler_params=pltpu.CompilerParams(vmem_limit_bytes=1 << 20),
        name="write_out",
    )(fields, head)


def step(state, burn, fmap):
    hbm = pl.BlockSpec(memory_space=pltpu.HBM)
    vmem = pl.BlockSpec(memory_space=pltpu.VMEM)
    tab, bh, bl = tables()
    vm = pltpu.VMEM
    layers = (CZ + 2 * HALO) * LEVEL
    return pl.pallas_call(
        kernel,
        out_shape=(
            jax.ShapeDtypeStruct((FIELDS, CZ, NX * NY), F32),
            jax.ShapeDtypeStruct((CZ, NX * NY), F32),
        ),
        in_specs=[hbm] * 6,
        out_specs=(vmem, vmem),
        scratch_shapes=[
            vm((FIELDS, CZ, NX * NY), F32),
            vm((CZ, NX * NY), F32),
            vm((layers, 128), F32),
            vm((layers, 128), F32),
            vm((CZ * LEVEL, 128), F32),
            vm((CZ * PLANE, 128), F32),
            vm((CZ * PLANE, 128), F32),
            vm((CZ * PLANE, 128), F32),
            vm((CZ * PLANE, 128), F32),
            vm((CZ * PLANE, 128), F32),
            vm((SECTIONS, (CZ + 6) * PLANE, 128), F32),
            vm((512, 128), F32),
            vm((7 * FIELDS * 48, 128), F32),
            vm((2, 80 + FIELDS * 16, 128), F32),
            vm((SECTIONS, 2, PLANE, 128), F32),
            vm((SECTIONS, 4, PLANE, 128), F32),
            vm((SECTIONS, 2, 16, 128), F32),
            vm((SECTIONS, 2, 16, 128), F32),
            vm((SECTIONS, 2, 3 * PLANE, 128), F32),
            vm((SECTIONS, 16, 128), F32),
            vm((SECTIONS, 4, 8, 128), F32),
            vm((SECTIONS, FIELDS * 8, 128), F32),
            vm((SECTIONS, FIELDS * 8, 128), F32),
            vm((1, 16, 128), F32),
            vm((T_ROWS, 128), F32),
            vm((B_ROWS, 128), BF16),
            vm((B_ROWS, 128), BF16),
            vm((4, 8, 128), jnp.int32),
            pltpu.SemaphoreType.DMA((FIELDS + 1,)),
            pltpu.SemaphoreType.DMA((4,)),
            pltpu.SemaphoreType.DMA((48,)),
            pltpu.SemaphoreType.DMA((48,)),
        ],
        compiler_params=pltpu.CompilerParams(
            collective_id=0, has_side_effects=True, vmem_limit_bytes=40 << 20
        ),
        name="fire_step",
    )(*[pltpu.with_memory_space_constraint(v, pltpu.HBM) for v in (state, burn, fmap, jnp.asarray(tab), jnp.asarray(bh), jnp.asarray(bl))])


def shards(state, burn_rate, face_map):
    fields, head = write_out(*step(state[0], burn_rate[0], face_map.reshape(8, 128)))
    return fields[None], head[None]


def solution(mesh):
    placed = (P("grp", None, "mesh", None), P("grp", "mesh", None), P("grp", "mesh", None))
    return jax.shard_map(
        shards,
        mesh=mesh,
        in_specs=placed,
        out_specs=(P("grp", None, "mesh", None), P("grp", "mesh", None)),
        check_vma=False,
    )
```
